256 devices in a mesh: grid: 32 (over z, y), atom: 8 (over x, core).
Axes of the slice: x: 4, y: 4, z: 8, core: 2. Of those that a mesh axis runs over, the one named last changes fastest.
Arguments:
- weights: float32 [4194304], P(('grid', 'atom')), may hold values from 0.25 to 4
- target: float32 [4194304], P(('grid', 'atom')), may hold values from -6 to 6
- coupling: float32 [4194304], P(('grid', 'atom')), may hold values from -0.9 to 0.9
- multipole_basis: float32 [25, 4194304], P(None, ('grid', 'atom')), may hold values from -6 to 6
- rho_hist: float32 [8, 4194304], P(None, ('grid', 'atom')), may hold values from -6 to 6
- res_hist: float32 [8, 4194304], P(None, ('grid', 'atom')), may hold values from -6 to 6
- batch_atom: int32 [16384], P(('grid', 'atom')), may hold values from 0 to 4095
- owner_slot: int32 [4096], replicated, may hold values from 0 to 4095, each once
- slot_index: int32 [2], replicated, may hold values from 0 to 7
Outputs:
- density: float32 [4194304], P(('grid', 'atom'))
- moments: float32 [25, 4096], P(None, 'atom')
The draws below stay inside these ranges and needn't reach their ends.
Inputs may be any that keep to these rules, and one draw needn't show every extreme that they name: `owner_slot`: each slot 0 to 4095 belongs to exactly one atom.
All inputs are finite; a program needn't handle non-finite values.
Results may differ from the reference program's by a relative error of at most 0.00011.
Values sent between devices are 32-bit elements; how exact they have to be, the bound alone decides.
A program may use at most 64 MiB of HBM per device.

```python
import math
import jax
import jax.numpy as jnp
import numpy as np
from jax import lax

H = 8
LM = 25
BATCH = 256
ITERS = 2
POINTS = 4194304
BATCHES = 16384
ATOMS = 4096
ATOM_PTS = 1024


def place_ends(result, key, least, largest):
    spot = [jax.random.randint(jax.random.fold_in(key, axis), (), 0, length) for axis, length in enumerate(result.shape)]
    longest = result.shape.index(max(result.shape))
    neighbour = spot[:longest] + [(spot[longest] + 1) % result.shape[longest]] + spot[longest + 1:]
    return result.at[tuple(spot)].set(least).at[tuple(neighbour)].set(largest)


def levels(own_key, dims, pieces, smallest, top_value):
    def one(position, shards_of):
        heights = jax.random.uniform(jax.random.fold_in(jax.random.fold_in(own_key, 6), position), (shards_of,), jnp.float32, smallest / len(pieces), top_value / len(pieces))
        return jnp.repeat(jnp.exp(heights), dims[position] // shards_of).reshape((-1,) + (1,) * (len(dims) - position - 1))

    gain = one(*pieces[0])
    for cut in pieces[1:]:
        gain = gain * one(*cut)
    return gain


def noise(stream_key, shape, scale, reach, shards=(), held_as=jnp.bfloat16):
    gain = levels(stream_key, shape, shards, -0.22, 0.18) if shards else 1.0
    entries = jax.random.normal(stream_key, shape, jnp.float32) * scale * gain
    return jnp.minimum(jnp.maximum(entries, -reach), reach).astype(held_as)


def setup_inputs(seed: int = 0) -> dict:
    splits = jax.random.split(jax.random.key(seed), 10)
    return {
        "weights": jnp.clip(jnp.exp(math.log(4.0) - 2.7725887 * jax.random.uniform(splits[0], (POINTS,), jnp.float32) ** levels(splits[0], (POINTS,), ((0, 256),), -0.2, 0.2)), 0.25, 4.0),
        "target": noise(splits[1], (POINTS,), 1.0, 6.0, ((0, 256),), jnp.float32),
        "coupling": jnp.clip(jax.random.uniform(splits[2], (POINTS,), jnp.float32, -0.9, 0.9) * levels(splits[2], (POINTS,), ((0, 256),), -0.4, 0.0), -0.9, 0.9),
        "multipole_basis": noise(splits[3], (LM, POINTS), 1.0, 6.0, ((1, 256),), jnp.float32),
        "rho_hist": noise(splits[4], (H, POINTS), 1.0, 6.0, ((1, 256),), jnp.float32),
        "res_hist": noise(splits[5], (H, POINTS), 1.0, 6.0, ((1, 256),), jnp.float32),
        "batch_atom": place_ends(jax.random.randint(splits[6], (BATCHES,), 0, ATOMS), jax.random.fold_in(splits[6], 1), 0, ATOMS - 1).astype(jnp.int32),
        "owner_slot": jax.random.permutation(splits[7], ATOMS).astype(jnp.int32),
        "slot_index": jax.random.randint(splits[8], (ITERS,), 0, H).astype(jnp.int32),
    }


damping_table = np.array([1.0 / (1 + degree) for degree in range(5) for order in range(2 * degree + 1)], dtype=np.float32)
mixing_beta = 0.5
ridge_share = 0.1

def mixing_weights(intersect):
    hist_len = intersect.shape[0]
    ridge_val = ridge_share * jnp.trace(intersect) / hist_len
    shifted = intersect + ridge_val * jnp.eye(hist_len, dtype=intersect.dtype)
    factor = jnp.linalg.cholesky(shifted)
    forward = []
    for row_at in range(hist_len):
        entry_val = 1.0
        for col_at in range(row_at):
            entry_val = entry_val - factor[row_at, col_at] * forward[col_at]
        forward.append(entry_val / factor[row_at, row_at])
    backward = [None] * hist_len
    for row_at in reversed(range(hist_len)):
        entry_val = forward[row_at]
        for col_at in range(row_at + 1, hist_len):
            entry_val = entry_val - factor[col_at, row_at] * backward[col_at]
        backward[row_at] = entry_val / factor[row_at, row_at]
    solved = jnp.stack(backward)
    return solved / jnp.sum(solved)

def reference(weights, target, coupling, multipole_basis, rho_hist, res_hist, batch_atom, owner_slot, slot_index):
    hi_prec = lax.Precision.HIGHEST
    damping = jnp.asarray(damping_table, dtype=weights.dtype)
    batch_slot = owner_slot[batch_atom].astype(jnp.int32)
    basis_blocks = multipole_basis.reshape(LM, BATCHES, BATCH)
    density = None
    moments = None
    for iteration in range(ITERS):
        intersect = jnp.dot(res_hist * weights[None, :], res_hist.T, precision=hi_prec)
        coeffs = mixing_weights(intersect)
        rho_mix = jnp.dot(coeffs, rho_hist, precision=hi_prec)
        res_mix = jnp.dot(coeffs, res_hist, precision=hi_prec)
        per_batch = lax.optimization_barrier(jnp.sum((weights * res_mix).reshape(1, BATCHES, BATCH) * basis_blocks, axis=2))
        moments = jax.ops.segment_sum(per_batch.T, batch_slot, num_segments=ATOMS).T / jnp.sqrt(jnp.float32(ATOM_PTS)).astype(weights.dtype)
        at_batch = damping[:, None] * moments[:, batch_slot]
        correct = lax.optimization_barrier(jnp.sum(at_batch[:, :, None] * basis_blocks, axis=0)).reshape(POINTS)
        density = rho_mix + mixing_beta * (res_mix - correct)
        res_new = target + coupling * jnp.tanh(density) - density
        where = slot_index[iteration]
        rho_hist = rho_hist.at[where].set(density)
        res_hist = res_hist.at[where].set(res_new)
    return (density, moments)
```

```python
import jax
import jax.numpy as jnp
from jax import lax
from jax.experimental import pallas as pl
from jax.experimental.pallas import tpu as pltpu
from jax.sharding import Mesh
from jax.sharding import PartitionSpec as P

AXES = ("z", "y", "x", "c")
SIZES = {"z": 8, "y": 4, "x": 4, "c": 2}
HIST = 8
LANES = 128
MESH = pl.DeviceIdType.MESH
F32 = jnp.float32
MIX_BETA = 0.5
RIDGE_SHARE = 0.1
GROUP = 16
ROWS = 13
INT0_A, INT0_B, META_A, META_B, PB0_A, PB0_B, INT1_A, INT1_B, PB1_A, PB1_B, MOM_B, MOM_Z = range(12)
EXCHANGES = 12
LD_RES, LD_W, LD_ATOM, LD_OWNER, LD_BASIS, LD_RHO, LD_TARGET, LD_COUPLING, ST_DEN, ST_MOM = range(10)
LOCALS = 10


def iota(shape, dim):
    return lax.broadcasted_iota(jnp.int32, shape, dim)


def sublane_total(x):
    x = x + pltpu.roll(x, 4, 0)
    x = x + pltpu.roll(x, 2, 0)
    return x + pltpu.roll(x, 1, 0)


def mixing_weights(entry):
    matrix = [[entry[i][j] for j in range(i + 1)] for i in range(HIST)]
    trace = matrix[0][0]
    for i in range(1, HIST):
        trace = trace + matrix[i][i]
    ridge = trace * (RIDGE_SHARE / HIST)
    for i in range(HIST):
        matrix[i][i] = matrix[i][i] + ridge
    forward = [jnp.ones((8, LANES), F32) for _ in range(HIST)]
    pivot = [None] * HIST
    lower = [[None] * HIST for _ in range(HIST)]
    for j in range(HIST):
        pivot[j] = 1.0 / matrix[j][j]
        for i in range(j + 1, HIST):
            ratio = matrix[i][j] * pivot[j]
            for k in range(j + 1, i + 1):
                matrix[i][k] = matrix[i][k] - ratio * matrix[k][j]
            forward[i] = forward[i] - ratio * forward[j]
            lower[i][j] = ratio
    solved = [None] * HIST
    for i in reversed(range(HIST)):
        value = forward[i] * pivot[i]
        for k in range(i + 1, HIST):
            value = value - lower[k][i] * solved[k]
        solved[i] = value
    total = solved[0]
    for i in range(1, HIST):
        total = total + solved[i]
    scale = 1.0 / total
    return [value * scale for value in solved]


def history_column(values):
    sub = iota((8, LANES), 0)
    column = jnp.zeros((8, LANES), F32)
    for i in range(HIST):
        column = jnp.where(sub == i, values[i], column)
    return column


def three_parts(x):
    high = x.astype(jnp.bfloat16)
    rest = x - high.astype(F32)
    middle = rest.astype(jnp.bfloat16)
    low = (rest - middle.astype(F32)).astype(jnp.bfloat16)
    return jnp.concatenate([high, middle, low], axis=0)


def body(
    w_h, t_h, cpl_h, basis_h, rho_h, res_h, atom_h, owner_h, slot_index,
    den_h, mom_h,
    w, t, cpl, basis, rho, res, atom, owner, den, rnew, mom,
    entries, same_atom, same_slot,
    int0_a, int0_b, int1_a, int1_b, meta_a, meta_b,
    pb0_a, pb0_b, pb1_a, pb1_b, mom_b, mom_z, send0, send1, send2,
    local_sem, send_sem, recv_sem,
):
    me = {name: lax.axis_index(name) for name in AXES}
    own_a = me["y"] * 4 + me["x"]
    own_b = me["c"] * 8 + me["z"]
    blocks = w.shape[0]

    loads = {}
    for key, src, dst in (
        (LD_RES, res_h, res), (LD_W, w_h, w), (LD_ATOM, atom_h, atom), (LD_OWNER, owner_h, owner),
        (LD_BASIS, basis_h, basis), (LD_RHO, rho_h, rho), (LD_TARGET, t_h, t), (LD_COUPLING, cpl_h, cpl),
    ):
        loads[key] = pltpu.make_async_copy(src, dst, local_sem.at[key])
        loads[key].start()

    peers_a = []
    for dy in range(4):
        for dx in range(4):
            if dy or dx:
                peers_a.append({"y": lax.rem(me["y"] + dy, 4), "x": lax.rem(me["x"] + dx, 4)})
    peers_b = []
    for dc in range(2):
        for dz in range(8):
            if dc or dz:
                peers_b.append({"z": lax.rem(me["z"] + dz, 8), "c": lax.rem(me["c"] + dc, 2)})

    barrier = pltpu.get_barrier_semaphore()
    for peer in peers_a + peers_b:
        pl.semaphore_signal(barrier, inc=1, device_id=peer, device_id_type=MESH)

    def send(src, dst, key, peer):
        pltpu.make_async_remote_copy(
            src_ref=src, dst_ref=dst, send_sem=send_sem.at[key], recv_sem=recv_sem.at[key],
            device_id=peer, device_id_type=MESH,
        ).start()

    def gather(buf, own, key, peers):
        for peer in peers:
            send(buf.at[own], buf.at[own], key, peer)

    def arrived(buf, key, count):
        view = buf.at[pl.ds(0, count)]
        pltpu.make_async_copy(view, view, recv_sem.at[key]).wait()

    def sent(buf, key, count):
        view = buf.at[pl.ds(0, count)]
        pltpu.make_async_copy(view, view, send_sem.at[key]).wait()

    sub = iota((8, LANES), 0)
    lane = iota((8, LANES), 1)

    loads[LD_RES].wait()
    loads[LD_W].wait()

    def products(q, accs):
        accs = list(accs)
        for u in range(8):
            off = pl.multiple_of((q * 8 + u) * LANES, LANES)
            r = res[:, pl.ds(off, LANES)]
            rw = r * jnp.broadcast_to(w[pl.ds(q * 8 + u, 1), :], (8, LANES))
            accs[0] = accs[0] + rw * r
            for s in range(1, 5):
                accs[s] = accs[s] + rw * pltpu.roll(r, s, 0)
        return tuple(accs)

    zero = jnp.zeros((8, LANES), F32)
    accs = lax.fori_loop(0, blocks // 8, products, (zero,) * 5)
    placed = zero
    for s in range(5):
        total = jnp.sum(accs[s], axis=1, keepdims=True)
        placed = jnp.where(lane == 8 * s + sub, total, placed)
    int0_a[own_a] = sublane_total(placed)[0:1, :]

    pl.semaphore_wait(barrier, len(peers_a) + len(peers_b))
    gather(int0_a, own_a, INT0_A, peers_a)

    loads[LD_ATOM].wait()
    loads[LD_OWNER].wait()
    batches = 64
    wide_sub = iota((batches, LANES), 0)
    wide_lane = iota((batches, LANES), 1)
    atom_row = atom[0:1, :].astype(F32)
    atom_col = jnp.sum(
        jnp.where(wide_lane == wide_sub, jnp.broadcast_to(atom_row, (batches, LANES)), 0.0), axis=1, keepdims=True
    )

    def look_up(j, found):
        owners = jnp.broadcast_to(owner[pl.ds(j, 1), :].astype(F32), (batches, LANES))
        number = (wide_lane + j * LANES).astype(F32)
        return found + jnp.where(number == atom_col, owners, 0.0)

    found = lax.fori_loop(0, owner.shape[0], look_up, jnp.zeros((batches, LANES), F32))
    slot_col = jnp.sum(found, axis=1, keepdims=True)
    slot_wide = jnp.sum(
        jnp.where((wide_lane == wide_sub) | (wide_lane == wide_sub + batches), slot_col, 0.0), axis=0, keepdims=True
    )
    atom_wide = jnp.sum(
        jnp.where((wide_lane == wide_sub) | (wide_lane == wide_sub + batches), atom_col, 0.0), axis=0, keepdims=True
    )
    meta = jnp.concatenate([atom_wide, slot_wide], axis=0).astype(jnp.int32)
    meta_a[own_a] = meta
    meta_b[own_b] = meta
    gather(meta_a, own_a, META_A, peers_a)
    gather(meta_b, own_b, META_B, peers_b)

    def group_sum(buf, own, key):
        arrived(buf, key, GROUP - 1)
        total = buf[0]
        for i in range(1, GROUP):
            total = total + buf[i]
        return total

    int0_b[own_b] = group_sum(int0_a, own_a, INT0_A)
    gather(int0_b, own_b, INT0_B, peers_b)

    arrived(meta_a, META_A, GROUP - 1)
    arrived(meta_b, META_B, GROUP - 1)
    half = iota((1, LANES), 1) < batches
    atoms_b = [
        jnp.where(half, meta_b[2 * q, 0:1, :], meta_b[2 * q + 1, 0:1, :]).astype(F32) for q in range(GROUP // 2)
    ]
    slot_base = me["x"] * (GROUP * batches)

    def relate(s, nothing):
        both = meta_a[s].astype(F32)
        own_lane = wide_lane == wide_sub
        atoms_a = jnp.sum(jnp.where(own_lane, jnp.broadcast_to(both[0:1], (batches, LANES)), 0.0), axis=1, keepdims=True)
        slots_a = jnp.sum(jnp.where(own_lane, jnp.broadcast_to(both[1:2], (batches, LANES)), 0.0), axis=1, keepdims=True)
        at = pl.ds(pl.multiple_of(s * batches, batches), batches)
        for q in range(GROUP // 2):
            cols = pl.ds(q * LANES, LANES)
            same_atom[at, cols] = jnp.where(atoms_a == atoms_b[q], 1.0, 0.0).astype(jnp.bfloat16)
            number = (iota((1, LANES), 1) + (slot_base + q * LANES)).astype(F32)
            same_slot[at, cols] = jnp.where(slots_a == number, 1.0, 0.0).astype(jnp.bfloat16)
        return nothing

    lax.fori_loop(0, GROUP, relate, 0)

    def entry_values(row, count):
        rows = iota((count, LANES), 0)
        lanes = iota((count, LANES), 1)
        total = jnp.sum(jnp.where(rows == lanes, jnp.broadcast_to(row, (count, LANES)), 0.0), axis=1, keepdims=True)
        return jnp.broadcast_to(total, (count, LANES))

    def splat(base, i):
        return jnp.broadcast_to(entries[pl.ds(base + i, 1), :], (8, LANES))

    def batch_moments(column):
        def four(q, carry):
            k01, k2, k3 = carry
            for u in range(4):
                b = q * 4 + u
                offs, field = [], []
                for h in range(2):
                    j = q * 8 + 2 * u + h
                    off = pl.ds(pl.multiple_of(j * LANES, LANES), LANES)
                    mixed = sublane_total(column * res[:, off])
                    field.append(mixed * jnp.broadcast_to(w[pl.ds(j, 1), :], (8, LANES)))
                    offs.append(off)
                parts = []
                for kt in range(3):
                    rows = pl.ds(kt * 8, 8)
                    product = basis[rows, offs[0]] * field[0] + basis[rows, offs[1]] * field[1]
                    parts.append(jnp.sum(product, axis=1, keepdims=True))
                last = basis[24:25, offs[0]] * field[0][0:1] + basis[24:25, offs[1]] * field[1][0:1]
                last = jnp.sum(last, axis=1, keepdims=True)
                k01 = jnp.where(lane == b, parts[0], k01)
                k01 = jnp.where(lane == b + batches, parts[1], k01)
                k2 = jnp.where(lane == b + jnp.where(sub >= 4, batches, 0), parts[2], k2)
                k3 = jnp.where(lane[0:1] == b, last, k3)
            return k01, k2, k3

        return lax.fori_loop(0, batches // 4, four, (zero, zero, zero[0:1]))

    def put_moments(buf, at, k01, k2, k3):
        buf[at, 0:8] = k01
        buf[at, 8:12] = (k2 + pltpu.roll(k2, 4, 0))[0:4]
        buf[at, 12:13] = k3

    def left_sides(buf):
        is_low = iota((ROWS, LANES), 1) < batches
        lows, highs = [], []
        for q in range(GROUP // 2):
            first, second = buf[2 * q], buf[2 * q + 1]
            lows.append(jnp.where(is_low, first, pltpu.roll(second, batches, 1)))
            highs.append(jnp.where(is_low, pltpu.roll(first, batches, 1), second))
        pad = jnp.zeros((16 - ROWS, GROUP * batches), F32)
        low = jnp.concatenate(lows, axis=1)
        high = jnp.concatenate(highs, axis=1)
        return three_parts(jnp.concatenate([low, pad, high, pad], axis=0))

    def contributions(parts, matrix, out):
        result = jnp.dot(parts, matrix[...], preferred_element_type=F32)
        result = result[0:32] + result[32:64] + result[64:96]
        is_low = iota((ROWS, LANES), 1) < batches
        for q in range(GROUP // 2):
            cols = slice(q * LANES, (q + 1) * LANES)
            low, high = result[0:ROWS, cols], result[16:16 + ROWS, cols]
            out[2 * q] = jnp.where(is_low, low, pltpu.roll(high, batches, 1))
            out[2 * q + 1] = jnp.where(is_low, pltpu.roll(low, batches, 1), high)

    def scatter(out, buf, key):
        buf[own_b] = out[own_b]
        for peer in peers_b:
            send(out.at[peer.get("c") * 8 + peer.get("z")], buf.at[own_b], key, peer)

    def packed_scale(rows):
        r, c = iota((rows, LANES), 0), iota((rows, LANES), 1)
        high = c >= batches
        k = jnp.where(r < 8, jnp.where(high, r + 8, r), jnp.where(high, r + 12, r + 8))
        k = jnp.where(r == 12, 24, k)
        degree = (
            jnp.where(k >= 1, 1, 0) + jnp.where(k >= 4, 1, 0) + jnp.where(k >= 9, 1, 0) + jnp.where(k >= 16, 1, 0)
        )
        return 1.0 / (1.0 + degree.astype(F32))

    moment_scale = 1.0 / 32.0

    def mixed_density(total, column, final):
        total = total * (packed_scale(ROWS) * (MIX_BETA * moment_scale))
        first = total[0:8]
        rest = jnp.concatenate([total[8:13], jnp.zeros((3, LANES), F32)], axis=0)
        second = jnp.where(sub < 4, rest, pltpu.roll(pltpu.roll(rest, 4, 0), batches, 1))
        last = jnp.broadcast_to(rest[4:5], (8, LANES))

        def eight(q, carry):
            first, second, last = carry
            dense = zero
            for u in range(4):
                cols = (
                    jnp.broadcast_to(first[:, u:u + 1], (8, LANES)),
                    jnp.broadcast_to(first[:, batches + u:batches + u + 1], (8, LANES)),
                    jnp.broadcast_to(second[:, u:u + 1], (8, LANES)),
                )
                col_last = jnp.broadcast_to(last[:, u:u + 1], (8, LANES))
                for h in range(2):
                    r = 2 * u + h
                    off = pl.ds(pl.multiple_of((q * 8 + r) * LANES, LANES), LANES)
                    y = column * (rho[:, off] + MIX_BETA * res[:, off])
                    for kt in range(3):
                        y = y - cols[kt] * basis[kt * 8:kt * 8 + 8, off]
                    y = sublane_total(y) - col_last * jnp.broadcast_to(basis[24:25, off], (8, LANES))
                    dense = jnp.where(sub == r, y, dense)
            at = pl.ds(pl.multiple_of(q * 8, 8), 8)
            den[at, :] = dense
            if not final:
                rnew[at, :] = t[at, :] + cpl[at, :] * jnp.tanh(dense) - dense
            return tuple(pltpu.roll(x, LANES - 4, 1) for x in (first, second, last))

        lax.fori_loop(0, blocks // 8, eight, (first, second, last))

    row = group_sum(int0_b, own_b, INT0_B)
    entries[0:40, :] = entry_values(row, 40)

    def pair(i, j):
        s = (i - j) % 8
        return splat(0, 8 * s + i) if s <= 4 else splat(0, 8 * ((j - i) % 8) + j)

    column0 = history_column(mixing_weights([[pair(i, j) for j in range(i + 1)] for i in range(HIST)]))
    loads[LD_BASIS].wait()
    put_moments(pb0_a, own_a, *batch_moments(column0))
    gather(pb0_a, own_a, PB0_A, peers_a)
    arrived(pb0_a, PB0_A, GROUP - 1)
    contributions(left_sides(pb0_a), same_atom, send0)
    scatter(send0, pb0_b, PB0_B)
    loads[LD_RHO].wait()
    loads[LD_TARGET].wait()
    loads[LD_COUPLING].wait()
    mixed_density(group_sum(pb0_b, own_b, PB0_B), column0, False)

    where = slot_index[0]
    at_slot = sub == where

    def new_products(q, acc):
        for u in range(8):
            j = q * 8 + u
            off = pl.ds(pl.multiple_of(j * LANES, LANES), LANES)
            fresh = jnp.broadcast_to(rnew[pl.ds(j, 1), :], (8, LANES))
            kept = jnp.where(at_slot, fresh, res[:, off])
            res[:, off] = kept
            rho[:, off] = jnp.where(at_slot, jnp.broadcast_to(den[pl.ds(j, 1), :], (8, LANES)), rho[:, off])
            acc = acc + kept * (fresh * jnp.broadcast_to(w[pl.ds(j, 1), :], (8, LANES)))
        return acc

    acc = lax.fori_loop(0, blocks // 8, new_products, zero)
    total = jnp.sum(acc, axis=1, keepdims=True)
    int1_a[own_a] = sublane_total(jnp.where(lane == sub, total, 0.0))[0:1, :]
    gather(int1_a, own_a, INT1_A, peers_a)
    int1_b[own_b] = group_sum(int1_a, own_a, INT1_A)
    gather(int1_b, own_b, INT1_B, peers_b)
    row = group_sum(int1_b, own_b, INT1_B)
    entries[40:48, :] = entry_values(row, 8)
    fresh_row = [splat(40, i) for i in range(HIST)]
    column1 = history_column(
        mixing_weights([
            [jnp.where(where == i, fresh_row[j], jnp.where(where == j, fresh_row[i], pair(i, j))) for j in range(i + 1)]
            for i in range(HIST)
        ])
    )

    put_moments(pb1_a, own_a, *batch_moments(column1))
    gather(pb1_a, own_a, PB1_A, peers_a)
    arrived(pb1_a, PB1_A, GROUP - 1)
    sides = left_sides(pb1_a)
    contributions(sides, same_atom, send1)
    scatter(send1, pb1_b, PB1_B)
    contributions(sides, same_slot, send2)
    scatter(send2, mom_b, MOM_B)
    mixed_total = group_sum(pb1_b, own_b, PB1_B)
    owned = group_sum(mom_b, own_b, MOM_B) * moment_scale
    mom_z[me["z"]] = owned
    for dz in range(1, 8):
        send(mom_z.at[me["z"]], mom_z.at[me["z"]], MOM_Z, {"z": lax.rem(me["z"] + dz, 8)})
    mixed_density(mixed_total, column1, True)
    store_den = pltpu.make_async_copy(den, den_h, local_sem.at[ST_DEN])
    store_den.start()
    arrived(mom_z, MOM_Z, 7)
    low_half = iota((8, LANES), 1) < batches
    for q in range(4):
        first, second = mom_z[2 * q], mom_z[2 * q + 1]
        cols = slice(q * LANES, (q + 1) * LANES)
        is_low = iota((ROWS, LANES), 1) < batches
        low = jnp.where(is_low, first, pltpu.roll(second, batches, 1))
        high = jnp.where(is_low, pltpu.roll(first, batches, 1), second)
        mom[0:8, cols] = low[0:8]
        mom[8:16, cols] = high[0:8]
        mom[16:20, cols] = low[8:12]
        mom[20:24, cols] = high[8:12]
        mom[24:25, cols] = low[12:13]
    store_mom = pltpu.make_async_copy(mom, mom_h, local_sem.at[ST_MOM])
    store_mom.start()

    for buf, key, count in (
        (int0_a, INT0_A, 15), (int0_b, INT0_B, 15), (meta_a, META_A, 15), (meta_b, META_B, 15),
        (pb0_a, PB0_A, 15), (pb0_b, PB0_B, 15), (int1_a, INT1_A, 15), (int1_b, INT1_B, 15),
        (pb1_a, PB1_A, 15), (pb1_b, PB1_B, 15), (mom_b, MOM_B, 15), (mom_z, MOM_Z, 7),
    ):
        sent(buf, key, count)
    store_den.wait()
    store_mom.wait()


def local(weights, target, coupling, basis, rho_hist, res_hist, batch_atom, owner_slot, slot_index):
    points = weights.shape[0]
    blocks = points // LANES
    harmonics = basis.shape[0]
    batches = batch_atom.shape[0]
    slots = owner_slot.shape[0]
    dense = lambda x: x.reshape(blocks, LANES)
    atom_row = jnp.pad(batch_atom, (0, LANES - batches)).reshape(1, LANES)
    hbm = pl.BlockSpec(memory_space=pltpu.HBM)
    smem = pl.BlockSpec(memory_space=pltpu.SMEM)
    small = lambda: pltpu.VMEM((GROUP, 1, LANES), F32)
    block = lambda count: pltpu.VMEM((count, ROWS, LANES), F32)
    relation = pltpu.VMEM((GROUP * batches, GROUP * batches), jnp.bfloat16)
    density, moments = pl.pallas_call(
        body,
        out_shape=(
            jax.ShapeDtypeStruct((blocks, LANES), F32),
            jax.ShapeDtypeStruct((harmonics, slots // 8), F32),
        ),
        in_specs=[hbm] * 8 + [smem],
        out_specs=(hbm, hbm),
        scratch_shapes=[
            pltpu.VMEM((blocks, LANES), F32),
            pltpu.VMEM((blocks, LANES), F32),
            pltpu.VMEM((blocks, LANES), F32),
            pltpu.VMEM((harmonics, points), F32),
            pltpu.VMEM((HIST, points), F32),
            pltpu.VMEM((HIST, points), F32),
            pltpu.VMEM((1, LANES), jnp.int32),
            pltpu.VMEM((slots // LANES, LANES), jnp.int32),
            pltpu.VMEM((blocks, LANES), F32),
            pltpu.VMEM((blocks, LANES), F32),
            pltpu.VMEM((harmonics, slots // 8), F32),
            pltpu.VMEM((48, LANES), F32),
            relation,
            relation,
            small(), small(), small(), small(),
            pltpu.VMEM((GROUP, 2, LANES), jnp.int32),
            pltpu.VMEM((GROUP, 2, LANES), jnp.int32),
            block(GROUP), block(GROUP), block(GROUP), block(GROUP), block(GROUP), block(8),
            block(GROUP), block(GROUP), block(GROUP),
            pltpu.SemaphoreType.DMA((LOCALS,)),
            pltpu.SemaphoreType.DMA((EXCHANGES,)),
            pltpu.SemaphoreType.DMA((EXCHANGES,)),
        ],
        compiler_params=pltpu.CompilerParams(collective_id=0, has_side_effects=True),
    )(
        dense(weights), dense(target), dense(coupling), basis, rho_hist, res_hist,
        atom_row, owner_slot.reshape(slots // LANES, LANES), slot_index,
    )
    return density.reshape(points), moments


def solution(mesh):
    torus = Mesh(mesh.devices.reshape(tuple(SIZES.values())), AXES)
    points = P(AXES)
    rows = P(None, AXES)
    return jax.shard_map(
        local,
        mesh=torus,
        in_specs=(points, points, points, rows, rows, rows, points, P(), P()),
        out_specs=(points, P(None, ("x", "c"))),
        check_vma=False,
    )
```

```python
import itertools

import jax
import jax.numpy as jnp
from jax import lax
from jax.experimental import pallas as pl
from jax.experimental.pallas import tpu as pltpu
from jax.sharding import Mesh
from jax.sharding import PartitionSpec as P

AXES = ("z", "y", "x", "c")
SIZES = {"z": 8, "y": 4, "x": 4, "c": 2}
HIST = 8
LANES = 128
MESH = pl.DeviceIdType.MESH
F32 = jnp.float32
MIX_BETA = 0.5
RIDGE_SHARE = 0.1
GROUP = 16
ROWS = 13
INT0_A, INT0_B, ATOM_A, ATOM_B, SLOT_A, HIST_A, NEW_A, INT1_B, PB0_B, PB1_B, MOM_B, MOM_Z = range(12)
EXCHANGES = 12
LD_RES, LD_W, LD_ATOM, LD_OWNER, LD_BASIS, LD_RHO, LD_TARGET, LD_COUPLING, ST_DEN, ST_MOM = range(10)
LOCALS = 10


def iota(shape, dim):
    return lax.broadcasted_iota(jnp.int32, shape, dim)


def sublane_total(x):
    x = x + pltpu.roll(x, 4, 0)
    x = x + pltpu.roll(x, 2, 0)
    return x + pltpu.roll(x, 1, 0)


def mixing_weights(entry):
    matrix = [[entry[i][j] for j in range(i + 1)] for i in range(HIST)]
    trace = matrix[0][0]
    for i in range(1, HIST):
        trace = trace + matrix[i][i]
    ridge = trace * (RIDGE_SHARE / HIST)
    for i in range(HIST):
        matrix[i][i] = matrix[i][i] + ridge
    forward = [jnp.ones((8, LANES), F32) for _ in range(HIST)]
    pivot = [None] * HIST
    lower = [[None] * HIST for _ in range(HIST)]
    for j in range(HIST):
        pivot[j] = 1.0 / matrix[j][j]
        for i in range(j + 1, HIST):
            ratio = matrix[i][j] * pivot[j]
            for k in range(j + 1, i + 1):
                matrix[i][k] = matrix[i][k] - ratio * matrix[k][j]
            forward[i] = forward[i] - ratio * forward[j]
            lower[i][j] = ratio
    solved = [None] * HIST
    for i in reversed(range(HIST)):
        value = forward[i] * pivot[i]
        for k in range(i + 1, HIST):
            value = value - lower[k][i] * solved[k]
        solved[i] = value
    total = solved[0]
    for i in range(1, HIST):
        total = total + solved[i]
    scale = 1.0 / total
    return [value * scale for value in solved]


def history_column(values):
    sub = iota((8, LANES), 0)
    column = jnp.zeros((8, LANES), F32)
    for i in range(HIST):
        column = jnp.where(sub == i, values[i], column)
    return column


def three_parts(x):
    high = x.astype(jnp.bfloat16)
    rest = x - high.astype(F32)
    middle = rest.astype(jnp.bfloat16)
    low = (rest - middle.astype(F32)).astype(jnp.bfloat16)
    return jnp.concatenate([high, middle, low], axis=0)


def body(
    w_h, t_h, cpl_h, basis_h, rho_h, res_h, atom_h, owner_h, slot_index,
    den_h, mom_h,
    w, t, cpl, basis, rho, res, wres, atom, owner, den, rnew, mom,
    entries, same_atom, same_slot,
    int0_a, int0_b, int1_b, atom_a, atom_b, slot_a,
    hist_a, new_a, pb0_b, pb1_b, mom_b, mom_z, send0, send1, send2,
    local_sem, send_sem, recv_sem,
):
    me = {name: lax.axis_index(name) for name in AXES}
    own_a = me["y"] * 4 + me["x"]
    own_b = me["c"] * 8 + me["z"]
    blocks = w.shape[0]

    loads = {}
    for key, src, dst in (
        (LD_RES, res_h, res), (LD_W, w_h, w), (LD_ATOM, atom_h, atom), (LD_OWNER, owner_h, owner),
        (LD_BASIS, basis_h, basis), (LD_RHO, rho_h, rho), (LD_TARGET, t_h, t), (LD_COUPLING, cpl_h, cpl),
    ):
        loads[key] = pltpu.make_async_copy(src, dst, local_sem.at[key])
        loads[key].start()

    def peers(*names):
        steps = [s for s in itertools.product(*(range(SIZES[name]) for name in names)) if any(s)]
        hops = lambda s: sum(min(d, SIZES[name] - d) for d, name in zip(s, names))
        steps.sort(key=hops, reverse=True)
        return [{name: lax.rem(me[name] + d, SIZES[name]) for d, name in zip(s, names)} for s in steps]

    peers_a, peers_b, peers_z = peers("y", "x"), peers("z", "c"), peers("z")

    barrier = pltpu.get_barrier_semaphore()
    for peer in peers_a + peers_b:
        pl.semaphore_signal(barrier, inc=1, device_id=peer, device_id_type=MESH)

    def send(src, dst, key, peer):
        pltpu.make_async_remote_copy(
            src_ref=src, dst_ref=dst, send_sem=send_sem.at[key], recv_sem=recv_sem.at[key],
            device_id=peer, device_id_type=MESH,
        ).start()

    def gather(buf, own, key, peers):
        for peer in peers:
            send(buf.at[own], buf.at[own], key, peer)

    def arrived(buf, key, count):
        view = buf.at[pl.ds(0, count)]
        pltpu.make_async_copy(view, view, recv_sem.at[key]).wait()

    def sent(buf, key, count):
        view = buf.at[pl.ds(0, count)]
        pltpu.make_async_copy(view, view, send_sem.at[key]).wait()

    sub = iota((8, LANES), 0)
    lane = iota((8, LANES), 1)

    loads[LD_RES].wait()
    loads[LD_W].wait()

    def products(q, accs):
        accs = list(accs)
        for u in range(8):
            off = pl.multiple_of((q * 8 + u) * LANES, LANES)
            r = res[:, pl.ds(off, LANES)]
            rw = r * jnp.broadcast_to(w[pl.ds(q * 8 + u, 1), :], (8, LANES))
            wres[:, pl.ds(off, LANES)] = rw
            accs[0] = accs[0] + rw * r
            for s in range(1, 5):
                accs[s] = accs[s] + rw * pltpu.roll(r, s, 0)
        return tuple(accs)

    zero = jnp.zeros((8, LANES), F32)
    accs = lax.fori_loop(0, blocks // 8, products, (zero,) * 5)
    placed = zero
    for s in range(5):
        total = jnp.sum(accs[s], axis=1, keepdims=True)
        placed = jnp.where(lane == 8 * s + sub, total, placed)
    int0_a[own_a] = sublane_total(placed)[0:1, :]

    batches = 64
    loads[LD_BASIS].wait()

    def place(b, parts, k01, k2):
        k01 = jnp.where(lane == b, parts[0], k01)
        k01 = jnp.where(lane == b + batches, parts[1], k01)
        return k01, jnp.where(lane == b + jnp.where(sub >= 4, batches, 0), parts[2], k2)

    def history_batch(b, carry):
        carry = list(carry)
        offs = [pl.ds(pl.multiple_of((2 * b + h) * LANES, LANES), LANES) for h in range(2)]
        tiles = [[basis[kt * 8:kt * 8 + 8, off] for off in offs] for kt in range(3)]
        for i in range(HIST):
            field = [jnp.broadcast_to(wres[i:i + 1, off], (8, LANES)) for off in offs]
            parts = [
                jnp.sum(tiles[kt][0] * field[0] + tiles[kt][1] * field[1], axis=1, keepdims=True) for kt in range(3)
            ]
            carry[2 * i], carry[2 * i + 1] = place(b, parts, carry[2 * i], carry[2 * i + 1])
        last = [wres[:, off] * jnp.broadcast_to(basis[24:25, off], (8, LANES)) for off in offs]
        last = jnp.sum(last[0] + last[1], axis=1, keepdims=True)
        carry[16] = jnp.where(lane == b, last, carry[16])
        return tuple(carry)

    def put_moments(buf, at, k01, k2, k3):
        buf[(*at, slice(0, 8))] = k01
        buf[(*at, slice(8, 12))] = (k2 + pltpu.roll(k2, 4, 0))[0:4]
        buf[(*at, slice(12, 13))] = k3

    moments0 = lax.fori_loop(0, batches, history_batch, (zero,) * 17, unroll=2)
    for i in range(HIST):
        put_moments(hist_a, (own_a, i), moments0[2 * i], moments0[2 * i + 1], moments0[16][i:i + 1])

    loads[LD_ATOM].wait()
    atom_wide = jnp.concatenate([atom[...], atom[...]], axis=1)
    atom_a[own_a] = atom_wide
    atom_b[own_b] = atom_wide

    pl.semaphore_wait(barrier, len(peers_a) + len(peers_b))
    gather(int0_a, own_a, INT0_A, peers_a)
    gather(atom_a, own_a, ATOM_A, peers_a)
    gather(atom_b, own_b, ATOM_B, peers_b)
    gather(hist_a, own_a, HIST_A, peers_a)

    loads[LD_OWNER].wait()
    wide_sub = iota((batches, LANES), 0)
    wide_lane = iota((batches, LANES), 1)
    own_lane = wide_lane == wide_sub

    def as_column(row):
        return jnp.sum(jnp.where(own_lane, jnp.broadcast_to(row, (batches, LANES)), 0.0), axis=1, keepdims=True)

    atom_col = as_column(atom_wide.astype(F32))

    def look_up(j, found):
        owners = jnp.broadcast_to(owner[pl.ds(j, 1), :].astype(F32), (batches, LANES))
        number = (wide_lane + j * LANES).astype(F32)
        return found + jnp.where(number == atom_col, owners, 0.0)

    found = lax.fori_loop(0, owner.shape[0], look_up, jnp.zeros((batches, LANES), F32))
    slot_col = jnp.sum(found, axis=1, keepdims=True)
    slot_a[own_a] = jnp.sum(jnp.where(own_lane, slot_col, 0.0), axis=0, keepdims=True).astype(jnp.int32)
    gather(slot_a, own_a, SLOT_A, peers_a)

    def group_sum(buf, own, key):
        arrived(buf, key, GROUP - 1)
        total = buf[0]
        for i in range(1, GROUP):
            total = total + buf[i]
        return total

    int0_b[own_b] = group_sum(int0_a, own_a, INT0_A)
    gather(int0_b, own_b, INT0_B, peers_b)

    arrived(atom_a, ATOM_A, GROUP - 1)
    arrived(atom_b, ATOM_B, GROUP - 1)
    arrived(slot_a, SLOT_A, GROUP - 1)
    half = iota((1, LANES), 1) < batches
    atoms_b = [jnp.where(half, atom_b[2 * q], atom_b[2 * q + 1]).astype(F32) for q in range(GROUP // 2)]
    slot_base = me["x"] * (GROUP * batches)

    def relate(s, nothing):
        atoms_a = as_column(atom_a[s].astype(F32))
        slots_a = as_column(slot_a[s].astype(F32))
        at = pl.ds(pl.multiple_of(s * batches, batches), batches)
        for q in range(GROUP // 2):
            cols = pl.ds(q * LANES, LANES)
            same_atom[at, cols] = jnp.where(atoms_a == atoms_b[q], 1.0, 0.0).astype(jnp.bfloat16)
            number = (iota((1, LANES), 1) + (slot_base + q * LANES)).astype(F32)
            same_slot[at, cols] = jnp.where(slots_a == number, 1.0, 0.0).astype(jnp.bfloat16)
        return nothing

    lax.fori_loop(0, GROUP, relate, 0)

    def entry_values(row, count):
        rows = iota((count, LANES), 0)
        lanes = iota((count, LANES), 1)
        total = jnp.sum(jnp.where(rows == lanes, jnp.broadcast_to(row, (count, LANES)), 0.0), axis=1, keepdims=True)
        return jnp.broadcast_to(total, (count, LANES))

    def splat(base, i):
        return jnp.broadcast_to(entries[pl.ds(base + i, 1), :], (8, LANES))

    def left_sides(block_of):
        is_low = iota((ROWS, LANES), 1) < batches
        lows, highs = [], []
        for q in range(GROUP // 2):
            first, second = block_of(2 * q), block_of(2 * q + 1)
            lows.append(jnp.where(is_low, first, pltpu.roll(second, batches, 1)))
            highs.append(jnp.where(is_low, pltpu.roll(first, batches, 1), second))
        pad = jnp.zeros((16 - ROWS, GROUP * batches), F32)
        low = jnp.concatenate(lows, axis=1)
        high = jnp.concatenate(highs, axis=1)
        return three_parts(jnp.concatenate([low, pad, high, pad], axis=0))

    def contributions(parts, matrix, out):
        result = jnp.dot(parts, matrix[...], preferred_element_type=F32)
        result = result[0:32] + result[32:64] + result[64:96]
        is_low = iota((ROWS, LANES), 1) < batches
        for q in range(GROUP // 2):
            cols = slice(q * LANES, (q + 1) * LANES)
            low, high = result[0:ROWS, cols], result[16:16 + ROWS, cols]
            out[2 * q] = jnp.where(is_low, low, pltpu.roll(high, batches, 1))
            out[2 * q + 1] = jnp.where(is_low, pltpu.roll(low, batches, 1), high)

    def scatter(out, buf, key):
        buf[own_b] = out[own_b]
        for peer in peers_b:
            send(out.at[peer.get("c") * 8 + peer.get("z")], buf.at[own_b], key, peer)

    def packed_scale(rows):
        r, c = iota((rows, LANES), 0), iota((rows, LANES), 1)
        high = c >= batches
        k = jnp.where(r < 8, jnp.where(high, r + 8, r), jnp.where(high, r + 12, r + 8))
        k = jnp.where(r == 12, 24, k)
        degree = (
            jnp.where(k >= 1, 1, 0) + jnp.where(k >= 4, 1, 0) + jnp.where(k >= 9, 1, 0) + jnp.where(k >= 16, 1, 0)
        )
        return 1.0 / (1.0 + degree.astype(F32))

    moment_scale = 1.0 / 32.0

    def mixed_density(total, column, final):
        total = total * (packed_scale(ROWS) * (MIX_BETA * moment_scale))
        first = total[0:8]
        rest = jnp.concatenate([total[8:13], jnp.zeros((3, LANES), F32)], axis=0)
        second = jnp.where(sub < 4, rest, pltpu.roll(pltpu.roll(rest, 4, 0), batches, 1))
        last = jnp.broadcast_to(rest[4:5], (8, LANES))

        def eight(q, carry):
            first, second, last = carry
            dense = zero
            for u in range(4):
                cols = (
                    jnp.broadcast_to(first[:, u:u + 1], (8, LANES)),
                    jnp.broadcast_to(first[:, batches + u:batches + u + 1], (8, LANES)),
                    jnp.broadcast_to(second[:, u:u + 1], (8, LANES)),
                )
                col_last = jnp.broadcast_to(last[:, u:u + 1], (8, LANES))
                for h in range(2):
                    r = 2 * u + h
                    off = pl.ds(pl.multiple_of((q * 8 + r) * LANES, LANES), LANES)
                    y = column * (rho[:, off] + MIX_BETA * res[:, off])
                    for kt in range(3):
                        y = y - cols[kt] * basis[kt * 8:kt * 8 + 8, off]
                    y = sublane_total(y) - col_last * jnp.broadcast_to(basis[24:25, off], (8, LANES))
                    dense = jnp.where(sub == r, y, dense)
            at = pl.ds(pl.multiple_of(q * 8, 8), 8)
            den[at, :] = dense
            if not final:
                rnew[at, :] = t[at, :] + cpl[at, :] * jnp.tanh(dense) - dense
            return tuple(pltpu.roll(x, LANES - 4, 1) for x in (first, second, last))

        lax.fori_loop(0, blocks // 8, eight, (first, second, last))

    row = group_sum(int0_b, own_b, INT0_B)
    entries[0:40, :] = entry_values(row, 40)

    def pair(i, j):
        s = (i - j) % 8
        return splat(0, 8 * s + i) if s <= 4 else splat(0, 8 * ((j - i) % 8) + j)

    weights0 = mixing_weights([[pair(i, j) for j in range(i + 1)] for i in range(HIST)])
    column0 = history_column(weights0)

    def mixed_block(values, s):
        total = jnp.broadcast_to(values[0][0:1], (ROWS, LANES)) * hist_a[s, 0]
        for i in range(1, HIST):
            total = total + jnp.broadcast_to(values[i][0:1], (ROWS, LANES)) * hist_a[s, i]
        return total

    arrived(hist_a, HIST_A, GROUP - 1)
    contributions(left_sides(lambda s: mixed_block(weights0, s)), same_atom, send0)
    scatter(send0, pb0_b, PB0_B)
    loads[LD_RHO].wait()
    loads[LD_TARGET].wait()
    loads[LD_COUPLING].wait()
    mixed_density(group_sum(pb0_b, own_b, PB0_B), column0, False)

    where = slot_index[0]
    at_slot = sub == where

    def new_batches(q, carry):
        acc, k01, k2, k3 = carry
        for u in range(4):
            b = q * 4 + u
            offs = [pl.ds(pl.multiple_of((2 * b + h) * LANES, LANES), LANES) for h in range(2)]
            field = []
            for h in range(2):
                fresh = jnp.broadcast_to(rnew[pl.ds(2 * b + h, 1), :], (8, LANES))
                field.append(fresh * jnp.broadcast_to(w[pl.ds(2 * b + h, 1), :], (8, LANES)))
                acc = acc + jnp.where(at_slot, fresh, res[:, offs[h]]) * field[h]
            parts = []
            for kt in range(3):
                rows = slice(kt * 8, kt * 8 + 8)
                product = basis[rows, offs[0]] * field[0] + basis[rows, offs[1]] * field[1]
                parts.append(jnp.sum(product, axis=1, keepdims=True))
            last = basis[24:25, offs[0]] * field[0][0:1] + basis[24:25, offs[1]] * field[1][0:1]
            k01, k2 = place(b, parts, k01, k2)
            k3 = jnp.where(lane[0:1] == b, jnp.sum(last, axis=1, keepdims=True), k3)
        return acc, k01, k2, k3

    acc, k01, k2, k3 = lax.fori_loop(0, batches // 4, new_batches, (zero, zero, zero, zero[0:1]))
    total = jnp.sum(acc, axis=1, keepdims=True)
    row = sublane_total(jnp.where(lane == sub + batches, total, 0.0))[0:1, :]
    put_moments(new_a, (own_a,), k01, k2, jnp.where(half, k3, row))
    gather(new_a, own_a, NEW_A, peers_a)

    def overwrite(q, nothing):
        for u in range(8):
            j = q * 8 + u
            off = pl.ds(pl.multiple_of(j * LANES, LANES), LANES)
            res[:, off] = jnp.where(at_slot, jnp.broadcast_to(rnew[pl.ds(j, 1), :], (8, LANES)), res[:, off])
            rho[:, off] = jnp.where(at_slot, jnp.broadcast_to(den[pl.ds(j, 1), :], (8, LANES)), rho[:, off])
        return nothing

    lax.fori_loop(0, blocks // 8, overwrite, 0)
    arrived(new_a, NEW_A, GROUP - 1)
    row = new_a[0, 12:13]
    for s in range(1, GROUP):
        row = row + new_a[s, 12:13]
    int1_b[own_b] = pltpu.roll(row, batches, 1)
    gather(int1_b, own_b, INT1_B, peers_b)
    row = group_sum(int1_b, own_b, INT1_B)
    entries[40:48, :] = entry_values(row, 8)
    fresh_row = [splat(40, i) for i in range(HIST)]
    weights1 = mixing_weights([
        [jnp.where(where == i, fresh_row[j], jnp.where(where == j, fresh_row[i], pair(i, j))) for j in range(i + 1)]
        for i in range(HIST)
    ])
    column1 = history_column(weights1)

    kept = [jnp.where(where == i, 0.0, weights1[i]) for i in range(HIST)]
    fresh_weight = jnp.where(where == 0, weights1[0], 0.0)
    for i in range(1, HIST):
        fresh_weight = fresh_weight + jnp.where(where == i, weights1[i], 0.0)
    sides = left_sides(
        lambda s: mixed_block(kept, s) + jnp.broadcast_to(fresh_weight[0:1], (ROWS, LANES)) * new_a[s]
    )
    contributions(sides, same_atom, send1)
    scatter(send1, pb1_b, PB1_B)
    contributions(sides, same_slot, send2)
    scatter(send2, mom_b, MOM_B)
    mixed_total = group_sum(pb1_b, own_b, PB1_B)
    owned = group_sum(mom_b, own_b, MOM_B) * moment_scale
    mom_z[me["z"]] = owned
    gather(mom_z, me["z"], MOM_Z, peers_z)
    mixed_density(mixed_total, column1, True)
    store_den = pltpu.make_async_copy(den, den_h, local_sem.at[ST_DEN])
    store_den.start()
    arrived(mom_z, MOM_Z, 7)
    for q in range(4):
        first, second = mom_z[2 * q], mom_z[2 * q + 1]
        cols = slice(q * LANES, (q + 1) * LANES)
        is_low = iota((ROWS, LANES), 1) < batches
        low = jnp.where(is_low, first, pltpu.roll(second, batches, 1))
        high = jnp.where(is_low, pltpu.roll(first, batches, 1), second)
        mom[0:8, cols] = low[0:8]
        mom[8:16, cols] = high[0:8]
        mom[16:20, cols] = low[8:12]
        mom[20:24, cols] = high[8:12]
        mom[24:25, cols] = low[12:13]
    store_mom = pltpu.make_async_copy(mom, mom_h, local_sem.at[ST_MOM])
    store_mom.start()

    for buf, key, count in (
        (int0_a, INT0_A, 15), (int0_b, INT0_B, 15), (atom_a, ATOM_A, 15), (atom_b, ATOM_B, 15),
        (slot_a, SLOT_A, 15), (hist_a, HIST_A, 15), (new_a, NEW_A, 15), (int1_b, INT1_B, 15),
        (pb0_b, PB0_B, 15), (pb1_b, PB1_B, 15), (mom_b, MOM_B, 15), (mom_z, MOM_Z, 7),
    ):
        sent(buf, key, count)
    store_den.wait()
    store_mom.wait()


def local(weights, target, coupling, basis, rho_hist, res_hist, batch_atom, owner_slot, slot_index):
    points = weights.shape[0]
    blocks = points // LANES
    harmonics = basis.shape[0]
    batches = batch_atom.shape[0]
    slots = owner_slot.shape[0]
    dense = lambda x: x.reshape(blocks, LANES)
    hbm = pl.BlockSpec(memory_space=pltpu.HBM)
    smem = pl.BlockSpec(memory_space=pltpu.SMEM)
    small = lambda dtype: pltpu.VMEM((GROUP, 1, LANES), dtype)
    block = lambda count: pltpu.VMEM((count, ROWS, LANES), F32)
    relation = pltpu.VMEM((GROUP * batches, GROUP * batches), jnp.bfloat16)
    density, moments = pl.pallas_call(
        body,
        out_shape=(
            jax.ShapeDtypeStruct((blocks, LANES), F32),
            jax.ShapeDtypeStruct((harmonics, slots // 8), F32),
        ),
        in_specs=[hbm] * 8 + [smem],
        out_specs=(hbm, hbm),
        scratch_shapes=[
            pltpu.VMEM((blocks, LANES), F32),
            pltpu.VMEM((blocks, LANES), F32),
            pltpu.VMEM((blocks, LANES), F32),
            pltpu.VMEM((harmonics, points), F32),
            pltpu.VMEM((HIST, points), F32),
            pltpu.VMEM((HIST, points), F32),
            pltpu.VMEM((HIST, points), F32),
            pltpu.VMEM((1, batches), jnp.int32),
            pltpu.VMEM((slots // LANES, LANES), jnp.int32),
            pltpu.VMEM((blocks, LANES), F32),
            pltpu.VMEM((blocks, LANES), F32),
            pltpu.VMEM((harmonics, slots // 8), F32),
            pltpu.VMEM((48, LANES), F32),
            relation,
            relation,
            small(F32), small(F32), small(F32), small(jnp.int32), small(jnp.int32), small(jnp.int32),
            pltpu.VMEM((GROUP, HIST, ROWS, LANES), F32),
            block(GROUP), block(GROUP), block(GROUP), block(GROUP), block(8),
            block(GROUP), block(GROUP), block(GROUP),
            pltpu.SemaphoreType.DMA((LOCALS,)),
            pltpu.SemaphoreType.DMA((EXCHANGES,)),
            pltpu.SemaphoreType.DMA((EXCHANGES,)),
        ],
        compiler_params=pltpu.CompilerParams(collective_id=0, has_side_effects=True),
    )(
        dense(weights), dense(target), dense(coupling), basis, rho_hist, res_hist,
        batch_atom.reshape(1, batches), owner_slot.reshape(slots // LANES, LANES), slot_index,
    )
    return density.reshape(points), moments


def solution(mesh):
    torus = Mesh(mesh.devices.reshape(tuple(SIZES.values())), AXES)
    points = P(AXES)
    rows = P(None, AXES)
    return jax.shard_map(
        local,
        mesh=torus,
        in_specs=(points, points, points, rows, rows, rows, points, P(), P()),
        out_specs=(points, P(None, ("x", "c"))),
        check_vma=False,
    )
```

```python
import itertools

import jax
import jax.numpy as jnp
from jax import lax
from jax.experimental import pallas as pl
from jax.experimental.pallas import tpu as pltpu
from jax.sharding import Mesh
from jax.sharding import PartitionSpec as P

AXES = ("z", "y", "x", "c")
SIZES = {"z": 8, "y": 4, "x": 4, "c": 2}
HIST = 8
LANES = 128
MESH = pl.DeviceIdType.MESH
F32 = jnp.float32
MIX_BETA = 0.5
RIDGE_SHARE = 0.1
GROUP = 16
ROWS = 13
INT0_A, INT0_B, ATOM_A, ATOM_B, SLOT_A, HIST_0, HIST_1, HIST_2, HIST_3, NEW_A, INT1_B, PB0_B, PB1_B, MOM_B, MOM_Z = range(15)
EXCHANGES = 15
HIST_KEYS = (HIST_0, HIST_1, HIST_2, HIST_3)
LD_RES, LD_W, LD_ATOM, LD_OWNER, LD_BASIS, LD_RHO, LD_TARGET, LD_COUPLING, LD_INDEX = range(9)
LOCALS = 9


def iota(shape, dim):
    return lax.broadcasted_iota(jnp.int32, shape, dim)


def sublane_total(x):
    x = x + pltpu.roll(x, 4, 0)
    x = x + pltpu.roll(x, 2, 0)
    return x + pltpu.roll(x, 1, 0)


def mixing_weights(entry):
    matrix = [[entry[i][j] for j in range(i + 1)] for i in range(HIST)]
    trace = matrix[0][0]
    for i in range(1, HIST):
        trace = trace + matrix[i][i]
    ridge = trace * (RIDGE_SHARE / HIST)
    for i in range(HIST):
        matrix[i][i] = matrix[i][i] + ridge
    forward = [jnp.ones((8, LANES), F32) for _ in range(HIST)]
    pivot = [None] * HIST
    lower = [[None] * HIST for _ in range(HIST)]
    for j in range(HIST):
        pivot[j] = 1.0 / matrix[j][j]
        for i in range(j + 1, HIST):
            ratio = matrix[i][j] * pivot[j]
            for k in range(j + 1, i + 1):
                matrix[i][k] = matrix[i][k] - ratio * matrix[k][j]
            forward[i] = forward[i] - ratio * forward[j]
            lower[i][j] = ratio
    solved = [None] * HIST
    for i in reversed(range(HIST)):
        value = forward[i] * pivot[i]
        for k in range(i + 1, HIST):
            value = value - lower[k][i] * solved[k]
        solved[i] = value
    total = solved[0]
    for i in range(1, HIST):
        total = total + solved[i]
    scale = 1.0 / total
    return [value * scale for value in solved]


def history_column(values):
    sub = iota((8, LANES), 0)
    column = jnp.zeros((8, LANES), F32)
    for i in range(HIST):
        column = jnp.where(sub == i, values[i], column)
    return column


def three_parts(x):
    high = x.astype(jnp.bfloat16)
    rest = x - high.astype(F32)
    middle = rest.astype(jnp.bfloat16)
    low = (rest - middle.astype(F32)).astype(jnp.bfloat16)
    return jnp.concatenate([high, middle, low], axis=0)


def body(
    w_h, t_h, cpl_h, basis_h, rho_h, res_h, atom_h, owner_h, index_h,
    den, mom,
    w, t, cpl, basis, rho, res, wres, atom, owner, rnew, last_rows, slot_index,
    entries, same_atom, same_slot,
    int0_a, int0_b, int1_b, atom_a, atom_b, slot_a,
    hist_0, hist_1, hist_2, hist_3, new_a, pb0_b, pb1_b, mom_b, mom_z, send0, send1, send2,
    local_sem, send_sem, recv_sem,
):
    me = {name: lax.axis_index(name) for name in AXES}
    own_a = me["y"] * 4 + me["x"]
    hist_a = (hist_0, hist_1, hist_2, hist_3)
    own_b = me["c"] * 8 + me["z"]
    blocks = w.shape[0]

    loads = {}
    for key, src, dst in (
        (LD_RES, res_h, res), (LD_W, w_h, w), (LD_ATOM, atom_h, atom), (LD_OWNER, owner_h, owner),
        (LD_BASIS, basis_h, basis), (LD_RHO, rho_h, rho), (LD_TARGET, t_h, t), (LD_COUPLING, cpl_h, cpl),
        (LD_INDEX, index_h, slot_index),
    ):
        loads[key] = pltpu.make_async_copy(src, dst, local_sem.at[key])
        loads[key].start()

    def peers(*names):
        steps = [s for s in itertools.product(*(range(SIZES[name]) for name in names)) if any(s)]
        hops = lambda s: sum(min(d, SIZES[name] - d) for d, name in zip(s, names))
        steps.sort(key=hops, reverse=True)
        return [{name: lax.rem(me[name] + d, SIZES[name]) for d, name in zip(s, names)} for s in steps]

    peers_a, peers_b, peers_z = peers("y", "x"), peers("z", "c"), peers("z")

    barrier = pltpu.get_barrier_semaphore()
    for peer in peers_a + peers_b:
        pl.semaphore_signal(barrier, inc=1, device_id=peer, device_id_type=MESH)

    def send(src, dst, key, peer):
        pltpu.make_async_remote_copy(
            src_ref=src, dst_ref=dst, send_sem=send_sem.at[key], recv_sem=recv_sem.at[key],
            device_id=peer, device_id_type=MESH,
        ).start()

    def gather(buf, own, key, peers):
        for peer in peers:
            send(buf.at[own], buf.at[own], key, peer)

    def arrived(buf, key, count):
        view = buf.at[pl.ds(0, count)]
        pltpu.make_async_copy(view, view, recv_sem.at[key]).wait()

    def sent(buf, key, count):
        view = buf.at[pl.ds(0, count)]
        pltpu.make_async_copy(view, view, send_sem.at[key]).wait()

    sub = iota((8, LANES), 0)
    lane = iota((8, LANES), 1)

    loads[LD_RES].wait()
    loads[LD_W].wait()

    def products(q, accs):
        accs = list(accs)
        for u in range(8):
            off = pl.multiple_of((q * 8 + u) * LANES, LANES)
            r = res[:, pl.ds(off, LANES)]
            rw = r * jnp.broadcast_to(w[pl.ds(q * 8 + u, 1), :], (8, LANES))
            wres[:, pl.ds(off, LANES)] = rw
            accs[0] = accs[0] + rw * r
            for s in range(1, 5):
                accs[s] = accs[s] + rw * pltpu.roll(r, s, 0)
        return tuple(accs)

    zero = jnp.zeros((8, LANES), F32)
    accs = lax.fori_loop(0, blocks // 8, products, (zero,) * 5)
    placed = zero
    for s in range(5):
        total = jnp.sum(accs[s], axis=1, keepdims=True)
        placed = jnp.where(lane == 8 * s + sub, total, placed)
    int0_a[own_a] = sublane_total(placed)[0:1, :]

    batches = 64
    loads[LD_BASIS].wait()

    def place(b, parts, k01, k2):
        k01 = jnp.where(lane == b, parts[0], k01)
        k01 = jnp.where(lane == b + batches, parts[1], k01)
        return k01, jnp.where(lane == b + jnp.where(sub >= 4, batches, 0), parts[2], k2)

    def batch_spans(b):
        return [pl.ds(pl.multiple_of((2 * b + h) * LANES, LANES), LANES) for h in range(2)]

    def chunk_moments(chunk):
        def one(b, carry):
            carry = list(carry)
            offs = batch_spans(b)
            tiles = [[basis[kt * 8:kt * 8 + 8, off] for off in offs] for kt in range(3)]
            for n in range(2):
                i = 2 * chunk + n
                field = [jnp.broadcast_to(wres[i:i + 1, off], (8, LANES)) for off in offs]
                parts = [
                    jnp.sum(tiles[kt][0] * field[0] + tiles[kt][1] * field[1], axis=1, keepdims=True)
                    for kt in range(3)
                ]
                carry[2 * n], carry[2 * n + 1] = place(b, parts, carry[2 * n], carry[2 * n + 1])
            return tuple(carry)

        return lax.fori_loop(0, batches, one, (zero,) * 4, unroll=8)

    def last_harmonic(b, placed):
        offs = batch_spans(b)
        last = [wres[:, off] * jnp.broadcast_to(basis[24:25, off], (8, LANES)) for off in offs]
        return jnp.where(lane == b, jnp.sum(last[0] + last[1], axis=1, keepdims=True), placed)

    def put_moments(buf, at, k01, k2, k3):
        buf[(*at, slice(0, 8))] = k01
        buf[(*at, slice(8, 12))] = (k2 + pltpu.roll(k2, 4, 0))[0:4]
        buf[(*at, slice(12, 13))] = k3

    last_moments = lax.fori_loop(0, batches, last_harmonic, zero, unroll=8)

    def fill_chunk(chunk):
        found = chunk_moments(chunk)
        for n in range(2):
            i = 2 * chunk + n
            put_moments(hist_a[chunk], (own_a, n), found[2 * n], found[2 * n + 1], last_moments[i:i + 1])

    loads[LD_ATOM].wait()
    atom_wide = jnp.concatenate([atom[...], atom[...]], axis=1)
    atom_a[own_a] = atom_wide
    atom_b[own_b] = atom_wide
    fill_chunk(0)

    pl.semaphore_wait(barrier, len(peers_a) + len(peers_b))
    gather(int0_a, own_a, INT0_A, peers_a)
    gather(atom_a, own_a, ATOM_A, peers_a)
    gather(atom_b, own_b, ATOM_B, peers_b)
    gather(hist_a[0], own_a, HIST_0, peers_a)
    for chunk in range(1, 4):
        fill_chunk(chunk)
        gather(hist_a[chunk], own_a, HIST_KEYS[chunk], peers_a)

    loads[LD_OWNER].wait()
    wide_sub = iota((batches, LANES), 0)
    wide_lane = iota((batches, LANES), 1)
    own_lane = wide_lane == wide_sub

    def as_column(row):
        return jnp.sum(jnp.where(own_lane, jnp.broadcast_to(row, (batches, LANES)), 0.0), axis=1, keepdims=True)

    atom_col = as_column(atom_wide.astype(F32))

    def look_up(j, found):
        owners = jnp.broadcast_to(owner[pl.ds(j, 1), :].astype(F32), (batches, LANES))
        number = (wide_lane + j * LANES).astype(F32)
        return found + jnp.where(number == atom_col, owners, 0.0)

    found = lax.fori_loop(0, owner.shape[0], look_up, jnp.zeros((batches, LANES), F32))
    slot_col = jnp.sum(found, axis=1, keepdims=True)
    slot_a[own_a] = jnp.sum(jnp.where(own_lane, slot_col, 0.0), axis=0, keepdims=True).astype(jnp.int32)
    gather(slot_a, own_a, SLOT_A, peers_a)

    def group_sum(buf, own, key):
        arrived(buf, key, GROUP - 1)
        total = buf[0]
        for i in range(1, GROUP):
            total = total + buf[i]
        return total

    int0_b[own_b] = group_sum(int0_a, own_a, INT0_A)
    gather(int0_b, own_b, INT0_B, peers_b)

    arrived(atom_a, ATOM_A, GROUP - 1)
    arrived(atom_b, ATOM_B, GROUP - 1)
    half = iota((1, LANES), 1) < batches
    atoms_b = [jnp.where(half, atom_b[2 * q], atom_b[2 * q + 1]).astype(F32) for q in range(GROUP // 2)]

    def relate_atoms(s, nothing):
        atoms_a = as_column(atom_a[s].astype(F32))
        at = pl.ds(pl.multiple_of(s * batches, batches), batches)
        for q in range(GROUP // 2):
            cols = pl.ds(q * LANES, LANES)
            same_atom[at, cols] = jnp.where(atoms_a == atoms_b[q], 1.0, 0.0).astype(jnp.bfloat16)
        return nothing

    lax.fori_loop(0, GROUP, relate_atoms, 0)

    def last_row(q, nothing):
        for u in range(8):
            j = q * 8 + u
            last_rows[pl.ds(j, 1), :] = basis[24:25, pl.ds(pl.multiple_of(j * LANES, LANES), LANES)]
        return nothing

    lax.fori_loop(0, blocks // 8, last_row, 0)

    def entry_values(row, count):
        rows = iota((count, LANES), 0)
        lanes = iota((count, LANES), 1)
        total = jnp.sum(jnp.where(rows == lanes, jnp.broadcast_to(row, (count, LANES)), 0.0), axis=1, keepdims=True)
        return jnp.broadcast_to(total, (count, LANES))

    def splat(base, i):
        return jnp.broadcast_to(entries[pl.ds(base + i, 1), :], (8, LANES))

    def left_sides(block_of):
        is_low = iota((ROWS, LANES), 1) < batches
        lows, highs = [], []
        for q in range(GROUP // 2):
            first, second = block_of(2 * q), block_of(2 * q + 1)
            lows.append(jnp.where(is_low, first, pltpu.roll(second, batches, 1)))
            highs.append(jnp.where(is_low, pltpu.roll(first, batches, 1), second))
        pad = jnp.zeros((16 - ROWS, GROUP * batches), F32)
        low = jnp.concatenate(lows, axis=1)
        high = jnp.concatenate(highs, axis=1)
        return three_parts(jnp.concatenate([low, pad, high, pad], axis=0))

    def contributions(parts, matrix, out):
        result = jnp.dot(parts, matrix[...], preferred_element_type=F32)
        result = result[0:32] + result[32:64] + result[64:96]
        is_low = iota((ROWS, LANES), 1) < batches
        for q in range(GROUP // 2):
            cols = slice(q * LANES, (q + 1) * LANES)
            low, high = result[0:ROWS, cols], result[16:16 + ROWS, cols]
            out[2 * q] = jnp.where(is_low, low, pltpu.roll(high, batches, 1))
            out[2 * q + 1] = jnp.where(is_low, pltpu.roll(low, batches, 1), high)

    def scatter(out, buf, key):
        buf[own_b] = out[own_b]
        for peer in peers_b:
            send(out.at[peer.get("c") * 8 + peer.get("z")], buf.at[own_b], key, peer)

    def packed_scale(rows):
        r, c = iota((rows, LANES), 0), iota((rows, LANES), 1)
        high = c >= batches
        k = jnp.where(r < 8, jnp.where(high, r + 8, r), jnp.where(high, r + 12, r + 8))
        k = jnp.where(r == 12, 24, k)
        degree = (
            jnp.where(k >= 1, 1, 0) + jnp.where(k >= 4, 1, 0) + jnp.where(k >= 9, 1, 0) + jnp.where(k >= 16, 1, 0)
        )
        return 1.0 / (1.0 + degree.astype(F32))

    moment_scale = 1.0 / 32.0

    def folded(tiles):
        for bit in (4, 2, 1):
            low = (sub & bit) == 0
            count = len(tiles) // 2
            merged = []
            for first, second in zip(tiles[:count], tiles[count:]):
                given = jnp.where(low, second, first)
                if bit == 4:
                    given = pltpu.roll(given, 4, 0)
                else:
                    given = jnp.where(low, pltpu.roll(given, 8 - bit, 0), pltpu.roll(given, bit, 0))
                merged.append(jnp.where(low, first, second) + given)
            tiles = merged
        return tiles[0]

    def mix_history(column):
        def eight(q, nothing):
            offs = [pl.ds(pl.multiple_of((q * 8 + r) * LANES, LANES), LANES) for r in range(8)]
            den[pl.ds(pl.multiple_of(q * 8, 8), 8), :] = folded(
                [column * (rho[:, off] + MIX_BETA * res[:, off]) for off in offs]
            )
            return nothing

        lax.fori_loop(0, blocks // 8, eight, 0, unroll=2)

    def correct_density(total, final):
        total = total * (packed_scale(ROWS) * (MIX_BETA * moment_scale))
        first = total[0:8]
        rest = jnp.concatenate([total[8:13], jnp.zeros((3, LANES), F32)], axis=0)
        second = jnp.where(sub < 4, rest, pltpu.roll(pltpu.roll(rest, 4, 0), batches, 1))
        last = jnp.broadcast_to(rest[4:5], (8, LANES))

        def wide(x, b):
            return jnp.broadcast_to(x[:, b:b + 1], (8, LANES))

        for q in range(blocks // 8):
            tiles = []
            last_col = None
            for u in range(4):
                b = 4 * q + u
                cols = (wide(first, b), wide(first, batches + b), wide(second, b))
                col = wide(last, b)
                last_col = col if u == 0 else jnp.where(sub >= 2 * u, col, last_col)
                for h in range(2):
                    off = slice((2 * b + h) * LANES, (2 * b + h + 1) * LANES)
                    tiles.append(
                        cols[0] * basis[0:8, off] + cols[1] * basis[8:16, off] + cols[2] * basis[16:24, off]
                    )
            at = slice(q * 8, q * 8 + 8)
            dense = den[at, :] - folded(tiles) - last_col * last_rows[at, :]
            den[at, :] = dense
            if not final:
                rnew[at, :] = t[at, :] + cpl[at, :] * jnp.tanh(dense) - dense

    row = group_sum(int0_b, own_b, INT0_B)
    entries[0:40, :] = entry_values(row, 40)

    def pair(i, j):
        s = (i - j) % 8
        return splat(0, 8 * s + i) if s <= 4 else splat(0, 8 * ((j - i) % 8) + j)

    weights0 = mixing_weights([[pair(i, j) for j in range(i + 1)] for i in range(HIST)])
    column0 = history_column(weights0)

    def mixed_block(values, s):
        total = jnp.broadcast_to(values[0][0:1], (ROWS, LANES)) * hist_a[0][s, 0]
        for i in range(1, HIST):
            total = total + jnp.broadcast_to(values[i][0:1], (ROWS, LANES)) * hist_a[i // 2][s, i % 2]
        return total

    for chunk in range(4):
        arrived(hist_a[chunk], HIST_KEYS[chunk], GROUP - 1)
    contributions(left_sides(lambda s: mixed_block(weights0, s)), same_atom, send0)
    scatter(send0, pb0_b, PB0_B)
    loads[LD_RHO].wait()
    loads[LD_TARGET].wait()
    loads[LD_COUPLING].wait()
    loads[LD_INDEX].wait()
    mix_history(column0)
    correct_density(group_sum(pb0_b, own_b, PB0_B), False)

    where = slot_index[0]
    at_slot = sub == where

    def new_batches(q, carry):
        acc, k01, k2, k3 = carry
        for u in range(4):
            b = q * 4 + u
            offs = [pl.ds(pl.multiple_of((2 * b + h) * LANES, LANES), LANES) for h in range(2)]
            field = []
            for h in range(2):
                fresh = jnp.broadcast_to(rnew[pl.ds(2 * b + h, 1), :], (8, LANES))
                field.append(fresh * jnp.broadcast_to(w[pl.ds(2 * b + h, 1), :], (8, LANES)))
                acc = acc + jnp.where(at_slot, fresh, res[:, offs[h]]) * field[h]
            parts = []
            for kt in range(3):
                rows = slice(kt * 8, kt * 8 + 8)
                product = basis[rows, offs[0]] * field[0] + basis[rows, offs[1]] * field[1]
                parts.append(jnp.sum(product, axis=1, keepdims=True))
            last = basis[24:25, offs[0]] * field[0][0:1] + basis[24:25, offs[1]] * field[1][0:1]
            k01, k2 = place(b, parts, k01, k2)
            k3 = jnp.where(lane[0:1] == b, jnp.sum(last, axis=1, keepdims=True), k3)
        return acc, k01, k2, k3

    acc, k01, k2, k3 = lax.fori_loop(0, batches // 4, new_batches, (zero, zero, zero, zero[0:1]), unroll=4)
    total = jnp.sum(acc, axis=1, keepdims=True)
    row = sublane_total(jnp.where(lane == sub + batches, total, 0.0))[0:1, :]
    put_moments(new_a, (own_a,), k01, k2, jnp.where(half, k3, row))
    gather(new_a, own_a, NEW_A, peers_a)

    def overwrite(q, nothing):
        for u in range(8):
            j = q * 8 + u
            off = pl.ds(pl.multiple_of(j * LANES, LANES), LANES)
            res[:, off] = jnp.where(at_slot, jnp.broadcast_to(rnew[pl.ds(j, 1), :], (8, LANES)), res[:, off])
            rho[:, off] = jnp.where(at_slot, jnp.broadcast_to(den[pl.ds(j, 1), :], (8, LANES)), rho[:, off])
        return nothing

    lax.fori_loop(0, blocks // 8, overwrite, 0)

    arrived(slot_a, SLOT_A, GROUP - 1)
    slot_base = me["x"] * (GROUP * batches)

    def relate_slots(s, nothing):
        slots_a = as_column(slot_a[s].astype(F32))
        at = pl.ds(pl.multiple_of(s * batches, batches), batches)
        for q in range(GROUP // 2):
            number = (iota((1, LANES), 1) + (slot_base + q * LANES)).astype(F32)
            same_slot[at, pl.ds(q * LANES, LANES)] = jnp.where(slots_a == number, 1.0, 0.0).astype(jnp.bfloat16)
        return nothing

    lax.fori_loop(0, GROUP, relate_slots, 0)
    arrived(new_a, NEW_A, GROUP - 1)
    row = new_a[0, 12:13]
    for s in range(1, GROUP):
        row = row + new_a[s, 12:13]
    int1_b[own_b] = pltpu.roll(row, batches, 1)
    gather(int1_b, own_b, INT1_B, peers_b)
    row = group_sum(int1_b, own_b, INT1_B)
    entries[40:48, :] = entry_values(row, 8)
    fresh_row = [splat(40, i) for i in range(HIST)]
    weights1 = mixing_weights([
        [jnp.where(where == i, fresh_row[j], jnp.where(where == j, fresh_row[i], pair(i, j))) for j in range(i + 1)]
        for i in range(HIST)
    ])
    column1 = history_column(weights1)

    kept = [jnp.where(where == i, 0.0, weights1[i]) for i in range(HIST)]
    fresh_weight = jnp.where(where == 0, weights1[0], 0.0)
    for i in range(1, HIST):
        fresh_weight = fresh_weight + jnp.where(where == i, weights1[i], 0.0)
    sides = left_sides(
        lambda s: mixed_block(kept, s) + jnp.broadcast_to(fresh_weight[0:1], (ROWS, LANES)) * new_a[s]
    )
    contributions(sides, same_atom, send1)
    scatter(send1, pb1_b, PB1_B)
    contributions(sides, same_slot, send2)
    scatter(send2, mom_b, MOM_B)
    mix_history(column1)
    mixed_total = group_sum(pb1_b, own_b, PB1_B)
    owned = group_sum(mom_b, own_b, MOM_B) * moment_scale
    mom_z[me["z"]] = owned
    gather(mom_z, me["z"], MOM_Z, peers_z)
    correct_density(mixed_total, True)
    arrived(mom_z, MOM_Z, 7)
    for q in range(4):
        first, second = mom_z[2 * q], mom_z[2 * q + 1]
        cols = slice(q * LANES, (q + 1) * LANES)
        is_low = iota((ROWS, LANES), 1) < batches
        low = jnp.where(is_low, first, pltpu.roll(second, batches, 1))
        high = jnp.where(is_low, pltpu.roll(first, batches, 1), second)
        mom[0:8, cols] = low[0:8]
        mom[8:16, cols] = high[0:8]
        mom[16:20, cols] = low[8:12]
        mom[20:24, cols] = high[8:12]
        mom[24:25, cols] = low[12:13]

    for buf, key, count in (
        (int0_a, INT0_A, 15), (int0_b, INT0_B, 15), (atom_a, ATOM_A, 15), (atom_b, ATOM_B, 15),
        (slot_a, SLOT_A, 15), (hist_0, HIST_0, 15), (hist_1, HIST_1, 15), (hist_2, HIST_2, 15), (hist_3, HIST_3, 15),
        (new_a, NEW_A, 15), (int1_b, INT1_B, 15),
        (pb0_b, PB0_B, 15), (pb1_b, PB1_B, 15), (mom_b, MOM_B, 15), (mom_z, MOM_Z, 7),
    ):
        sent(buf, key, count)


def hand_over(den, mom, den_h, mom_h, sem):
    copies = [pltpu.make_async_copy(den, den_h, sem.at[0]), pltpu.make_async_copy(mom, mom_h, sem.at[1])]
    for copy in copies:
        copy.start()
    for copy in copies:
        copy.wait()


def local(weights, target, coupling, basis, rho_hist, res_hist, batch_atom, owner_slot, slot_index):
    points = weights.shape[0]
    blocks = points // LANES
    harmonics = basis.shape[0]
    batches = batch_atom.shape[0]
    slots = owner_slot.shape[0]
    dense = lambda x: x.reshape(blocks, LANES)
    operands = (
        dense(weights), dense(target), dense(coupling), basis, rho_hist, res_hist,
        batch_atom.reshape(1, batches), owner_slot.reshape(slots // LANES, LANES), slot_index,
    )
    hbm = pl.BlockSpec(memory_space=pltpu.HBM)
    vmem = pl.BlockSpec(memory_space=pltpu.VMEM)
    small = lambda dtype: pltpu.VMEM((GROUP, 1, LANES), dtype)
    pair_block = lambda: pltpu.VMEM((GROUP, 2, ROWS, LANES), F32)
    block = lambda count: pltpu.VMEM((count, ROWS, LANES), F32)
    relation = pltpu.VMEM((GROUP * batches, GROUP * batches), jnp.bfloat16)
    density, moments = pl.pallas_call(
        body,
        out_shape=(
            jax.ShapeDtypeStruct((blocks, LANES), F32),
            jax.ShapeDtypeStruct((harmonics, slots // 8), F32),
        ),
        in_specs=[hbm] * len(operands),
        out_specs=(vmem, vmem),
        scratch_shapes=[
            pltpu.VMEM((blocks, LANES), F32),
            pltpu.VMEM((blocks, LANES), F32),
            pltpu.VMEM((blocks, LANES), F32),
            pltpu.VMEM((harmonics, points), F32),
            pltpu.VMEM((HIST, points), F32),
            pltpu.VMEM((HIST, points), F32),
            pltpu.VMEM((HIST, points), F32),
            pltpu.VMEM((1, batches), jnp.int32),
            pltpu.VMEM((slots // LANES, LANES), jnp.int32),
            pltpu.VMEM((blocks, LANES), F32),
            pltpu.VMEM((blocks, LANES), F32),
            pltpu.SMEM((2,), jnp.int32),
            pltpu.VMEM((48, LANES), F32),
            relation,
            relation,
            small(F32), small(F32), small(F32), small(jnp.int32), small(jnp.int32), small(jnp.int32),
            pair_block(), pair_block(), pair_block(), pair_block(),
            block(GROUP), block(GROUP), block(GROUP), block(GROUP), block(8),
            block(GROUP), block(GROUP), block(GROUP),
            pltpu.SemaphoreType.DMA((LOCALS,)),
            pltpu.SemaphoreType.DMA((EXCHANGES,)),
            pltpu.SemaphoreType.DMA((EXCHANGES,)),
        ],
        compiler_params=pltpu.CompilerParams(collective_id=0, has_side_effects=True, vmem_limit_bytes=24 << 20),
    )(
        *(pltpu.with_memory_space_constraint(x, pltpu.HBM) for x in operands)
    )
    density, moments = pl.pallas_call(
        hand_over,
        out_shape=(
            jax.ShapeDtypeStruct((blocks, LANES), F32),
            jax.ShapeDtypeStruct((harmonics, slots // 8), F32),
        ),
        in_specs=[vmem, vmem],
        out_specs=(hbm, hbm),
        scratch_shapes=[pltpu.SemaphoreType.DMA((2,))],
        compiler_params=pltpu.CompilerParams(vmem_limit_bytes=1 << 20),
    )(density, moments)
    return density.reshape(points), moments


def solution(mesh):
    torus = Mesh(mesh.devices.reshape(tuple(SIZES.values())), AXES)
    points = P(AXES)
    rows = P(None, AXES)
    return jax.shard_map(
        local,
        mesh=torus,
        in_specs=(points, points, points, rows, rows, rows, points, P(), P()),
        out_specs=(points, P(None, ("x", "c"))),
        check_vma=False,
    )
```

```python
import itertools

import jax
import jax.numpy as jnp
from jax import lax
from jax.experimental import pallas as pl
from jax.experimental.pallas import tpu as pltpu
from jax.sharding import Mesh
from jax.sharding import PartitionSpec as P

AXES = ("z", "y", "x", "c")
SIZES = {"z": 8, "y": 4, "x": 4, "c": 2}
HIST = 8
LANES = 128
MESH = pl.DeviceIdType.MESH
F32 = jnp.float32
MIX_BETA = 0.5
RIDGE_SHARE = 0.1
GROUP = 16
ROWS = 13
INT0_A, INT0_B, ATOM_A, ATOM_B, SLOT_A, HIST_0, HIST_1, HIST_2, HIST_3, LAST_A, NEW_A, INT1_B, PB0_B, PB1_B, OLD_B, FRESH_B, MOM_ZY = range(17)
EXCHANGES = 17
HIST_KEYS = (HIST_0, HIST_1, HIST_2, HIST_3)
LD_RES, LD_W, LD_ATOM, LD_OWNER, LD_BASIS, LD_RHO, LD_TARGET, LD_COUPLING, LD_INDEX = range(9)
LOCALS = 9


def iota(shape, dim):
    return lax.broadcasted_iota(jnp.int32, shape, dim)


def sublane_total(x):
    x = x + pltpu.roll(x, 4, 0)
    x = x + pltpu.roll(x, 2, 0)
    return x + pltpu.roll(x, 1, 0)


def mixing_weights(entry):
    matrix = [[entry[i][j] for j in range(i + 1)] for i in range(HIST)]
    trace = matrix[0][0]
    for i in range(1, HIST):
        trace = trace + matrix[i][i]
    ridge = trace * (RIDGE_SHARE / HIST)
    for i in range(HIST):
        matrix[i][i] = matrix[i][i] + ridge
    forward = [jnp.ones((8, LANES), F32) for _ in range(HIST)]
    pivot = [None] * HIST
    lower = [[None] * HIST for _ in range(HIST)]
    for j in range(HIST):
        pivot[j] = 1.0 / matrix[j][j]
        for i in range(j + 1, HIST):
            ratio = matrix[i][j] * pivot[j]
            for k in range(j + 1, i + 1):
                matrix[i][k] = matrix[i][k] - ratio * matrix[k][j]
            forward[i] = forward[i] - ratio * forward[j]
            lower[i][j] = ratio
    solved = [None] * HIST
    for i in reversed(range(HIST)):
        value = forward[i] * pivot[i]
        for k in range(i + 1, HIST):
            value = value - lower[k][i] * solved[k]
        solved[i] = value
    total = solved[0]
    for i in range(1, HIST):
        total = total + solved[i]
    scale = 1.0 / total
    return [value * scale for value in solved]


def history_column(values):
    sub = iota((8, LANES), 0)
    column = jnp.zeros((8, LANES), F32)
    for i in range(HIST):
        column = jnp.where(sub == i, values[i], column)
    return column


def three_parts(x):
    high = x.astype(jnp.bfloat16)
    rest = x - high.astype(F32)
    middle = rest.astype(jnp.bfloat16)
    low = (rest - middle.astype(F32)).astype(jnp.bfloat16)
    return jnp.concatenate([high, middle, low], axis=0)


def body(
    w_h, t_h, cpl_h, basis_h, rho_h, res_h, atom_h, owner_h, index_h,
    den, mom,
    w, t, cpl, basis, rho, res, wres, atom, owner, rnew, last_rows, slot_index,
    entries, same_atom, owned_slot, sides8,
    int0_a, int0_b, int1_b, atom_a, atom_b, slot_a,
    hist_0, hist_1, hist_2, hist_3, last_a, new_a, pb0_b, pb1_b, old_b, fresh_b, mom_zy, send0, send1, send_old, send_fresh,
    local_sem, send_sem, recv_sem,
):
    me = {name: lax.axis_index(name) for name in AXES}
    own_a = me["y"] * 4 + me["x"]
    hist_a = (hist_0, hist_1, hist_2, hist_3)
    own_b = me["c"] * 8 + me["z"]
    blocks = w.shape[0]

    loads = {}
    for key, src, dst in (
        (LD_RES, res_h, res), (LD_W, w_h, w), (LD_ATOM, atom_h, atom), (LD_OWNER, owner_h, owner),
        (LD_BASIS, basis_h, basis), (LD_RHO, rho_h, rho), (LD_TARGET, t_h, t), (LD_COUPLING, cpl_h, cpl),
        (LD_INDEX, index_h, slot_index),
    ):
        loads[key] = pltpu.make_async_copy(src, dst, local_sem.at[key])
        loads[key].start()

    def peers(*names):
        steps = [s for s in itertools.product(*(range(SIZES[name]) for name in names)) if any(s)]
        hops = lambda s: sum(min(d, SIZES[name] - d) for d, name in zip(s, names))
        steps.sort(key=hops, reverse=True)
        return [{name: lax.rem(me[name] + d, SIZES[name]) for d, name in zip(s, names)} for s in steps]

    peers_a, peers_b, peers_zy = peers("y", "x"), peers("z", "c"), peers("z", "y")

    barrier = pltpu.get_barrier_semaphore()
    for peer in peers_a + peers_b:
        pl.semaphore_signal(barrier, inc=1, device_id=peer, device_id_type=MESH)

    def send(src, dst, key, peer):
        pltpu.make_async_remote_copy(
            src_ref=src, dst_ref=dst, send_sem=send_sem.at[key], recv_sem=recv_sem.at[key],
            device_id=peer, device_id_type=MESH,
        ).start()

    def gather(buf, own, key, peers):
        for peer in peers:
            send(buf.at[own], buf.at[own], key, peer)

    def arrived(buf, key, count):
        view = buf.at[pl.ds(0, count)]
        pltpu.make_async_copy(view, view, recv_sem.at[key]).wait()

    def sent(buf, key, count):
        view = buf.at[pl.ds(0, count)]
        pltpu.make_async_copy(view, view, send_sem.at[key]).wait()

    sub = iota((8, LANES), 0)
    lane = iota((8, LANES), 1)

    loads[LD_RES].wait()
    loads[LD_W].wait()

    def products(q, accs):
        accs = list(accs)
        for u in range(8):
            off = pl.multiple_of((q * 8 + u) * LANES, LANES)
            r = res[:, pl.ds(off, LANES)]
            rw = r * jnp.broadcast_to(w[pl.ds(q * 8 + u, 1), :], (8, LANES))
            wres[:, pl.ds(off, LANES)] = rw
            accs[0] = accs[0] + rw * r
            for s in range(1, 5):
                accs[s] = accs[s] + rw * pltpu.roll(r, s, 0)
        return tuple(accs)

    zero = jnp.zeros((8, LANES), F32)
    accs = lax.fori_loop(0, blocks // 8, products, (zero,) * 5)
    placed = zero
    for s in range(5):
        total = jnp.sum(accs[s], axis=1, keepdims=True)
        placed = jnp.where(lane == 8 * s + sub, total, placed)
    int0_a[own_a] = sublane_total(placed)[0:1, :]

    batches = 64
    loads[LD_BASIS].wait()

    def place(b, parts, k01, k2):
        k01 = jnp.where(lane == b, parts[0], k01)
        k01 = jnp.where(lane == b + batches, parts[1], k01)
        return k01, jnp.where(lane == b + jnp.where(sub >= 4, batches, 0), parts[2], k2)

    def batch_spans(b):
        return [pl.ds(pl.multiple_of((2 * b + h) * LANES, LANES), LANES) for h in range(2)]

    def chunk_moments(chunk):
        def one(b, carry):
            carry = list(carry)
            offs = batch_spans(b)
            tiles = [[basis[kt * 8:kt * 8 + 8, off] for off in offs] for kt in range(3)]
            for n in range(2):
                i = 2 * chunk + n
                field = [jnp.broadcast_to(wres[i:i + 1, off], (8, LANES)) for off in offs]
                parts = [
                    jnp.sum(tiles[kt][0] * field[0] + tiles[kt][1] * field[1], axis=1, keepdims=True)
                    for kt in range(3)
                ]
                carry[2 * n], carry[2 * n + 1] = place(b, parts, carry[2 * n], carry[2 * n + 1])
            return tuple(carry)

        return lax.fori_loop(0, batches, one, (zero,) * 4, unroll=8)

    def last_harmonic(b, placed):
        offs = batch_spans(b)
        last = [wres[:, off] * jnp.broadcast_to(basis[24:25, off], (8, LANES)) for off in offs]
        return jnp.where(lane == b, jnp.sum(last[0] + last[1], axis=1, keepdims=True), placed)

    def put_moments(buf, at, k01, k2):
        buf[(*at, slice(0, 8))] = k01
        buf[(*at, slice(8, 12))] = (k2 + pltpu.roll(k2, 4, 0))[0:4]

    def fill_chunk(chunk):
        found = chunk_moments(chunk)
        for n in range(2):
            put_moments(hist_a[chunk], (own_a, n), found[2 * n], found[2 * n + 1])

    loads[LD_ATOM].wait()
    atom_wide = jnp.concatenate([atom[...], atom[...]], axis=1)
    atom_a[own_a] = atom_wide
    atom_b[own_b] = atom_wide
    fill_chunk(0)

    pl.semaphore_wait(barrier, len(peers_a) + len(peers_b))
    gather(int0_a, own_a, INT0_A, peers_a)
    gather(atom_a, own_a, ATOM_A, peers_a)
    gather(atom_b, own_b, ATOM_B, peers_b)
    gather(hist_a[0], own_a, HIST_0, peers_a)
    for chunk in range(1, 4):
        fill_chunk(chunk)
        gather(hist_a[chunk], own_a, HIST_KEYS[chunk], peers_a)
    last_a[own_a] = lax.fori_loop(0, batches, last_harmonic, zero, unroll=8)
    gather(last_a, own_a, LAST_A, peers_a)

    loads[LD_OWNER].wait()
    wide_sub = iota((batches, LANES), 0)
    wide_lane = iota((batches, LANES), 1)
    own_lane = wide_lane == wide_sub

    def as_column(row):
        return jnp.sum(jnp.where(own_lane, jnp.broadcast_to(row, (batches, LANES)), 0.0), axis=1, keepdims=True)

    atom_col = as_column(atom_wide.astype(F32))

    def look_up(j, found):
        owners = jnp.broadcast_to(owner[pl.ds(j, 1), :].astype(F32), (batches, LANES))
        number = (wide_lane + j * LANES).astype(F32)
        return found + jnp.where(number == atom_col, owners, 0.0)

    found = lax.fori_loop(0, owner.shape[0], look_up, jnp.zeros((batches, LANES), F32))
    slot_col = jnp.sum(found, axis=1, keepdims=True)
    slot_a[own_a] = jnp.sum(jnp.where(own_lane, slot_col, 0.0), axis=0, keepdims=True).astype(jnp.int32)
    gather(slot_a, own_a, SLOT_A, peers_a)

    def group_sum(buf, own, key):
        arrived(buf, key, GROUP - 1)
        total = buf[0]
        for i in range(1, GROUP):
            total = total + buf[i]
        return total

    int0_b[own_b] = group_sum(int0_a, own_a, INT0_A)
    gather(int0_b, own_b, INT0_B, peers_b)

    arrived(atom_a, ATOM_A, GROUP - 1)
    arrived(atom_b, ATOM_B, GROUP - 1)
    half = iota((1, LANES), 1) < batches
    atoms_b = [jnp.where(half, atom_b[2 * q], atom_b[2 * q + 1]).astype(F32) for q in range(GROUP // 2)]

    def relate_atoms(s, nothing):
        atoms_a = as_column(atom_a[s].astype(F32))
        at = pl.ds(pl.multiple_of(s * batches, batches), batches)
        for q in range(GROUP // 2):
            cols = pl.ds(q * LANES, LANES)
            same_atom[at, cols] = jnp.where(atoms_a == atoms_b[q], 1.0, 0.0).astype(jnp.bfloat16)
        return nothing

    lax.fori_loop(0, GROUP, relate_atoms, 0)

    def last_row(q, nothing):
        for u in range(8):
            j = q * 8 + u
            last_rows[pl.ds(j, 1), :] = basis[24:25, pl.ds(pl.multiple_of(j * LANES, LANES), LANES)]
        return nothing

    lax.fori_loop(0, blocks // 8, last_row, 0)

    def entry_values(row, count):
        rows = iota((count, LANES), 0)
        lanes = iota((count, LANES), 1)
        total = jnp.sum(jnp.where(rows == lanes, jnp.broadcast_to(row, (count, LANES)), 0.0), axis=1, keepdims=True)
        return jnp.broadcast_to(total, (count, LANES))

    def splat(base, i):
        return jnp.broadcast_to(entries[pl.ds(base + i, 1), :], (8, LANES))

    def left_sides(block_of):
        is_low = iota((ROWS, LANES), 1) < batches
        lows, highs = [], []
        for q in range(GROUP // 2):
            first, second = block_of(2 * q), block_of(2 * q + 1)
            lows.append(jnp.where(is_low, first, pltpu.roll(second, batches, 1)))
            highs.append(jnp.where(is_low, pltpu.roll(first, batches, 1), second))
        pad = jnp.zeros((16 - ROWS, GROUP * batches), F32)
        low = jnp.concatenate(lows, axis=1)
        high = jnp.concatenate(highs, axis=1)
        return three_parts(jnp.concatenate([low, pad, high, pad], axis=0))

    def contributions(parts, matrix, out):
        result = jnp.dot(parts, matrix[...], preferred_element_type=F32)
        result = result[0:32] + result[32:64] + result[64:96]
        is_low = iota((ROWS, LANES), 1) < batches
        for q in range(GROUP // 2):
            cols = slice(q * LANES, (q + 1) * LANES)
            low, high = result[0:ROWS, cols], result[16:16 + ROWS, cols]
            out[2 * q] = jnp.where(is_low, low, pltpu.roll(high, batches, 1))
            out[2 * q + 1] = jnp.where(is_low, pltpu.roll(low, batches, 1), high)

    def scatter(out, buf, key):
        buf[own_b] = out[own_b]
        for peer in peers_b:
            send(out.at[peer.get("c") * 8 + peer.get("z")], buf.at[own_b], key, peer)

    def packed_scale(rows):
        r, c = iota((rows, LANES), 0), iota((rows, LANES), 1)
        high = c >= batches
        k = jnp.where(r < 8, jnp.where(high, r + 8, r), jnp.where(high, r + 12, r + 8))
        k = jnp.where(r == 12, 24, k)
        degree = (
            jnp.where(k >= 1, 1, 0) + jnp.where(k >= 4, 1, 0) + jnp.where(k >= 9, 1, 0) + jnp.where(k >= 16, 1, 0)
        )
        return 1.0 / (1.0 + degree.astype(F32))

    moment_scale = 1.0 / 32.0

    def folded(tiles):
        for bit in (4, 2, 1):
            low = (sub & bit) == 0
            count = len(tiles) // 2
            merged = []
            for first, second in zip(tiles[:count], tiles[count:]):
                given = jnp.where(low, second, first)
                if bit == 4:
                    given = pltpu.roll(given, 4, 0)
                else:
                    given = jnp.where(low, pltpu.roll(given, 8 - bit, 0), pltpu.roll(given, bit, 0))
                merged.append(jnp.where(low, first, second) + given)
            tiles = merged
        return tiles[0]

    def mix_history(column):
        def eight(q, nothing):
            offs = [pl.ds(pl.multiple_of((q * 8 + r) * LANES, LANES), LANES) for r in range(8)]
            den[pl.ds(pl.multiple_of(q * 8, 8), 8), :] = folded(
                [column * (rho[:, off] + MIX_BETA * res[:, off]) for off in offs]
            )
            return nothing

        lax.fori_loop(0, blocks // 8, eight, 0, unroll=2)

    def correct_density(total, final):
        total = total * (packed_scale(ROWS) * (MIX_BETA * moment_scale))
        first = total[0:8]
        rest = jnp.concatenate([total[8:13], jnp.zeros((3, LANES), F32)], axis=0)
        second = jnp.where(sub < 4, rest, pltpu.roll(pltpu.roll(rest, 4, 0), batches, 1))
        last = jnp.broadcast_to(rest[4:5], (8, LANES))

        def wide(x, b):
            return jnp.broadcast_to(x[:, b:b + 1], (8, LANES))

        for q in range(blocks // 8):
            tiles = []
            last_col = None
            for u in range(4):
                b = 4 * q + u
                cols = (wide(first, b), wide(first, batches + b), wide(second, b))
                col = wide(last, b)
                last_col = col if u == 0 else jnp.where(sub >= 2 * u, col, last_col)
                for h in range(2):
                    off = slice((2 * b + h) * LANES, (2 * b + h + 1) * LANES)
                    tiles.append(
                        cols[0] * basis[0:8, off] + cols[1] * basis[8:16, off] + cols[2] * basis[16:24, off]
                    )
            at = slice(q * 8, q * 8 + 8)
            dense = den[at, :] - folded(tiles) - last_col * last_rows[at, :]
            den[at, :] = dense
            if not final:
                rnew[at, :] = t[at, :] + cpl[at, :] * jnp.tanh(dense) - dense

    row = group_sum(int0_b, own_b, INT0_B)
    entries[0:40, :] = entry_values(row, 40)

    def pair(i, j):
        s = (i - j) % 8
        return splat(0, 8 * s + i) if s <= 4 else splat(0, 8 * ((j - i) % 8) + j)

    weights0 = mixing_weights([[pair(i, j) for j in range(i + 1)] for i in range(HIST)])
    column0 = history_column(weights0)

    def history_block(i, s):
        return jnp.concatenate([hist_a[i // 2][s, i % 2], last_a[s, i:i + 1]], axis=0)

    def mixed_block(values, column, s):
        total = jnp.broadcast_to(values[0][0:1], (ROWS - 1, LANES)) * hist_a[0][s, 0]
        for i in range(1, HIST):
            total = total + jnp.broadcast_to(values[i][0:1], (ROWS - 1, LANES)) * hist_a[i // 2][s, i % 2]
        return jnp.concatenate([total, sublane_total(column * last_a[s])[0:1]], axis=0)

    for chunk in range(4):
        arrived(hist_a[chunk], HIST_KEYS[chunk], GROUP - 1)
    arrived(last_a, LAST_A, GROUP - 1)
    contributions(left_sides(lambda s: mixed_block(weights0, column0, s)), same_atom, send0)
    scatter(send0, pb0_b, PB0_B)
    loads[LD_RHO].wait()
    loads[LD_TARGET].wait()
    loads[LD_COUPLING].wait()
    loads[LD_INDEX].wait()
    mix_history(column0)

    arrived(slot_a, SLOT_A, GROUP - 1)
    place_of = iota((GROUP * 16, LANES), 0)
    number = me["x"] * (GROUP * batches) + me["y"] * 4
    number = number + (place_of >> 7) * 512 + ((place_of >> 4) & 7) * 16 + ((place_of >> 2) & 3) * LANES + (place_of & 3)
    for q in range(GROUP // 2):
        slots = jnp.where(half, slot_a[2 * q], pltpu.roll(slot_a[2 * q + 1], batches, 1))
        owned_slot[:, q * LANES:(q + 1) * LANES] = jnp.where(number == slots, 1.0, 0.0).astype(jnp.bfloat16)

    def slot_sums(parts):
        return lax.dot_general(owned_slot[...], parts, (((1,), (1,)), ((), ())), preferred_element_type=F32)

    for i in range(HIST):
        parts = left_sides(lambda s: history_block(i, s))
        for part in range(3):
            sides8[part * 256 + i * 32:part * 256 + i * 32 + 32, :] = parts[part * 32:part * 32 + 32]
    sums = slot_sums(sides8[...])
    sums = sums[:, 0:256] + sums[:, 256:512] + sums[:, 512:768]
    for p in range(GROUP):
        send_old[p] = sums[p * 16:p * 16 + 16]
    pb0_total = group_sum(pb0_b, own_b, PB0_B)
    scatter(send_old, old_b, OLD_B)
    correct_density(pb0_total, False)

    where = slot_index[0]
    at_slot = sub == where

    def new_batches(q, carry):
        acc, k01, k2, k3 = carry
        for u in range(4):
            b = q * 4 + u
            offs = [pl.ds(pl.multiple_of((2 * b + h) * LANES, LANES), LANES) for h in range(2)]
            field = []
            for h in range(2):
                fresh = jnp.broadcast_to(rnew[pl.ds(2 * b + h, 1), :], (8, LANES))
                field.append(fresh * jnp.broadcast_to(w[pl.ds(2 * b + h, 1), :], (8, LANES)))
                acc = acc + jnp.where(at_slot, fresh, res[:, offs[h]]) * field[h]
            parts = []
            for kt in range(3):
                rows = slice(kt * 8, kt * 8 + 8)
                product = basis[rows, offs[0]] * field[0] + basis[rows, offs[1]] * field[1]
                parts.append(jnp.sum(product, axis=1, keepdims=True))
            last = basis[24:25, offs[0]] * field[0][0:1] + basis[24:25, offs[1]] * field[1][0:1]
            k01, k2 = place(b, parts, k01, k2)
            k3 = jnp.where(lane[0:1] == b, jnp.sum(last, axis=1, keepdims=True), k3)
        return acc, k01, k2, k3

    acc, k01, k2, k3 = lax.fori_loop(0, batches // 4, new_batches, (zero, zero, zero, zero[0:1]), unroll=4)
    total = jnp.sum(acc, axis=1, keepdims=True)
    row = sublane_total(jnp.where(lane == sub + batches, total, 0.0))[0:1, :]
    put_moments(new_a, (own_a,), k01, k2)
    new_a[own_a, 12:13] = jnp.where(half, k3, row)
    gather(new_a, own_a, NEW_A, peers_a)

    def overwrite(q, nothing):
        for u in range(8):
            j = q * 8 + u
            off = pl.ds(pl.multiple_of(j * LANES, LANES), LANES)
            res[:, off] = jnp.where(at_slot, jnp.broadcast_to(rnew[pl.ds(j, 1), :], (8, LANES)), res[:, off])
            rho[:, off] = jnp.where(at_slot, jnp.broadcast_to(den[pl.ds(j, 1), :], (8, LANES)), rho[:, off])
        return nothing

    lax.fori_loop(0, blocks // 8, overwrite, 0)

    arrived(new_a, NEW_A, GROUP - 1)
    row = new_a[0, 12:13]
    for s in range(1, GROUP):
        row = row + new_a[s, 12:13]
    int1_b[own_b] = pltpu.roll(row, batches, 1)
    gather(int1_b, own_b, INT1_B, peers_b)
    fresh_parts = left_sides(lambda s: new_a[s])
    fresh_sums = slot_sums(jnp.concatenate([fresh_parts, jnp.zeros((32, GROUP * batches), jnp.bfloat16)], axis=0))
    for p in range(GROUP):
        send_fresh[p] = fresh_sums[p * 16:p * 16 + 16]
    scatter(send_fresh, fresh_b, FRESH_B)
    old_total = group_sum(old_b, own_b, OLD_B)
    row = group_sum(int1_b, own_b, INT1_B)
    entries[40:48, :] = entry_values(row, 8)
    fresh_row = [splat(40, i) for i in range(HIST)]
    weights1 = mixing_weights([
        [jnp.where(where == i, fresh_row[j], jnp.where(where == j, fresh_row[i], pair(i, j))) for j in range(i + 1)]
        for i in range(HIST)
    ])
    column1 = history_column(weights1)

    kept = [jnp.where(where == i, 0.0, weights1[i]) for i in range(HIST)]
    fresh_weight = jnp.where(where == 0, weights1[0], 0.0)
    for i in range(1, HIST):
        fresh_weight = fresh_weight + jnp.where(where == i, weights1[i], 0.0)
    kept_column = history_column(kept)
    sides = left_sides(
        lambda s: mixed_block(kept, kept_column, s) + jnp.broadcast_to(fresh_weight[0:1], (ROWS, LANES)) * new_a[s]
    )
    contributions(sides, same_atom, send1)
    scatter(send1, pb1_b, PB1_B)

    part_of = lane >> 5
    lower = kept[3]
    upper = kept[7]
    for n in range(3):
        lower = jnp.where(part_of == n, kept[n], lower)
        upper = jnp.where(part_of == n, kept[n + 4], upper)
    fresh_total = group_sum(fresh_b, own_b, FRESH_B)
    owned = []
    for n in range(2):
        rows = slice(8 * n, 8 * n + 8)
        value = old_total[rows, 0:LANES] * lower + old_total[rows, LANES:2 * LANES] * upper
        value = value + fresh_total[rows] * fresh_weight
        value = value + pltpu.roll(value, 64, 1)
        owned.append((value + pltpu.roll(value, 32, 1)) * moment_scale)
    piece = jnp.where(
        part_of < 2,
        jnp.where(part_of == 0, owned[0], pltpu.roll(owned[0], 4, 0)),
        jnp.where(part_of == 2, owned[1], pltpu.roll(owned[1], 4, 0)),
    )
    own_zy = me["z"] * 4 + me["y"]
    mom_zy[own_zy] = piece[0:4]
    gather(mom_zy, own_zy, MOM_ZY, peers_zy)

    mix_history(column1)
    correct_density(group_sum(pb1_b, own_b, PB1_B), True)
    arrived(mom_zy, MOM_ZY, len(peers_zy))
    by_slot = jnp.concatenate([mom_zy[p] for p in range(32)], axis=0).T
    for g in range(4):
        cols, at = slice(g * LANES, (g + 1) * LANES), g * 32
        mom[0:8, cols] = by_slot[at:at + 8]
        mom[8:16, cols] = by_slot[at + 16:at + 24]
        mom[16:20, cols] = by_slot[at + 8:at + 12]
        mom[20:24, cols] = by_slot[at + 24:at + 28]
        mom[24:25, cols] = by_slot[at + 12:at + 13]

    for buf, key, count in (
        (int0_a, INT0_A, 15), (int0_b, INT0_B, 15), (atom_a, ATOM_A, 15), (atom_b, ATOM_B, 15),
        (slot_a, SLOT_A, 15), (hist_0, HIST_0, 15), (hist_1, HIST_1, 15), (hist_2, HIST_2, 15), (hist_3, HIST_3, 15),
        (last_a, LAST_A, 15),
        (new_a, NEW_A, 15), (int1_b, INT1_B, 15),
        (pb0_b, PB0_B, 15), (pb1_b, PB1_B, 15), (old_b, OLD_B, 15), (fresh_b, FRESH_B, 15), (mom_zy, MOM_ZY, 31),
    ):
        sent(buf, key, count)


def hand_over(den, mom, den_h, mom_h, sem):
    copies = [pltpu.make_async_copy(den, den_h, sem.at[0]), pltpu.make_async_copy(mom, mom_h, sem.at[1])]
    for copy in copies:
        copy.start()
    for copy in copies:
        copy.wait()


def local(weights, target, coupling, basis, rho_hist, res_hist, batch_atom, owner_slot, slot_index):
    points = weights.shape[0]
    blocks = points // LANES
    harmonics = basis.shape[0]
    batches = batch_atom.shape[0]
    slots = owner_slot.shape[0]
    dense = lambda x: x.reshape(blocks, LANES)
    operands = (
        dense(weights), dense(target), dense(coupling), basis, rho_hist, res_hist,
        batch_atom.reshape(1, batches), owner_slot.reshape(slots // LANES, LANES), slot_index,
    )
    hbm = pl.BlockSpec(memory_space=pltpu.HBM)
    vmem = pl.BlockSpec(memory_space=pltpu.VMEM)
    small = lambda dtype: pltpu.VMEM((GROUP, 1, LANES), dtype)
    pair_block = lambda: pltpu.VMEM((GROUP, 2, ROWS - 1, LANES), F32)
    block = lambda count: pltpu.VMEM((count, ROWS, LANES), F32)
    relation = pltpu.VMEM((GROUP * batches, GROUP * batches), jnp.bfloat16)
    density, moments = pl.pallas_call(
        body,
        out_shape=(
            jax.ShapeDtypeStruct((blocks, LANES), F32),
            jax.ShapeDtypeStruct((harmonics, slots // 8), F32),
        ),
        in_specs=[hbm] * len(operands),
        out_specs=(vmem, vmem),
        scratch_shapes=[
            pltpu.VMEM((blocks, LANES), F32),
            pltpu.VMEM((blocks, LANES), F32),
            pltpu.VMEM((blocks, LANES), F32),
            pltpu.VMEM((harmonics, points), F32),
            pltpu.VMEM((HIST, points), F32),
            pltpu.VMEM((HIST, points), F32),
            pltpu.VMEM((HIST, points), F32),
            pltpu.VMEM((1, batches), jnp.int32),
            pltpu.VMEM((slots // LANES, LANES), jnp.int32),
            pltpu.VMEM((blocks, LANES), F32),
            pltpu.VMEM((blocks, LANES), F32),
            pltpu.SMEM((2,), jnp.int32),
            pltpu.VMEM((48, LANES), F32),
            relation,
            pltpu.VMEM((GROUP * 16, GROUP * batches), jnp.bfloat16),
            pltpu.VMEM((HIST * 3 * 32, GROUP * batches), jnp.bfloat16),
            small(F32), small(F32), small(F32), small(jnp.int32), small(jnp.int32), small(jnp.int32),
            pair_block(), pair_block(), pair_block(), pair_block(),
            pltpu.VMEM((GROUP, HIST, LANES), F32),
            block(GROUP), block(GROUP), block(GROUP),
            pltpu.VMEM((GROUP, 16, 2 * LANES), F32),
            pltpu.VMEM((GROUP, 16, LANES), F32),
            pltpu.VMEM((32, 4, LANES), F32),
            block(GROUP), block(GROUP),
            pltpu.VMEM((GROUP, 16, 2 * LANES), F32),
            pltpu.VMEM((GROUP, 16, LANES), F32),
            pltpu.SemaphoreType.DMA((LOCALS,)),
            pltpu.SemaphoreType.DMA((EXCHANGES,)),
            pltpu.SemaphoreType.DMA((EXCHANGES,)),
        ],
        compiler_params=pltpu.CompilerParams(collective_id=0, has_side_effects=True, vmem_limit_bytes=24 << 20),
    )(
        *(pltpu.with_memory_space_constraint(x, pltpu.HBM) for x in operands)
    )
    density, moments = pl.pallas_call(
        hand_over,
        out_shape=(
            jax.ShapeDtypeStruct((blocks, LANES), F32),
            jax.ShapeDtypeStruct((harmonics, slots // 8), F32),
        ),
        in_specs=[vmem, vmem],
        out_specs=(hbm, hbm),
        scratch_shapes=[pltpu.SemaphoreType.DMA((2,))],
        compiler_params=pltpu.CompilerParams(vmem_limit_bytes=1 << 20),
    )(density, moments)
    return density.reshape(points), moments


def solution(mesh):
    torus = Mesh(mesh.devices.reshape(tuple(SIZES.values())), AXES)
    points = P(AXES)
    rows = P(None, AXES)
    return jax.shard_map(
        local,
        mesh=torus,
        in_specs=(points, points, points, rows, rows, rows, points, P(), P()),
        out_specs=(points, P(None, ("x", "c"))),
        check_vma=False,
    )
```

```python
import itertools

import jax
import jax.numpy as jnp
from jax import lax
from jax.experimental import pallas as pl
from jax.experimental.pallas import tpu as pltpu
from jax.sharding import Mesh
from jax.sharding import PartitionSpec as P

AXES = ("z", "y", "x", "c")
SIZES = {"z": 8, "y": 4, "x": 4, "c": 2}
HIST = 8
LANES = 128
MESH = pl.DeviceIdType.MESH
F32 = jnp.float32
MIX_BETA = 0.5
RIDGE_SHARE = 0.1
GROUP = 16
ROWS = 13
INT0_A, INT0_B, ATOM_A, ATOM_B, SLOT_A, HIST_0, HIST_1, HIST_2, HIST_3, LAST_A, NEW_A, INT1_B, PB0_B, PB1_B, OLD_B, FRESH_B, MOM_ZY = range(17)
EXCHANGES = 17
HIST_KEYS = (HIST_0, HIST_1, HIST_2, HIST_3)
LD_RES, LD_W, LD_ATOM, LD_OWNER, LD_BASIS, LD_RHO, LD_TARGET, LD_COUPLING, LD_INDEX = range(9)
LOCALS = 9


def iota(shape, dim):
    return lax.broadcasted_iota(jnp.int32, shape, dim)


def sublane_total(x):
    x = x + pltpu.roll(x, 4, 0)
    x = x + pltpu.roll(x, 2, 0)
    return x + pltpu.roll(x, 1, 0)


def mixing_weights(entry):
    matrix = [[entry[i][j] for j in range(i + 1)] for i in range(HIST)]
    trace = matrix[0][0]
    for i in range(1, HIST):
        trace = trace + matrix[i][i]
    ridge = trace * (RIDGE_SHARE / HIST)
    for i in range(HIST):
        matrix[i][i] = matrix[i][i] + ridge
    forward = [jnp.ones((8, LANES), F32) for _ in range(HIST)]
    pivot = [None] * HIST
    lower = [[None] * HIST for _ in range(HIST)]
    for j in range(HIST):
        pivot[j] = 1.0 / matrix[j][j]
        for i in range(j + 1, HIST):
            ratio = matrix[i][j] * pivot[j]
            for k in range(j + 1, i + 1):
                matrix[i][k] = matrix[i][k] - ratio * matrix[k][j]
            forward[i] = forward[i] - ratio * forward[j]
            lower[i][j] = ratio
    solved = [None] * HIST
    for i in reversed(range(HIST)):
        value = forward[i] * pivot[i]
        for k in range(i + 1, HIST):
            value = value - lower[k][i] * solved[k]
        solved[i] = value
    total = solved[0]
    for i in range(1, HIST):
        total = total + solved[i]
    scale = 1.0 / total
    return [value * scale for value in solved]


def history_column(values):
    sub = iota((8, LANES), 0)
    column = jnp.zeros((8, LANES), F32)
    for i in range(HIST):
        column = jnp.where(sub == i, values[i], column)
    return column


def three_parts(x):
    high = x.astype(jnp.bfloat16)
    rest = x - high.astype(F32)
    middle = rest.astype(jnp.bfloat16)
    low = (rest - middle.astype(F32)).astype(jnp.bfloat16)
    return jnp.concatenate([high, middle, low], axis=0)


def body(
    w_h, t_h, cpl_h, basis_h, rho_h, res_h, atom_h, owner_h, index_h,
    den, mom,
    w, t, cpl, basis, rho, res, wres, atom, owner, rnew, wnew, last_rows, slot_index,
    entries, same_atom, owned_slot, sides8, old_out, fresh_out,
    int0_a, int0_b, int1_b, atom_a, atom_b, slot_a,
    hist_0, hist_1, hist_2, hist_3, last_a, new_a, pb0_b, pb1_b, old_b, fresh_b, mom_zy, send0, send1, send_old, send_fresh,
    local_sem, send_sem, recv_sem,
):
    me = {name: lax.axis_index(name) for name in AXES}
    own_a = me["y"] * 4 + me["x"]
    hist_a = (hist_0, hist_1, hist_2, hist_3)
    own_b = me["c"] * 8 + me["z"]
    blocks = w.shape[0]

    loads = {}
    for key, src, dst in (
        (LD_RES, res_h, res), (LD_W, w_h, w), (LD_ATOM, atom_h, atom), (LD_OWNER, owner_h, owner),
        (LD_BASIS, basis_h, basis), (LD_RHO, rho_h, rho), (LD_TARGET, t_h, t), (LD_COUPLING, cpl_h, cpl),
        (LD_INDEX, index_h, slot_index),
    ):
        loads[key] = pltpu.make_async_copy(src, dst, local_sem.at[key])
        loads[key].start()

    def peers(*names):
        steps = [s for s in itertools.product(*(range(SIZES[name]) for name in names)) if any(s)]
        hops = lambda s: sum(min(d, SIZES[name] - d) for d, name in zip(s, names))
        steps.sort(key=hops, reverse=True)
        return [{name: lax.rem(me[name] + d, SIZES[name]) for d, name in zip(s, names)} for s in steps]

    peers_a, peers_b, peers_zy = peers("y", "x"), peers("z", "c"), peers("z", "y")

    barrier = pltpu.get_barrier_semaphore()
    for peer in peers_a + peers_b:
        pl.semaphore_signal(barrier, inc=1, device_id=peer, device_id_type=MESH)

    def send(src, dst, key, peer):
        pltpu.make_async_remote_copy(
            src_ref=src, dst_ref=dst, send_sem=send_sem.at[key], recv_sem=recv_sem.at[key],
            device_id=peer, device_id_type=MESH,
        ).start()

    def gather(buf, own, key, peers):
        for peer in peers:
            send(buf.at[own], buf.at[own], key, peer)

    def arrived(buf, key, count):
        view = buf.at[pl.ds(0, count)]
        pltpu.make_async_copy(view, view, recv_sem.at[key]).wait()

    def sent(buf, key, count):
        view = buf.at[pl.ds(0, count)]
        pltpu.make_async_copy(view, view, send_sem.at[key]).wait()

    sub = iota((8, LANES), 0)
    lane = iota((8, LANES), 1)

    loads[LD_RES].wait()
    loads[LD_W].wait()

    def products(q, accs):
        accs = list(accs)
        for u in range(8):
            off = pl.multiple_of((q * 8 + u) * LANES, LANES)
            r = res[:, pl.ds(off, LANES)]
            rw = r * jnp.broadcast_to(w[pl.ds(q * 8 + u, 1), :], (8, LANES))
            wres[:, pl.ds(off, LANES)] = rw
            accs[0] = accs[0] + rw * r
            for s in range(1, 5):
                accs[s] = accs[s] + rw * pltpu.roll(r, s, 0)
        return tuple(accs)

    zero = jnp.zeros((8, LANES), F32)
    accs = lax.fori_loop(0, blocks // 8, products, (zero,) * 5)
    placed = zero
    for s in range(5):
        total = jnp.sum(accs[s], axis=1, keepdims=True)
        placed = jnp.where(lane == 8 * s + sub, total, placed)
    int0_a[own_a] = sublane_total(placed)[0:1, :]

    batches = 64
    loads[LD_BASIS].wait()

    def place(b, parts, k01, k2):
        k01 = jnp.where(lane == b, parts[0], k01)
        k01 = jnp.where(lane == b + batches, parts[1], k01)
        return k01, jnp.where(lane == b + jnp.where(sub >= 4, batches, 0), parts[2], k2)

    def batch_spans(b):
        return [pl.ds(pl.multiple_of((2 * b + h) * LANES, LANES), LANES) for h in range(2)]

    def chunk_moments(chunk):
        def one(b, carry):
            carry = list(carry)
            offs = batch_spans(b)
            tiles = [[basis[kt * 8:kt * 8 + 8, off] for off in offs] for kt in range(3)]
            for n in range(2):
                i = 2 * chunk + n
                field = [jnp.broadcast_to(wres[i:i + 1, off], (8, LANES)) for off in offs]
                parts = [
                    jnp.sum(tiles[kt][0] * field[0] + tiles[kt][1] * field[1], axis=1, keepdims=True)
                    for kt in range(3)
                ]
                carry[2 * n], carry[2 * n + 1] = place(b, parts, carry[2 * n], carry[2 * n + 1])
            return tuple(carry)

        return lax.fori_loop(0, batches, one, (zero,) * 4, unroll=8)

    def last_harmonic(b, placed):
        offs = batch_spans(b)
        last = [wres[:, off] * jnp.broadcast_to(basis[24:25, off], (8, LANES)) for off in offs]
        return jnp.where(lane == b, jnp.sum(last[0] + last[1], axis=1, keepdims=True), placed)

    def put_moments(buf, at, k01, k2):
        buf[(*at, slice(0, 8))] = k01
        buf[(*at, slice(8, 12))] = (k2 + pltpu.roll(k2, 4, 0))[0:4]

    def fill_chunk(chunk):
        found = chunk_moments(chunk)
        for n in range(2):
            put_moments(hist_a[chunk], (own_a, n), found[2 * n], found[2 * n + 1])

    loads[LD_ATOM].wait()
    atom_wide = jnp.concatenate([atom[...], atom[...]], axis=1)
    atom_a[own_a] = atom_wide
    atom_b[own_b] = atom_wide
    fill_chunk(0)

    pl.semaphore_wait(barrier, len(peers_a) + len(peers_b))
    gather(int0_a, own_a, INT0_A, peers_a)
    gather(atom_a, own_a, ATOM_A, peers_a)
    gather(atom_b, own_b, ATOM_B, peers_b)
    gather(hist_a[0], own_a, HIST_0, peers_a)
    for chunk in range(1, 4):
        if chunk == 3:
            last = lax.fori_loop(0, batches, last_harmonic, zero, unroll=8)
            last = jnp.where(lane < batches, last, pltpu.roll(pltpu.roll(last, 4, 0), batches, 1))
            last_a[own_a] = last[0:4]
            gather(last_a, own_a, LAST_A, peers_a)
        fill_chunk(chunk)
        gather(hist_a[chunk], own_a, HIST_KEYS[chunk], peers_a)

    loads[LD_OWNER].wait()
    wide_sub = iota((batches, LANES), 0)
    wide_lane = iota((batches, LANES), 1)
    own_lane = wide_lane == wide_sub

    def as_column(row):
        return jnp.sum(jnp.where(own_lane, jnp.broadcast_to(row, (batches, LANES)), 0.0), axis=1, keepdims=True)

    atom_col = as_column(atom_wide.astype(F32))

    def look_up(j, found):
        owners = jnp.broadcast_to(owner[pl.ds(j, 1), :].astype(F32), (batches, LANES))
        number = (wide_lane + j * LANES).astype(F32)
        return found + jnp.where(number == atom_col, owners, 0.0)

    found = lax.fori_loop(0, owner.shape[0], look_up, jnp.zeros((batches, LANES), F32))
    slot_col = jnp.sum(found, axis=1, keepdims=True)
    slot_a[own_a] = jnp.sum(jnp.where(own_lane, slot_col, 0.0), axis=0, keepdims=True).astype(jnp.int32)
    gather(slot_a, own_a, SLOT_A, peers_a)

    def group_sum(buf, own, key):
        arrived(buf, key, GROUP - 1)
        total = buf[0]
        for i in range(1, GROUP):
            total = total + buf[i]
        return total

    int0_b[own_b] = group_sum(int0_a, own_a, INT0_A)
    gather(int0_b, own_b, INT0_B, peers_b)

    arrived(atom_a, ATOM_A, GROUP - 1)
    arrived(atom_b, ATOM_B, GROUP - 1)
    half = iota((1, LANES), 1) < batches
    atoms_b = [jnp.where(half, atom_b[2 * q], atom_b[2 * q + 1]).astype(F32) for q in range(GROUP // 2)]

    def relate_atoms(s, nothing):
        atoms_a = as_column(atom_a[s].astype(F32))
        at = pl.ds(pl.multiple_of(s * batches, batches), batches)
        for q in range(GROUP // 2):
            cols = pl.ds(q * LANES, LANES)
            same_atom[at, cols] = jnp.where(atoms_a == atoms_b[q], 1.0, 0.0).astype(jnp.bfloat16)
        return nothing

    lax.fori_loop(0, GROUP, relate_atoms, 0)

    def last_row(q, nothing):
        for u in range(8):
            j = q * 8 + u
            last_rows[pl.ds(j, 1), :] = basis[24:25, pl.ds(pl.multiple_of(j * LANES, LANES), LANES)]
        return nothing

    lax.fori_loop(0, blocks // 8, last_row, 0)

    def entry_values(row, count):
        rows = iota((count, LANES), 0)
        lanes = iota((count, LANES), 1)
        total = jnp.sum(jnp.where(rows == lanes, jnp.broadcast_to(row, (count, LANES)), 0.0), axis=1, keepdims=True)
        return jnp.broadcast_to(total, (count, LANES))

    def splat(base, i):
        return jnp.broadcast_to(entries[pl.ds(base + i, 1), :], (8, LANES))

    def left_sides(block_of):
        is_low = iota((ROWS, LANES), 1) < batches
        lows, highs = [], []
        for q in range(GROUP // 2):
            first, second = block_of(2 * q), block_of(2 * q + 1)
            lows.append(jnp.where(is_low, first, pltpu.roll(second, batches, 1)))
            highs.append(jnp.where(is_low, pltpu.roll(first, batches, 1), second))
        pad = jnp.zeros((16 - ROWS, GROUP * batches), F32)
        low = jnp.concatenate(lows, axis=1)
        high = jnp.concatenate(highs, axis=1)
        return three_parts(jnp.concatenate([low, pad, high, pad], axis=0))

    def contributions(parts, matrix, out):
        result = jnp.dot(parts, matrix[...], preferred_element_type=F32)
        pack_contributions(result[0:32] + result[32:64] + result[64:96], out)

    def pack_contributions(result, out):
        is_low = iota((ROWS, LANES), 1) < batches
        for q in range(GROUP // 2):
            cols = slice(q * LANES, (q + 1) * LANES)
            low, high = result[0:ROWS, cols], result[16:16 + ROWS, cols]
            out[2 * q] = jnp.where(is_low, low, pltpu.roll(high, batches, 1))
            out[2 * q + 1] = jnp.where(is_low, pltpu.roll(low, batches, 1), high)

    def scatter(out, buf, key):
        buf[own_b] = out[own_b]
        for peer in peers_b:
            send(out.at[peer.get("c") * 8 + peer.get("z")], buf.at[own_b], key, peer)

    def packed_scale(rows):
        r, c = iota((rows, LANES), 0), iota((rows, LANES), 1)
        high = c >= batches
        k = jnp.where(r < 8, jnp.where(high, r + 8, r), jnp.where(high, r + 12, r + 8))
        k = jnp.where(r == 12, 24, k)
        degree = (
            jnp.where(k >= 1, 1, 0) + jnp.where(k >= 4, 1, 0) + jnp.where(k >= 9, 1, 0) + jnp.where(k >= 16, 1, 0)
        )
        return 1.0 / (1.0 + degree.astype(F32))

    moment_scale = 1.0 / 32.0

    def folded(tiles):
        for bit in (4, 2, 1):
            low = (sub & bit) == 0
            count = len(tiles) // 2
            merged = []
            for first, second in zip(tiles[:count], tiles[count:]):
                given = jnp.where(low, second, first)
                if bit == 4:
                    given = pltpu.roll(given, 4, 0)
                else:
                    given = jnp.where(low, pltpu.roll(given, 8 - bit, 0), pltpu.roll(given, bit, 0))
                merged.append(jnp.where(low, first, second) + given)
            tiles = merged
        return tiles[0]

    def mix_history(column):
        def eight(q, nothing):
            offs = [pl.ds(pl.multiple_of((q * 8 + r) * LANES, LANES), LANES) for r in range(8)]
            den[pl.ds(pl.multiple_of(q * 8, 8), 8), :] = folded(
                [column * (rho[:, off] + MIX_BETA * res[:, off]) for off in offs]
            )
            return nothing

        lax.fori_loop(0, blocks // 8, eight, 0, unroll=2)

    def correct_density(total, final):
        total = total * (packed_scale(ROWS) * (MIX_BETA * moment_scale))
        first = total[0:8]
        rest = jnp.concatenate([total[8:13], jnp.zeros((3, LANES), F32)], axis=0)
        second = jnp.where(sub < 4, rest, pltpu.roll(pltpu.roll(rest, 4, 0), batches, 1))
        last = jnp.broadcast_to(rest[4:5], (8, LANES))

        def wide(x, b):
            return jnp.broadcast_to(x[:, b:b + 1], (8, LANES))

        for q in range(blocks // 8):
            tiles = []
            last_col = None
            for u in range(4):
                b = 4 * q + u
                cols = (wide(first, b), wide(first, batches + b), wide(second, b))
                col = wide(last, b)
                last_col = col if u == 0 else jnp.where(sub >= 2 * u, col, last_col)
                for h in range(2):
                    off = slice((2 * b + h) * LANES, (2 * b + h + 1) * LANES)
                    tiles.append(
                        cols[0] * basis[0:8, off] + cols[1] * basis[8:16, off] + cols[2] * basis[16:24, off]
                    )
            at = slice(q * 8, q * 8 + 8)
            dense = den[at, :] - folded(tiles) - last_col * last_rows[at, :]
            den[at, :] = dense
            if not final:
                fresh = t[at, :] + cpl[at, :] * jnp.tanh(dense) - dense
                rnew[at, :] = fresh
                wnew[at, :] = fresh * w[at, :]

    def new_batches(at_slot):
        def four(q, carry):
            acc, k01, k2, k3 = carry
            at = pl.ds(pl.multiple_of(q * 8, 8), 8)
            found = jnp.sum(wnew[at, :] * last_rows[at, :], axis=1, keepdims=True)
            k3 = jnp.where(lane == 4 * q + (sub >> 1), found, k3)
            for u in range(4):
                b = q * 4 + u
                offs = batch_spans(b)
                field = []
                for h in range(2):
                    field.append(jnp.broadcast_to(wnew[pl.ds(2 * b + h, 1), :], (8, LANES)))
                    fresh = jnp.broadcast_to(rnew[pl.ds(2 * b + h, 1), :], (8, LANES))
                    acc = acc + jnp.where(at_slot, fresh, res[:, offs[h]]) * field[h]
                parts = []
                for kt in range(3):
                    rows = slice(kt * 8, kt * 8 + 8)
                    product = basis[rows, offs[0]] * field[0] + basis[rows, offs[1]] * field[1]
                    parts.append(jnp.sum(product, axis=1, keepdims=True))
                k01, k2 = place(b, parts, k01, k2)
            return acc, k01, k2, k3

        acc, k01, k2, k3 = lax.fori_loop(0, batches // 4, four, (zero,) * 4, unroll=4)
        return acc, k01, k2, sublane_total(k3)[0:1]

    row = group_sum(int0_b, own_b, INT0_B)
    entries[0:40, :] = entry_values(row, 40)

    def pair(i, j):
        s = (i - j) % 8
        return splat(0, 8 * s + i) if s <= 4 else splat(0, 8 * ((j - i) % 8) + j)

    weights0 = mixing_weights([[pair(i, j) for j in range(i + 1)] for i in range(HIST)])
    column0 = history_column(weights0)

    def history_block(i, s):
        row = last_a[s, i % 4:i % 4 + 1]
        return jnp.concatenate([hist_a[i // 2][s, i % 2], row if i < 4 else pltpu.roll(row, batches, 1)], axis=0)

    def mixed_block(values, packed, s):
        total = jnp.broadcast_to(values[0][0:1], (ROWS - 1, LANES)) * hist_a[0][s, 0]
        for i in range(1, HIST):
            total = total + jnp.broadcast_to(values[i][0:1], (ROWS - 1, LANES)) * hist_a[i // 2][s, i % 2]
        last = packed * last_a[s]
        last = last[0:1] + last[1:2] + last[2:3] + last[3:4]
        return jnp.concatenate([total, last + pltpu.roll(last, batches, 1)], axis=0)

    for chunk in range(4):
        arrived(hist_a[chunk], HIST_KEYS[chunk], GROUP - 1)
    arrived(last_a, LAST_A, GROUP - 1)
    packed0 = jnp.where(lane < batches, column0, pltpu.roll(column0, 4, 0))[0:4]
    contributions(left_sides(lambda s: mixed_block(weights0, packed0, s)), same_atom, send0)
    scatter(send0, pb0_b, PB0_B)
    loads[LD_RHO].wait()
    loads[LD_TARGET].wait()
    loads[LD_COUPLING].wait()
    loads[LD_INDEX].wait()
    mix_history(column0)

    arrived(slot_a, SLOT_A, GROUP - 1)
    place_of = iota((GROUP * 16, LANES), 0)
    number = me["x"] * (GROUP * batches) + me["y"] * 4
    number = number + (place_of >> 7) * 512 + ((place_of >> 4) & 7) * 16 + ((place_of >> 2) & 3) * LANES + (place_of & 3)
    for q in range(GROUP // 2):
        slots = jnp.where(half, slot_a[2 * q], pltpu.roll(slot_a[2 * q + 1], batches, 1))
        owned_slot[:, q * LANES:(q + 1) * LANES] = jnp.where(number == slots, 1.0, 0.0).astype(jnp.bfloat16)

    def slot_sums(parts):
        return lax.dot_general(owned_slot[...], parts, (((1,), (1,)), ((), ())), preferred_element_type=F32)

    for i in range(HIST):
        parts = left_sides(lambda s: history_block(i, s))
        for part in range(3):
            sides8[part * 256 + i * 32:part * 256 + i * 32 + 32, :] = parts[part * 32:part * 32 + 32]
    sums = slot_sums(sides8[...])
    sums = sums[:, 0:256] + sums[:, 256:512] + sums[:, 512:768]
    for p in range(GROUP):
        send_old[p] = sums[p * 16:p * 16 + 16]
    pb0_total = group_sum(pb0_b, own_b, PB0_B)
    scatter(send_old, old_b, OLD_B)
    correct_density(pb0_total, False)

    where = slot_index[0]
    at_slot = sub == where
    acc, k01, k2, k3 = new_batches(at_slot)
    total = jnp.sum(acc, axis=1, keepdims=True)
    row = sublane_total(jnp.where(lane == sub + batches, total, 0.0))[0:1, :]
    put_moments(new_a, (own_a,), k01, k2)
    new_a[own_a, 12:13] = jnp.where(half, k3, row)
    gather(new_a, own_a, NEW_A, peers_a)

    def overwrite(q, nothing):
        for u in range(8):
            j = q * 8 + u
            off = pl.ds(pl.multiple_of(j * LANES, LANES), LANES)
            res[:, off] = jnp.where(at_slot, jnp.broadcast_to(rnew[pl.ds(j, 1), :], (8, LANES)), res[:, off])
            rho[:, off] = jnp.where(at_slot, jnp.broadcast_to(den[pl.ds(j, 1), :], (8, LANES)), rho[:, off])
        return nothing

    lax.fori_loop(0, blocks // 8, overwrite, 0)
    for n in range(4):
        cols = slice(n * 256, n * 256 + 256)
        out = jnp.dot(sides8[...], same_atom[:, cols], preferred_element_type=F32)
        old_out[:, cols] = out[0:256] + out[256:512] + out[512:768]

    arrived(new_a, NEW_A, GROUP - 1)
    row = new_a[0, 12:13]
    for s in range(1, GROUP):
        row = row + new_a[s, 12:13]
    int1_b[own_b] = pltpu.roll(row, batches, 1)
    gather(int1_b, own_b, INT1_B, peers_b)
    fresh_parts = left_sides(lambda s: new_a[s])
    part_of = lane >> 5

    def every_part(x):
        x = x + pltpu.roll(x, 64, 1)
        return x + pltpu.roll(x, 32, 1)

    def packed_slots(low, high):
        return jnp.where(
            part_of < 2,
            jnp.where(part_of == 0, low, pltpu.roll(low, 4, 0)),
            jnp.where(part_of == 2, high, pltpu.roll(high, 4, 0)),
        )[0:4]

    fresh_sums = slot_sums(jnp.concatenate([fresh_parts, jnp.zeros((32, GROUP * batches), jnp.bfloat16)], axis=0))
    for p in range(GROUP):
        send_fresh[p] = packed_slots(
            every_part(fresh_sums[p * 16:p * 16 + 8]), every_part(fresh_sums[p * 16 + 8:p * 16 + 16])
        )
    scatter(send_fresh, fresh_b, FRESH_B)
    out = jnp.dot(fresh_parts, same_atom[...], preferred_element_type=F32)
    fresh_out[...] = out[0:32] + out[32:64] + out[64:96]
    old_total = group_sum(old_b, own_b, OLD_B)
    row = group_sum(int1_b, own_b, INT1_B)
    entries[40:48, :] = entry_values(row, 8)
    fresh_row = [splat(40, i) for i in range(HIST)]
    weights1 = mixing_weights([
        [jnp.where(where == i, fresh_row[j], jnp.where(where == j, fresh_row[i], pair(i, j))) for j in range(i + 1)]
        for i in range(HIST)
    ])
    column1 = history_column(weights1)

    kept = [jnp.where(where == i, 0.0, weights1[i]) for i in range(HIST)]
    fresh_weight = jnp.where(where == 0, weights1[0], 0.0)
    for i in range(1, HIST):
        fresh_weight = fresh_weight + jnp.where(where == i, weights1[i], 0.0)
    is_low = lane < batches
    for q in range(GROUP // 2):
        cols = slice(q * LANES, (q + 1) * LANES)
        tiles = []
        for r in range(4):
            tile = fresh_weight * fresh_out[8 * r:8 * r + 8, cols]
            for i in range(HIST):
                tile = tile + kept[i] * old_out[i * 32 + 8 * r:i * 32 + 8 * r + 8, cols]
            tiles.append(tile)
        for low, high, rows in ((tiles[0], tiles[2], 8), (tiles[1], tiles[3], ROWS - 8)):
            at = slice(0, 8) if rows == 8 else slice(8, ROWS)
            send1[2 * q, at] = jnp.where(is_low, low, pltpu.roll(high, batches, 1))[0:rows]
            send1[2 * q + 1, at] = jnp.where(is_low, pltpu.roll(low, batches, 1), high)[0:rows]
    scatter(send1, pb1_b, PB1_B)

    lower = kept[3]
    upper = kept[7]
    for n in range(3):
        lower = jnp.where(part_of == n, kept[n], lower)
        upper = jnp.where(part_of == n, kept[n + 4], upper)
    fresh_total = group_sum(fresh_b, own_b, FRESH_B)
    owned = []
    for n in range(2):
        rows = slice(8 * n, 8 * n + 8)
        value = old_total[rows, 0:LANES] * lower + old_total[rows, LANES:2 * LANES] * upper
        owned.append(every_part(value))
    piece = (packed_slots(*owned) + fresh_total * fresh_weight[0:4]) * moment_scale
    own_zy = me["z"] * 4 + me["y"]
    mom_zy[own_zy] = piece
    gather(mom_zy, own_zy, MOM_ZY, peers_zy)

    mix_history(column1)
    correct_density(group_sum(pb1_b, own_b, PB1_B), True)
    arrived(mom_zy, MOM_ZY, len(peers_zy))
    by_slot = jnp.concatenate([mom_zy[p] for p in range(32)], axis=0).T
    for g in range(4):
        cols, at = slice(g * LANES, (g + 1) * LANES), g * 32
        mom[0:8, cols] = by_slot[at:at + 8]
        mom[8:16, cols] = by_slot[at + 16:at + 24]
        mom[16:20, cols] = by_slot[at + 8:at + 12]
        mom[20:24, cols] = by_slot[at + 24:at + 28]
        mom[24:25, cols] = by_slot[at + 12:at + 13]

    for buf, key, count in (
        (int0_a, INT0_A, 15), (int0_b, INT0_B, 15), (atom_a, ATOM_A, 15), (atom_b, ATOM_B, 15),
        (slot_a, SLOT_A, 15), (hist_0, HIST_0, 15), (hist_1, HIST_1, 15), (hist_2, HIST_2, 15), (hist_3, HIST_3, 15),
        (last_a, LAST_A, 15),
        (new_a, NEW_A, 15), (int1_b, INT1_B, 15),
        (pb0_b, PB0_B, 15), (pb1_b, PB1_B, 15), (old_b, OLD_B, 15), (fresh_b, FRESH_B, 15), (mom_zy, MOM_ZY, 31),
    ):
        sent(buf, key, count)


def hand_over(den, mom, den_h, mom_h, sem):
    copies = [pltpu.make_async_copy(den, den_h, sem.at[0]), pltpu.make_async_copy(mom, mom_h, sem.at[1])]
    for copy in copies:
        copy.start()
    for copy in copies:
        copy.wait()


def local(weights, target, coupling, basis, rho_hist, res_hist, batch_atom, owner_slot, slot_index):
    points = weights.shape[0]
    blocks = points // LANES
    harmonics = basis.shape[0]
    batches = batch_atom.shape[0]
    slots = owner_slot.shape[0]
    dense = lambda x: x.reshape(blocks, LANES)
    operands = (
        dense(weights), dense(target), dense(coupling), basis, rho_hist, res_hist,
        batch_atom.reshape(1, batches), owner_slot.reshape(slots // LANES, LANES), slot_index,
    )
    hbm = pl.BlockSpec(memory_space=pltpu.HBM)
    vmem = pl.BlockSpec(memory_space=pltpu.VMEM)
    small = lambda dtype: pltpu.VMEM((GROUP, 1, LANES), dtype)
    pair_block = lambda: pltpu.VMEM((GROUP, 2, ROWS - 1, LANES), F32)
    block = lambda count: pltpu.VMEM((count, ROWS, LANES), F32)
    relation = pltpu.VMEM((GROUP * batches, GROUP * batches), jnp.bfloat16)
    density, moments = pl.pallas_call(
        body,
        out_shape=(
            jax.ShapeDtypeStruct((blocks, LANES), F32),
            jax.ShapeDtypeStruct((harmonics, slots // 8), F32),
        ),
        in_specs=[hbm] * len(operands),
        out_specs=(vmem, vmem),
        scratch_shapes=[
            pltpu.VMEM((blocks, LANES), F32),
            pltpu.VMEM((blocks, LANES), F32),
            pltpu.VMEM((blocks, LANES), F32),
            pltpu.VMEM((harmonics, points), F32),
            pltpu.VMEM((HIST, points), F32),
            pltpu.VMEM((HIST, points), F32),
            pltpu.VMEM((HIST, points), F32),
            pltpu.VMEM((1, batches), jnp.int32),
            pltpu.VMEM((slots // LANES, LANES), jnp.int32),
            pltpu.VMEM((blocks, LANES), F32),
            pltpu.VMEM((blocks, LANES), F32),
            pltpu.VMEM((blocks, LANES), F32),
            pltpu.SMEM((2,), jnp.int32),
            pltpu.VMEM((48, LANES), F32),
            relation,
            pltpu.VMEM((GROUP * 16, GROUP * batches), jnp.bfloat16),
            pltpu.VMEM((HIST * 3 * 32, GROUP * batches), jnp.bfloat16),
            pltpu.VMEM((HIST * 32, GROUP * batches), F32),
            pltpu.VMEM((32, GROUP * batches), F32),
            small(F32), small(F32), small(F32), small(jnp.int32), small(jnp.int32), small(jnp.int32),
            pair_block(), pair_block(), pair_block(), pair_block(),
            pltpu.VMEM((GROUP, 4, LANES), F32),
            block(GROUP), block(GROUP), block(GROUP),
            pltpu.VMEM((GROUP, 16, 2 * LANES), F32),
            pltpu.VMEM((GROUP, 4, LANES), F32),
            pltpu.VMEM((32, 4, LANES), F32),
            block(GROUP), block(GROUP),
            pltpu.VMEM((GROUP, 16, 2 * LANES), F32),
            pltpu.VMEM((GROUP, 4, LANES), F32),
            pltpu.SemaphoreType.DMA((LOCALS,)),
            pltpu.SemaphoreType.DMA((EXCHANGES,)),
            pltpu.SemaphoreType.DMA((EXCHANGES,)),
        ],
        compiler_params=pltpu.CompilerParams(collective_id=0, has_side_effects=True, vmem_limit_bytes=24 << 20),
    )(
        *(pltpu.with_memory_space_constraint(x, pltpu.HBM) for x in operands)
    )
    density, moments = pl.pallas_call(
        hand_over,
        out_shape=(
            jax.ShapeDtypeStruct((blocks, LANES), F32),
            jax.ShapeDtypeStruct((harmonics, slots // 8), F32),
        ),
        in_specs=[vmem, vmem],
        out_specs=(hbm, hbm),
        scratch_shapes=[pltpu.SemaphoreType.DMA((2,))],
        compiler_params=pltpu.CompilerParams(vmem_limit_bytes=1 << 20),
    )(density, moments)
    return density.reshape(points), moments


def solution(mesh):
    torus = Mesh(mesh.devices.reshape(tuple(SIZES.values())), AXES)
    points = P(AXES)
    rows = P(None, AXES)
    return jax.shard_map(
        local,
        mesh=torus,
        in_specs=(points, points, points, rows, rows, rows, points, P(), P()),
        out_specs=(points, P(None, ("x", "c"))),
        check_vma=False,
    )
```

```python
import itertools

import jax
import jax.numpy as jnp
from jax import lax
from jax.experimental import pallas as pl
from jax.experimental.pallas import tpu as pltpu
from jax.sharding import Mesh
from jax.sharding import PartitionSpec as P

AXES = ("z", "y", "x", "c")
SIZES = {"z": 8, "y": 4, "x": 4, "c": 2}
HIST = 8
LANES = 128
MESH = pl.DeviceIdType.MESH
F32 = jnp.float32
MIX_BETA = 0.5
RIDGE_SHARE = 0.1
GROUP = 16
ROWS = 13
INT0_A, INT0_B, ATOM_A, ATOM_B, SLOT_A, HIST_0, HIST_1, HIST_2, HIST_3, LAST_A, NEW_A, INT1_B, PB0_B, PB1_B, OLD_C, OLD_Z, FRESH_B, MOM_ZY = range(18)
EXCHANGES = 18
HIST_KEYS = (HIST_0, HIST_1, HIST_2, HIST_3)
LD_RES, LD_W, LD_ATOM, LD_OWNER, LD_BASIS, LD_RHO, LD_TARGET, LD_COUPLING, LD_INDEX = range(9)
LOCALS = 9


def iota(shape, dim):
    return lax.broadcasted_iota(jnp.int32, shape, dim)


def sublane_total(x):
    x = x + pltpu.roll(x, 4, 0)
    x = x + pltpu.roll(x, 2, 0)
    return x + pltpu.roll(x, 1, 0)


def mixing_weights(entry):
    matrix = [[entry[i][j] for j in range(i + 1)] for i in range(HIST)]
    trace = matrix[0][0]
    for i in range(1, HIST):
        trace = trace + matrix[i][i]
    ridge = trace * (RIDGE_SHARE / HIST)
    for i in range(HIST):
        matrix[i][i] = matrix[i][i] + ridge
    forward = [jnp.ones((8, LANES), F32) for _ in range(HIST)]
    pivot = [None] * HIST
    lower = [[None] * HIST for _ in range(HIST)]
    for j in range(HIST):
        pivot[j] = 1.0 / matrix[j][j]
        for i in range(j + 1, HIST):
            ratio = matrix[i][j] * pivot[j]
            for k in range(j + 1, i + 1):
                matrix[i][k] = matrix[i][k] - ratio * matrix[k][j]
            forward[i] = forward[i] - ratio * forward[j]
            lower[i][j] = ratio
    solved = [None] * HIST
    for i in reversed(range(HIST)):
        value = forward[i] * pivot[i]
        for k in range(i + 1, HIST):
            value = value - lower[k][i] * solved[k]
        solved[i] = value
    total = solved[0]
    for i in range(1, HIST):
        total = total + solved[i]
    scale = 1.0 / total
    return [value * scale for value in solved]


def history_column(values):
    sub = iota((8, LANES), 0)
    column = jnp.zeros((8, LANES), F32)
    for i in range(HIST):
        column = jnp.where(sub == i, values[i], column)
    return column


def three_parts(x):
    high = x.astype(jnp.bfloat16)
    rest = x - high.astype(F32)
    middle = rest.astype(jnp.bfloat16)
    low = (rest - middle.astype(F32)).astype(jnp.bfloat16)
    return jnp.concatenate([high, middle, low], axis=0)


def body(
    w_h, t_h, cpl_h, basis_h, rho_h, res_h, atom_h, owner_h, index_h,
    den, mom,
    w, t, cpl, basis, rho, res, wres, atom, owner, rows8, mixed, w_t, target_t, coupling_t, mixed_t, den_t, fresh_t, basis_t, res_t, coef, slot_index,
    entries, same_atom, owned_slot, sides8, old_out, fresh_out,
    int0_a, int0_b, int1_b, atom_a, atom_b, slot_a,
    hist_0, hist_1, hist_2, hist_3, last_a, new_a, pb0_b, pb1_b, old_c, old_z, fresh_b, mom_zy, send0, send1, send_old, mine_old, send_fresh,
    local_sem, send_sem, recv_sem,
):
    me = {name: lax.axis_index(name) for name in AXES}
    own_a = me["y"] * 4 + me["x"]
    hist_a = (hist_0, hist_1, hist_2, hist_3)
    own_b = me["c"] * 8 + me["z"]
    blocks = w.shape[0]

    loads = {}
    for key, src, dst in (
        (LD_RES, res_h, res), (LD_W, w_h, w), (LD_ATOM, atom_h, atom), (LD_OWNER, owner_h, owner),
        (LD_BASIS, basis_h, basis), (LD_RHO, rho_h, rho), (LD_TARGET, t_h, t), (LD_COUPLING, cpl_h, cpl),
        (LD_INDEX, index_h, slot_index),
    ):
        loads[key] = pltpu.make_async_copy(src, dst, local_sem.at[key])
        loads[key].start()

    def peers(*names):
        steps = [s for s in itertools.product(*(range(SIZES[name]) for name in names)) if any(s)]
        hops = lambda s: sum(min(d, SIZES[name] - d) for d, name in zip(s, names))
        steps.sort(key=hops, reverse=True)
        return [{name: lax.rem(me[name] + d, SIZES[name]) for d, name in zip(s, names)} for s in steps]

    peers_a, peers_b, peers_z, peers_zy = peers("y", "x"), peers("z", "c"), peers("z"), peers("z", "y")

    barrier = pltpu.get_barrier_semaphore()
    for peer in peers_a + peers_b:
        pl.semaphore_signal(barrier, inc=1, device_id=peer, device_id_type=MESH)

    def send(src, dst, key, peer):
        pltpu.make_async_remote_copy(
            src_ref=src, dst_ref=dst, send_sem=send_sem.at[key], recv_sem=recv_sem.at[key],
            device_id=peer, device_id_type=MESH,
        ).start()

    def gather(buf, own, key, peers):
        for peer in peers:
            send(buf.at[own], buf.at[own], key, peer)

    def arrived(buf, key, count):
        view = buf.at[pl.ds(0, count)]
        pltpu.make_async_copy(view, view, recv_sem.at[key]).wait()

    def sent(buf, key, count):
        view = buf.at[pl.ds(0, count)]
        pltpu.make_async_copy(view, view, send_sem.at[key]).wait()

    sub = iota((8, LANES), 0)
    lane = iota((8, LANES), 1)

    loads[LD_RES].wait()
    loads[LD_W].wait()

    def products(q, accs):
        accs = list(accs)
        for u in range(8):
            off = pl.multiple_of((q * 8 + u) * LANES, LANES)
            r = res[:, pl.ds(off, LANES)]
            rw = r * jnp.broadcast_to(w[pl.ds(q * 8 + u, 1), :], (8, LANES))
            wres[:, pl.ds(off, LANES)] = rw
            accs[0] = accs[0] + rw * r
            for s in range(1, 5):
                accs[s] = accs[s] + rw * pltpu.roll(r, s, 0)
        return tuple(accs)

    zero = jnp.zeros((8, LANES), F32)
    accs = lax.fori_loop(0, blocks // 8, products, (zero,) * 5)
    placed = zero
    for s in range(5):
        total = jnp.sum(accs[s], axis=1, keepdims=True)
        placed = jnp.where(lane == 8 * s + sub, total, placed)
    int0_a[own_a] = sublane_total(placed)[0:1, :]

    batches = 64
    loads[LD_BASIS].wait()

    def place(b, parts, k01, k2):
        k01 = jnp.where(lane == b, parts[0], k01)
        k01 = jnp.where(lane == b + batches, parts[1], k01)
        return k01, jnp.where(lane == b + jnp.where(sub >= 4, batches, 0), parts[2], k2)

    def batch_spans(b):
        return [pl.ds(pl.multiple_of((2 * b + h) * LANES, LANES), LANES) for h in range(2)]

    def chunk_moments(chunk):
        def one(b, carry):
            carry = list(carry)
            offs = batch_spans(b)
            tiles = [[basis[kt * 8:kt * 8 + 8, off] for off in offs] for kt in range(3)]
            for n in range(2):
                i = 2 * chunk + n
                field = [jnp.broadcast_to(wres[i:i + 1, off], (8, LANES)) for off in offs]
                parts = [
                    jnp.sum(tiles[kt][0] * field[0] + tiles[kt][1] * field[1], axis=1, keepdims=True)
                    for kt in range(3)
                ]
                carry[2 * n], carry[2 * n + 1] = place(b, parts, carry[2 * n], carry[2 * n + 1])
            return tuple(carry)

        return lax.fori_loop(0, batches, one, (zero,) * 4, unroll=8)

    def last_harmonic(b, placed):
        offs = batch_spans(b)
        last = [wres[:, off] * jnp.broadcast_to(basis[24:25, off], (8, LANES)) for off in offs]
        return jnp.where(lane == b, jnp.sum(last[0] + last[1], axis=1, keepdims=True), placed)

    def put_moments(buf, at, k01, k2):
        buf[(*at, slice(0, 8))] = k01
        buf[(*at, slice(8, 12))] = (k2 + pltpu.roll(k2, 4, 0))[0:4]

    def fill_chunk(chunk):
        found = chunk_moments(chunk)
        for n in range(2):
            put_moments(hist_a[chunk], (own_a, n), found[2 * n], found[2 * n + 1])

    loads[LD_ATOM].wait()
    atom_wide = jnp.concatenate([atom[...], atom[...]], axis=1)
    atom_a[own_a] = atom_wide
    atom_b[own_b] = atom_wide
    fill_chunk(0)

    pl.semaphore_wait(barrier, len(peers_a) + len(peers_b))
    gather(int0_a, own_a, INT0_A, peers_a)
    gather(atom_a, own_a, ATOM_A, peers_a)
    gather(atom_b, own_b, ATOM_B, peers_b)
    gather(hist_a[0], own_a, HIST_0, peers_a)
    for chunk in range(1, 4):
        if chunk == 3:
            last = lax.fori_loop(0, batches, last_harmonic, zero, unroll=8)
            last = jnp.where(lane < batches, last, pltpu.roll(pltpu.roll(last, 4, 0), batches, 1))
            last_a[own_a] = last[0:4]
            gather(last_a, own_a, LAST_A, peers_a)
        fill_chunk(chunk)
        gather(hist_a[chunk], own_a, HIST_KEYS[chunk], peers_a)

    loads[LD_OWNER].wait()
    wide_sub = iota((batches, LANES), 0)
    wide_lane = iota((batches, LANES), 1)
    own_lane = wide_lane == wide_sub

    def as_column(row):
        return jnp.sum(jnp.where(own_lane, jnp.broadcast_to(row, (batches, LANES)), 0.0), axis=1, keepdims=True)

    atom_col = as_column(atom_wide.astype(F32))

    def look_up(j, found):
        owners = jnp.broadcast_to(owner[pl.ds(j, 1), :].astype(F32), (batches, LANES))
        number = (wide_lane + j * LANES).astype(F32)
        return found + jnp.where(number == atom_col, owners, 0.0)

    found = lax.fori_loop(0, owner.shape[0], look_up, jnp.zeros((batches, LANES), F32))
    slot_col = jnp.sum(found, axis=1, keepdims=True)
    slot_a[own_a] = jnp.sum(jnp.where(own_lane, slot_col, 0.0), axis=0, keepdims=True).astype(jnp.int32)
    gather(slot_a, own_a, SLOT_A, peers_a)

    def group_sum(buf, key, count=GROUP):
        arrived(buf, key, count - 1)
        total = buf[0]
        for i in range(1, count):
            total = total + buf[i]
        return total

    int0_b[own_b] = group_sum(int0_a, INT0_A)
    gather(int0_b, own_b, INT0_B, peers_b)

    arrived(atom_a, ATOM_A, GROUP - 1)
    arrived(atom_b, ATOM_B, GROUP - 1)
    half = iota((1, LANES), 1) < batches
    atoms_b = [jnp.where(half, atom_b[2 * q], atom_b[2 * q + 1]).astype(F32) for q in range(GROUP // 2)]

    def relate_atoms(s, nothing):
        atoms_a = as_column(atom_a[s].astype(F32))
        at = pl.ds(pl.multiple_of(s * batches, batches), batches)
        for q in range(GROUP // 2):
            cols = pl.ds(q * LANES, LANES)
            same_atom[at, cols] = jnp.where(atoms_a == atoms_b[q], 1.0, 0.0).astype(jnp.bfloat16)
        return nothing

    lax.fori_loop(0, GROUP, relate_atoms, 0)

    def spread(tiles):
        for bit in (4, 2, 1):
            low = (sub & bit) == 0
            swapped = list(tiles)
            for j in range(8):
                if not j & bit:
                    first, second = tiles[j], tiles[j | bit]
                    swapped[j] = jnp.where(low, first, pltpu.roll(second, bit, 0))
                    swapped[j | bit] = jnp.where(low, pltpu.roll(first, 8 - bit, 0), second)
            tiles = swapped
        return tiles

    def block_span(g, r):
        j = 2 * (8 * (g & 7) + r) + (g >> 3)
        return pl.ds(pl.multiple_of(j * LANES, LANES), LANES)

    def group_rows(g):
        return pl.ds(pl.multiple_of(g * 8, 8), 8)

    def turn_rows(src, start, dst):
        def collect(g, nothing):
            for k, tile in enumerate(spread([src[start:start + 8, block_span(g, r)] for r in range(8)])):
                rows8[k, group_rows(g), :] = tile
            return nothing

        lax.fori_loop(0, blocks // 8, collect, 0, unroll=2)

        def turn(k, nothing):
            dst[start + k] = rows8[k].T
            return nothing

        lax.fori_loop(0, 8, turn, 0, unroll=2)

    def by_half(ref):
        return jnp.concatenate([ref[pl.ds(0, blocks // 2, stride=2), :], ref[pl.ds(1, blocks // 2, stride=2), :]], axis=0)

    for start in range(0, 24, 8):
        turn_rows(basis, start, basis_t)

    def last_row(q, nothing):
        for u in range(8):
            at = (u % 2) * (blocks // 2) + q * 4 + u // 2
            mixed[pl.ds(at, 1), :] = basis[24:25, pl.ds(pl.multiple_of((q * 8 + u) * LANES, LANES), LANES)]
        return nothing

    lax.fori_loop(0, blocks // 8, last_row, 0)
    basis_t[24] = mixed[...].T
    w_t[...] = by_half(w).T

    def entry_values(row, count):
        rows = iota((count, LANES), 0)
        lanes = iota((count, LANES), 1)
        total = jnp.sum(jnp.where(rows == lanes, jnp.broadcast_to(row, (count, LANES)), 0.0), axis=1, keepdims=True)
        return jnp.broadcast_to(total, (count, LANES))

    def splat(base, i):
        return jnp.broadcast_to(entries[pl.ds(base + i, 1), :], (8, LANES))

    def left_sides(block_of):
        is_low = iota((ROWS, LANES), 1) < batches
        lows, highs = [], []
        for q in range(GROUP // 2):
            first, second = block_of(2 * q), block_of(2 * q + 1)
            lows.append(jnp.where(is_low, first, pltpu.roll(second, batches, 1)))
            highs.append(jnp.where(is_low, pltpu.roll(first, batches, 1), second))
        pad = jnp.zeros((16 - ROWS, GROUP * batches), F32)
        low = jnp.concatenate(lows, axis=1)
        high = jnp.concatenate(highs, axis=1)
        return three_parts(jnp.concatenate([low, pad, high, pad], axis=0))

    def contributions(parts, matrix, out):
        result = jnp.dot(parts, matrix[...], preferred_element_type=F32)
        pack_contributions(result[0:32] + result[32:64] + result[64:96], out)

    def pack_contributions(result, out):
        is_low = iota((ROWS, LANES), 1) < batches
        for q in range(GROUP // 2):
            cols = slice(q * LANES, (q + 1) * LANES)
            low, high = result[0:ROWS, cols], result[16:16 + ROWS, cols]
            out[2 * q] = jnp.where(is_low, low, pltpu.roll(high, batches, 1))
            out[2 * q + 1] = jnp.where(is_low, pltpu.roll(low, batches, 1), high)

    def scatter(out, buf, key):
        buf[own_b] = out[own_b]
        for peer in peers_b:
            send(out.at[peer.get("c") * 8 + peer.get("z")], buf.at[own_b], key, peer)

    def packed_scale(rows):
        r, c = iota((rows, LANES), 0), iota((rows, LANES), 1)
        high = c >= batches
        k = jnp.where(r < 8, jnp.where(high, r + 8, r), jnp.where(high, r + 12, r + 8))
        k = jnp.where(r == 12, 24, k)
        degree = (
            jnp.where(k >= 1, 1, 0) + jnp.where(k >= 4, 1, 0) + jnp.where(k >= 9, 1, 0) + jnp.where(k >= 16, 1, 0)
        )
        return 1.0 / (1.0 + degree.astype(F32))

    moment_scale = 1.0 / 32.0

    def folded(tiles):
        for bit in (4, 2, 1):
            low = (sub & bit) == 0
            count = len(tiles) // 2
            merged = []
            for first, second in zip(tiles[:count], tiles[count:]):
                given = jnp.where(low, second, first)
                if bit == 4:
                    given = pltpu.roll(given, 4, 0)
                else:
                    given = jnp.where(low, pltpu.roll(given, 8 - bit, 0), pltpu.roll(given, bit, 0))
                merged.append(jnp.where(low, first, second) + given)
            tiles = merged
        return tiles[0]

    def mix_history(column):
        def eight(g, nothing):
            offs = [block_span(g, r) for r in range(8)]
            mixed[group_rows(g), :] = folded([column * (rho[:, off] + MIX_BETA * res[:, off]) for off in offs])
            return nothing

        lax.fori_loop(0, blocks // 8, eight, 0, unroll=2)
        return mixed[...].T

    whole_half = lane < batches

    def correct_density(total):
        total = total * (packed_scale(ROWS) * (MIX_BETA * moment_scale))
        first = total[0:8]
        turned = pltpu.roll(first, batches, 1)
        rest = jnp.concatenate([total[8:13], jnp.zeros((3, LANES), F32)], axis=0)
        rest_turned = pltpu.roll(rest, batches, 1)
        low = jnp.where(whole_half, rest, rest_turned)
        high = jnp.where(whole_half, rest_turned, rest)
        coef[0:8] = jnp.where(whole_half, first, turned)
        coef[8:16] = jnp.where(whole_half, turned, first)
        coef[16:24] = jnp.where(sub < 4, low, pltpu.roll(high, 4, 0))
        coef[24:25] = low[4:5]
        factors = [jnp.broadcast_to(coef[k:k + 1, :], (8, LANES)) for k in range(25)]
        found = []
        for v in range(blocks // 8):
            rows = slice(8 * v, 8 * v + 8)
            value = factors[0] * basis_t[0, rows]
            for k in range(1, 25):
                value = value + factors[k] * basis_t[k, rows]
            found.append(mixed_t[rows] - value)
            den_t[rows] = found[-1]
        return found

    def add_up(terms):
        while len(terms) > 1:
            terms = [sum(terms[n:n + 2][1:], terms[n]) for n in range(0, len(terms), 2)]
        return terms[0]

    def new_moments(dense, where):
        spans = [slice(8 * v, 8 * v + 8) for v in range(blocks // 8)]
        fresh, weighted = [], []
        for rows, value in zip(spans, dense):
            fresh.append(target_t[rows] + coupling_t[rows] * jnp.tanh(value) - value)
            fresh_t[rows] = fresh[-1]
            weighted.append(fresh[-1] * w_t[rows])

        def both_halves(x):
            return x + pltpu.roll(x, batches, 1)

        sums = [add_up([x * basis_t[k, rows] for x, rows in zip(weighted, spans)]) for k in range(25)]
        k0, k1, k2 = (both_halves(folded(sums[kt * 8:kt * 8 + 8])) for kt in range(3))
        k3 = both_halves(sublane_total(sums[24]))[0:1]
        itself = add_up([x * y for x, y in zip(weighted, fresh)])
        sums = [
            jnp.where(where == i, itself, add_up([x * res_t[i, rows] for x, rows in zip(weighted, spans)]))
            for i in range(HIST)
        ]
        total = jnp.sum(folded(sums), axis=1, keepdims=True)
        row = sublane_total(jnp.where(lane == sub + batches, total, 0.0))[0:1, :]
        new_a[own_a, 0:8] = jnp.where(whole_half, k0, k1)
        new_a[own_a, 8:12] = jnp.where(whole_half, k2, pltpu.roll(k2, 4, 0))[0:4]
        new_a[own_a, 12:13] = jnp.where(half, k3, row)

    row = group_sum(int0_b, INT0_B)
    entries[0:40, :] = entry_values(row, 40)

    def pair(i, j):
        s = (i - j) % 8
        return splat(0, 8 * s + i) if s <= 4 else splat(0, 8 * ((j - i) % 8) + j)

    weights0 = mixing_weights([[pair(i, j) for j in range(i + 1)] for i in range(HIST)])
    column0 = history_column(weights0)

    def history_block(i, s):
        row = last_a[s, i % 4:i % 4 + 1]
        return jnp.concatenate([hist_a[i // 2][s, i % 2], row if i < 4 else pltpu.roll(row, batches, 1)], axis=0)

    def mixed_block(values, packed, s):
        total = jnp.broadcast_to(values[0][0:1], (ROWS - 1, LANES)) * hist_a[0][s, 0]
        for i in range(1, HIST):
            total = total + jnp.broadcast_to(values[i][0:1], (ROWS - 1, LANES)) * hist_a[i // 2][s, i % 2]
        last = packed * last_a[s]
        last = last[0:1] + last[1:2] + last[2:3] + last[3:4]
        return jnp.concatenate([total, last + pltpu.roll(last, batches, 1)], axis=0)

    for chunk in range(4):
        arrived(hist_a[chunk], HIST_KEYS[chunk], GROUP - 1)
    arrived(last_a, LAST_A, GROUP - 1)
    packed0 = jnp.where(lane < batches, column0, pltpu.roll(column0, 4, 0))[0:4]
    contributions(left_sides(lambda s: mixed_block(weights0, packed0, s)), same_atom, send0)
    scatter(send0, pb0_b, PB0_B)
    loads[LD_RHO].wait()
    loads[LD_TARGET].wait()
    loads[LD_COUPLING].wait()
    loads[LD_INDEX].wait()
    mixed_t[...] = mix_history(column0)
    target_t[...] = by_half(t).T
    coupling_t[...] = by_half(cpl).T
    turn_rows(res, 0, res_t)

    arrived(slot_a, SLOT_A, GROUP - 1)
    place_of = iota((GROUP * 16, LANES), 0)
    number = me["x"] * (GROUP * batches) + me["y"] * 4
    number = number + (place_of >> 7) * 512 + ((place_of >> 4) & 7) * 16 + ((place_of >> 2) & 3) * LANES + (place_of & 3)
    for q in range(GROUP // 2):
        slots = jnp.where(half, slot_a[2 * q], pltpu.roll(slot_a[2 * q + 1], batches, 1))
        owned_slot[:, q * LANES:(q + 1) * LANES] = jnp.where(number == slots, 1.0, 0.0).astype(jnp.bfloat16)

    def slot_sums(parts):
        return lax.dot_general(owned_slot[...], parts, (((1,), (1,)), ((), ())), preferred_element_type=F32)

    for i in range(HIST):
        parts = left_sides(lambda s: history_block(i, s))
        for part in range(3):
            sides8[part * 256 + i * 32:part * 256 + i * 32 + 32, :] = parts[part * 32:part * 32 + 32]
    sums = slot_sums(sides8[...])
    sums = sums[:, 0:256] + sums[:, 256:512] + sums[:, 512:768]
    for p in range(GROUP):
        send_old[p] = sums[p * 16:p * 16 + 16]
    other = 1 - me["c"]
    send(send_old.at[pl.ds(other * 8, 8)], old_c, OLD_C, {"c": other})
    pb0_total = group_sum(pb0_b, PB0_B)

    where = slot_index[0]
    new_moments(correct_density(pb0_total), where)
    gather(new_a, own_a, NEW_A, peers_a)

    arrived(old_c, OLD_C, 8)
    for z in range(8):
        mine_old[z] = send_old[me["c"] * 8 + z] + old_c[z]
    old_z[me["z"]] = mine_old[me["z"]]
    for peer in peers_z:
        send(mine_old.at[peer["z"]], old_z.at[me["z"]], OLD_Z, peer)

    for n in range(4):
        cols = slice(n * 256, n * 256 + 256)
        out = jnp.dot(sides8[...], same_atom[:, cols], preferred_element_type=F32)
        old_out[:, cols] = out[0:256] + out[256:512] + out[512:768]

    arrived(new_a, NEW_A, GROUP - 1)
    row = new_a[0, 12:13]
    for s in range(1, GROUP):
        row = row + new_a[s, 12:13]
    int1_b[own_b] = pltpu.roll(row, batches, 1)
    gather(int1_b, own_b, INT1_B, peers_b)
    fresh_parts = left_sides(lambda s: new_a[s])
    part_of = lane >> 5

    def every_part(x):
        x = x + pltpu.roll(x, 64, 1)
        return x + pltpu.roll(x, 32, 1)

    def packed_slots(low, high):
        return jnp.where(
            part_of < 2,
            jnp.where(part_of == 0, low, pltpu.roll(low, 4, 0)),
            jnp.where(part_of == 2, high, pltpu.roll(high, 4, 0)),
        )[0:4]

    fresh_sums = slot_sums(jnp.concatenate([fresh_parts, jnp.zeros((32, GROUP * batches), jnp.bfloat16)], axis=0))
    for p in range(GROUP):
        send_fresh[p] = packed_slots(
            every_part(fresh_sums[p * 16:p * 16 + 8]), every_part(fresh_sums[p * 16 + 8:p * 16 + 16])
        )
    scatter(send_fresh, fresh_b, FRESH_B)
    out = jnp.dot(fresh_parts, same_atom[...], preferred_element_type=F32)
    fresh_out[...] = out[0:32] + out[32:64] + out[64:96]
    old_total = group_sum(old_z, OLD_Z, 8)
    row = group_sum(int1_b, INT1_B)
    entries[40:48, :] = entry_values(row, 8)
    fresh_row = [splat(40, i) for i in range(HIST)]
    weights1 = mixing_weights([
        [jnp.where(where == i, fresh_row[j], jnp.where(where == j, fresh_row[i], pair(i, j))) for j in range(i + 1)]
        for i in range(HIST)
    ])

    kept = [jnp.where(where == i, 0.0, weights1[i]) for i in range(HIST)]
    fresh_weight = jnp.where(where == 0, weights1[0], 0.0)
    for i in range(1, HIST):
        fresh_weight = fresh_weight + jnp.where(where == i, weights1[i], 0.0)
    is_low = lane < batches
    for q in range(GROUP // 2):
        cols = slice(q * LANES, (q + 1) * LANES)
        tiles = []
        for r in range(4):
            tile = fresh_weight * fresh_out[8 * r:8 * r + 8, cols]
            for i in range(HIST):
                tile = tile + kept[i] * old_out[i * 32 + 8 * r:i * 32 + 8 * r + 8, cols]
            tiles.append(tile)
        for low, high, rows in ((tiles[0], tiles[2], 8), (tiles[1], tiles[3], ROWS - 8)):
            at = slice(0, 8) if rows == 8 else slice(8, ROWS)
            send1[2 * q, at] = jnp.where(is_low, low, pltpu.roll(high, batches, 1))[0:rows]
            send1[2 * q + 1, at] = jnp.where(is_low, pltpu.roll(low, batches, 1), high)[0:rows]
    scatter(send1, pb1_b, PB1_B)

    lower = kept[3]
    upper = kept[7]
    for n in range(3):
        lower = jnp.where(part_of == n, kept[n], lower)
        upper = jnp.where(part_of == n, kept[n + 4], upper)
    fresh_total = group_sum(fresh_b, FRESH_B)
    owned = []
    for n in range(2):
        rows = slice(8 * n, 8 * n + 8)
        value = old_total[rows, 0:LANES] * lower + old_total[rows, LANES:2 * LANES] * upper
        owned.append(every_part(value))
    piece = (packed_slots(*owned) + fresh_total * fresh_weight[0:4]) * moment_scale
    own_zy = me["z"] * 4 + me["y"]
    mom_zy[own_zy] = piece
    gather(mom_zy, own_zy, MOM_ZY, peers_zy)

    mixed_t[...] = mix_history(history_column(kept)) + jnp.broadcast_to(fresh_weight[0:1], (blocks, LANES)) * (
        den_t[...] + MIX_BETA * fresh_t[...]
    )
    correct_density(group_sum(pb1_b, PB1_B))
    by_block = den_t[...].T
    den[pl.ds(0, blocks // 2, stride=2), :] = by_block[0:blocks // 2]
    den[pl.ds(1, blocks // 2, stride=2), :] = by_block[blocks // 2:blocks]
    arrived(mom_zy, MOM_ZY, len(peers_zy))
    by_slot = jnp.concatenate([mom_zy[p] for p in range(32)], axis=0).T
    for g in range(4):
        cols, at = slice(g * LANES, (g + 1) * LANES), g * 32
        mom[0:8, cols] = by_slot[at:at + 8]
        mom[8:16, cols] = by_slot[at + 16:at + 24]
        mom[16:20, cols] = by_slot[at + 8:at + 12]
        mom[20:24, cols] = by_slot[at + 24:at + 28]
        mom[24:25, cols] = by_slot[at + 12:at + 13]

    for buf, key, count in (
        (int0_a, INT0_A, 15), (int0_b, INT0_B, 15), (atom_a, ATOM_A, 15), (atom_b, ATOM_B, 15),
        (slot_a, SLOT_A, 15), (hist_0, HIST_0, 15), (hist_1, HIST_1, 15), (hist_2, HIST_2, 15), (hist_3, HIST_3, 15),
        (last_a, LAST_A, 15),
        (new_a, NEW_A, 15), (int1_b, INT1_B, 15),
        (pb0_b, PB0_B, 15), (pb1_b, PB1_B, 15), (old_c, OLD_C, 8), (old_z, OLD_Z, 7), (fresh_b, FRESH_B, 15), (mom_zy, MOM_ZY, 31),
    ):
        sent(buf, key, count)


def hand_over(den, mom, den_h, mom_h, sem):
    copies = [pltpu.make_async_copy(den, den_h, sem.at[0]), pltpu.make_async_copy(mom, mom_h, sem.at[1])]
    for copy in copies:
        copy.start()
    for copy in copies:
        copy.wait()


def local(weights, target, coupling, basis, rho_hist, res_hist, batch_atom, owner_slot, slot_index):
    points = weights.shape[0]
    blocks = points // LANES
    harmonics = basis.shape[0]
    batches = batch_atom.shape[0]
    slots = owner_slot.shape[0]
    dense = lambda x: x.reshape(blocks, LANES)
    operands = (
        dense(weights), dense(target), dense(coupling), basis, rho_hist, res_hist,
        batch_atom.reshape(1, batches), owner_slot.reshape(slots // LANES, LANES), slot_index,
    )
    hbm = pl.BlockSpec(memory_space=pltpu.HBM)
    vmem = pl.BlockSpec(memory_space=pltpu.VMEM)
    dense_rows = lambda: pltpu.VMEM((blocks, LANES), F32)
    small = lambda dtype: pltpu.VMEM((GROUP, 1, LANES), dtype)
    pair_block = lambda: pltpu.VMEM((GROUP, 2, ROWS - 1, LANES), F32)
    block = lambda count: pltpu.VMEM((count, ROWS, LANES), F32)
    relation = pltpu.VMEM((GROUP * batches, GROUP * batches), jnp.bfloat16)
    density, moments = pl.pallas_call(
        body,
        out_shape=(
            jax.ShapeDtypeStruct((blocks, LANES), F32),
            jax.ShapeDtypeStruct((harmonics, slots // 8), F32),
        ),
        in_specs=[hbm] * len(operands),
        out_specs=(vmem, vmem),
        scratch_shapes=[
            pltpu.VMEM((blocks, LANES), F32),
            pltpu.VMEM((blocks, LANES), F32),
            pltpu.VMEM((blocks, LANES), F32),
            pltpu.VMEM((harmonics, points), F32),
            pltpu.VMEM((HIST, points), F32),
            pltpu.VMEM((HIST, points), F32),
            pltpu.VMEM((HIST, points), F32),
            pltpu.VMEM((1, batches), jnp.int32),
            pltpu.VMEM((slots // LANES, LANES), jnp.int32),
            pltpu.VMEM((8, blocks, LANES), F32),
            dense_rows(), dense_rows(), dense_rows(), dense_rows(), dense_rows(), dense_rows(), dense_rows(),
            pltpu.VMEM((harmonics, blocks, LANES), F32),
            pltpu.VMEM((HIST, blocks, LANES), F32),
            pltpu.VMEM((32, LANES), F32),
            pltpu.SMEM((2,), jnp.int32),
            pltpu.VMEM((48, LANES), F32),
            relation,
            pltpu.VMEM((GROUP * 16, GROUP * batches), jnp.bfloat16),
            pltpu.VMEM((HIST * 3 * 32, GROUP * batches), jnp.bfloat16),
            pltpu.VMEM((HIST * 32, GROUP * batches), F32),
            pltpu.VMEM((32, GROUP * batches), F32),
            small(F32), small(F32), small(F32), small(jnp.int32), small(jnp.int32), small(jnp.int32),
            pair_block(), pair_block(), pair_block(), pair_block(),
            pltpu.VMEM((GROUP, 4, LANES), F32),
            block(GROUP), block(GROUP), block(GROUP),
            pltpu.VMEM((8, 16, 2 * LANES), F32),
            pltpu.VMEM((8, 16, 2 * LANES), F32),
            pltpu.VMEM((GROUP, 4, LANES), F32),
            pltpu.VMEM((32, 4, LANES), F32),
            block(GROUP), block(GROUP),
            pltpu.VMEM((GROUP, 16, 2 * LANES), F32),
            pltpu.VMEM((8, 16, 2 * LANES), F32),
            pltpu.VMEM((GROUP, 4, LANES), F32),
            pltpu.SemaphoreType.DMA((LOCALS,)),
            pltpu.SemaphoreType.DMA((EXCHANGES,)),
            pltpu.SemaphoreType.DMA((EXCHANGES,)),
        ],
        compiler_params=pltpu.CompilerParams(collective_id=0, has_side_effects=True, vmem_limit_bytes=24 << 20),
    )(
        *(pltpu.with_memory_space_constraint(x, pltpu.HBM) for x in operands)
    )
    density, moments = pl.pallas_call(
        hand_over,
        out_shape=(
            jax.ShapeDtypeStruct((blocks, LANES), F32),
            jax.ShapeDtypeStruct((harmonics, slots // 8), F32),
        ),
        in_specs=[vmem, vmem],
        out_specs=(hbm, hbm),
        scratch_shapes=[pltpu.SemaphoreType.DMA((2,))],
        compiler_params=pltpu.CompilerParams(vmem_limit_bytes=1 << 20),
    )(density, moments)
    return density.reshape(points), moments


def solution(mesh):
    torus = Mesh(mesh.devices.reshape(tuple(SIZES.values())), AXES)
    points = P(AXES)
    rows = P(None, AXES)
    return jax.shard_map(
        local,
        mesh=torus,
        in_specs=(points, points, points, rows, rows, rows, points, P(), P()),
        out_specs=(points, P(None, ("x", "c"))),
        check_vma=False,
    )
```

```python
import itertools

import jax
import jax.numpy as jnp
from jax import lax
from jax.experimental import pallas as pl
from jax.experimental.pallas import tpu as pltpu
from jax.sharding import Mesh
from jax.sharding import PartitionSpec as P

AXES = ("z", "y", "x", "c")
SIZES = {"z": 8, "y": 4, "x": 4, "c": 2}
HIST = 8
LANES = 128
MESH = pl.DeviceIdType.MESH
F32 = jnp.float32
MIX_BETA = 0.5
RIDGE_SHARE = 0.1
GROUP = 16
ROWS = 13
INT0_A, INT0_B, ATOM_A, ATOM_B, SLOT_A, HIST_0, HIST_1, HIST_2, HIST_3, LAST_A, NEW_A, INT1_B, PB0_B, PB1_B, OLD_C, OLD_Z, FRESH_B, MOM_ZY, ON_A = range(19)
EXCHANGES = 19
HIST_KEYS = (HIST_0, HIST_1, HIST_2, HIST_3)
LD_RES, LD_W, LD_ATOM, LD_OWNER, LD_BASIS, LD_RHO, LD_TARGET, LD_COUPLING, LD_INDEX = range(9)
LOCALS = 9


def iota(shape, dim):
    return lax.broadcasted_iota(jnp.int32, shape, dim)


def sublane_total(x):
    x = x + pltpu.roll(x, 4, 0)
    x = x + pltpu.roll(x, 2, 0)
    return x + pltpu.roll(x, 1, 0)


def mixing_weights(entry):
    matrix = [[entry[i][j] for j in range(i + 1)] for i in range(HIST)]
    trace = matrix[0][0]
    for i in range(1, HIST):
        trace = trace + matrix[i][i]
    ridge = trace * (RIDGE_SHARE / HIST)
    for i in range(HIST):
        matrix[i][i] = matrix[i][i] + ridge
    forward = [jnp.ones((8, LANES), F32) for _ in range(HIST)]
    pivot = [None] * HIST
    lower = [[None] * HIST for _ in range(HIST)]
    for j in range(HIST):
        pivot[j] = 1.0 / matrix[j][j]
        for i in range(j + 1, HIST):
            ratio = matrix[i][j] * pivot[j]
            for k in range(j + 1, i + 1):
                matrix[i][k] = matrix[i][k] - ratio * matrix[k][j]
            forward[i] = forward[i] - ratio * forward[j]
            lower[i][j] = ratio
    solved = [None] * HIST
    for i in reversed(range(HIST)):
        value = forward[i] * pivot[i]
        for k in range(i + 1, HIST):
            value = value - lower[k][i] * solved[k]
        solved[i] = value
    total = solved[0]
    for i in range(1, HIST):
        total = total + solved[i]
    scale = 1.0 / total
    return [value * scale for value in solved]


def history_column(values):
    sub = iota((8, LANES), 0)
    column = jnp.zeros((8, LANES), F32)
    for i in range(HIST):
        column = jnp.where(sub == i, values[i], column)
    return column


def three_parts(x):
    high = x.astype(jnp.bfloat16)
    rest = x - high.astype(F32)
    middle = rest.astype(jnp.bfloat16)
    low = (rest - middle.astype(F32)).astype(jnp.bfloat16)
    return jnp.concatenate([high, middle, low], axis=0)


def body(
    w_h, t_h, cpl_h, basis_h, rho_h, res_h, atom_h, owner_h, index_h,
    den, mom,
    w, t, cpl, basis, rho, res, wres, atom, owner, rows8, mixed, w_t, target_t, coupling_t, mixed_t, den_t, fresh_t, basis_t, res_t, coef, slot_index,
    entries, same_atom, owned_slot, sides8, old_out, fresh_out,
    int0_a, int0_b, int1_b, atom_a, atom_b, slot_a,
    hist_0, hist_1, hist_2, hist_3, last_a, new_a, pb0_b, pb1_b, old_c, old_z, fresh_b, mom_zy, send0, send1, send_old, mine_old, send_fresh,
    local_sem, send_sem, recv_sem,
):
    me = {name: lax.axis_index(name) for name in AXES}
    own_a = me["y"] * 4 + me["x"]
    hist_a = (hist_0, hist_1, hist_2, hist_3)
    own_b = me["c"] * 8 + me["z"]
    blocks = w.shape[0]

    loads = {}

    def load(*copies):
        for key, src, dst in copies:
            loads[key] = pltpu.make_async_copy(src, dst, local_sem.at[key])
            loads[key].start()

    load((LD_RES, res_h, res), (LD_W, w_h, w), (LD_BASIS, basis_h, basis), (LD_ATOM, atom_h, atom))

    def steps_along(*names):
        steps = [s for s in itertools.product(*(range(SIZES[name]) for name in names)) if any(s)]
        hops = lambda s: sum(min(d, SIZES[name] - d) for d, name in zip(s, names))
        return sorted(steps, key=hops, reverse=True)

    def peers(*names):
        return [
            {name: lax.rem(me[name] + d, SIZES[name]) for d, name in zip(s, names)} for s in steps_along(*names)
        ]

    peers_a, peers_b, peers_z, peers_zy = peers("y", "x"), peers("z", "c"), peers("z"), peers("z", "y")
    peers_near = [peer for peer, step in zip(peers_a, steps_along("y", "x")) if step[1] != 2]

    barrier = pltpu.get_barrier_semaphore()
    for peer in peers_a + peers_b:
        pl.semaphore_signal(barrier, inc=1, device_id=peer, device_id_type=MESH)
    load(
        (LD_OWNER, owner_h, owner), (LD_RHO, rho_h, rho), (LD_TARGET, t_h, t), (LD_COUPLING, cpl_h, cpl),
        (LD_INDEX, index_h, slot_index),
    )

    def send(src, dst, key, peer):
        pltpu.make_async_remote_copy(
            src_ref=src, dst_ref=dst, send_sem=send_sem.at[key], recv_sem=recv_sem.at[key],
            device_id=peer, device_id_type=MESH,
        ).start()

    def gather(buf, own, key, peers):
        for peer in peers:
            send(buf.at[own], buf.at[own], key, peer)

    def arrived(buf, key, count):
        view = buf.at[pl.ds(0, count)]
        pltpu.make_async_copy(view, view, recv_sem.at[key]).wait()

    def sent(buf, key, count):
        view = buf.at[pl.ds(0, count)]
        pltpu.make_async_copy(view, view, send_sem.at[key]).wait()

    sub = iota((8, LANES), 0)
    lane = iota((8, LANES), 1)

    loads[LD_RES].wait()
    loads[LD_W].wait()

    def products(q, accs):
        accs = list(accs)
        for u in range(8):
            off = pl.multiple_of((q * 8 + u) * LANES, LANES)
            r = res[:, pl.ds(off, LANES)]
            rw = r * jnp.broadcast_to(w[pl.ds(q * 8 + u, 1), :], (8, LANES))
            wres[:, pl.ds(off, LANES)] = rw
            accs[0] = accs[0] + rw * r
            for s in range(1, 5):
                accs[s] = accs[s] + rw * pltpu.roll(r, s, 0)
        return tuple(accs)

    zero = jnp.zeros((8, LANES), F32)
    accs = lax.fori_loop(0, blocks // 8, products, (zero,) * 5)
    placed = zero
    for s in range(5):
        total = jnp.sum(accs[s], axis=1, keepdims=True)
        placed = jnp.where(lane == 8 * s + sub, total, placed)
    int0_a[own_a] = sublane_total(placed)[0:1, :]

    batches = 64
    loads[LD_BASIS].wait()

    def place(b, parts, k01, k2):
        k01 = jnp.where(lane == b, parts[0], k01)
        k01 = jnp.where(lane == b + batches, parts[1], k01)
        return k01, jnp.where(lane == b + jnp.where(sub >= 4, batches, 0), parts[2], k2)

    def batch_spans(b):
        return [pl.ds(pl.multiple_of((2 * b + h) * LANES, LANES), LANES) for h in range(2)]

    def chunk_moments(chunk):
        def one(b, carry):
            carry = list(carry)
            offs = batch_spans(b)
            tiles = [[basis[kt * 8:kt * 8 + 8, off] for off in offs] for kt in range(3)]
            for n in range(2):
                i = 2 * chunk + n
                field = [jnp.broadcast_to(wres[i:i + 1, off], (8, LANES)) for off in offs]
                parts = [
                    jnp.sum(tiles[kt][0] * field[0] + tiles[kt][1] * field[1], axis=1, keepdims=True)
                    for kt in range(3)
                ]
                carry[2 * n], carry[2 * n + 1] = place(b, parts, carry[2 * n], carry[2 * n + 1])
            return tuple(carry)

        return lax.fori_loop(0, batches, one, (zero,) * 4, unroll=8)

    def last_harmonic(b, placed):
        offs = batch_spans(b)
        last = [wres[:, off] * jnp.broadcast_to(basis[24:25, off], (8, LANES)) for off in offs]
        return jnp.where(lane == b, jnp.sum(last[0] + last[1], axis=1, keepdims=True), placed)

    def put_moments(buf, at, k01, k2):
        buf[(*at, slice(0, 8))] = k01
        buf[(*at, slice(8, 12))] = (k2 + pltpu.roll(k2, 4, 0))[0:4]

    def fill_chunk(chunk):
        found = chunk_moments(chunk)
        for n in range(2):
            put_moments(hist_a[chunk], (own_a, n), found[2 * n], found[2 * n + 1])

    loads[LD_ATOM].wait()
    atom_wide = jnp.concatenate([atom[...], atom[...]], axis=1)
    atom_a[own_a] = atom_wide
    atom_b[own_b] = atom_wide
    fill_chunk(0)

    pl.semaphore_wait(barrier, len(peers_a) + len(peers_b))
    gather(int0_a, own_a, INT0_A, peers_a)
    gather(atom_a, own_a, ATOM_A, peers_a)
    gather(atom_b, own_b, ATOM_B, peers_b)
    gather(hist_a[0], own_a, HIST_0, peers_near)
    for chunk in range(1, 4):
        if chunk == 3:
            last = lax.fori_loop(0, batches, last_harmonic, zero, unroll=8)
            last = jnp.where(lane < batches, last, pltpu.roll(pltpu.roll(last, 4, 0), batches, 1))
            last_a[own_a] = last[0:4]
            gather(last_a, own_a, LAST_A, peers_a)
        fill_chunk(chunk)
        gather(hist_a[chunk], own_a, HIST_KEYS[chunk], peers_a)

    loads[LD_OWNER].wait()
    wide_sub = iota((batches, LANES), 0)
    wide_lane = iota((batches, LANES), 1)
    own_lane = wide_lane == wide_sub

    def as_column(row):
        return jnp.sum(jnp.where(own_lane, jnp.broadcast_to(row, (batches, LANES)), 0.0), axis=1, keepdims=True)

    atom_col = as_column(atom_wide.astype(F32))

    def look_up(j, found):
        owners = jnp.broadcast_to(owner[pl.ds(j, 1), :].astype(F32), (batches, LANES))
        number = (wide_lane + j * LANES).astype(F32)
        return found + jnp.where(number == atom_col, owners, 0.0)

    found = lax.fori_loop(0, owner.shape[0], look_up, jnp.zeros((batches, LANES), F32))
    slot_col = jnp.sum(found, axis=1, keepdims=True)
    slot_a[own_a] = jnp.sum(jnp.where(own_lane, slot_col, 0.0), axis=0, keepdims=True).astype(jnp.int32)
    gather(slot_a, own_a, SLOT_A, peers_a)

    def group_sum(buf, key, count=GROUP):
        arrived(buf, key, count - 1)
        total = buf[0]
        for i in range(1, count):
            total = total + buf[i]
        return total

    int0_b[own_b] = group_sum(int0_a, INT0_A)
    gather(int0_b, own_b, INT0_B, peers_b)

    arrived(hist_0, HIST_0, len(peers_near))
    for y in range(4):
        for n, step in ((0, 1), (1, 3)):
            block_at = hist_0.at[y * 4 + lax.rem(me["x"] + 4 - step, 4), n]
            send(block_at, block_at, ON_A, {"x": lax.rem(me["x"] + step, 4)})

    arrived(atom_a, ATOM_A, GROUP - 1)
    arrived(atom_b, ATOM_B, GROUP - 1)
    half = iota((1, LANES), 1) < batches
    atoms_b = [jnp.where(half, atom_b[2 * q], atom_b[2 * q + 1]).astype(F32) for q in range(GROUP // 2)]

    def relate_atoms(s, nothing):
        atoms_a = as_column(atom_a[s].astype(F32))
        at = pl.ds(pl.multiple_of(s * batches, batches), batches)
        for q in range(GROUP // 2):
            cols = pl.ds(q * LANES, LANES)
            same_atom[at, cols] = jnp.where(atoms_a == atoms_b[q], 1.0, 0.0).astype(jnp.bfloat16)
        return nothing

    lax.fori_loop(0, GROUP, relate_atoms, 0)

    def spread(tiles):
        for bit in (4, 2, 1):
            low = (sub & bit) == 0
            swapped = list(tiles)
            for j in range(8):
                if not j & bit:
                    first, second = tiles[j], tiles[j | bit]
                    swapped[j] = jnp.where(low, first, pltpu.roll(second, bit, 0))
                    swapped[j | bit] = jnp.where(low, pltpu.roll(first, 8 - bit, 0), second)
            tiles = swapped
        return tiles

    def block_span(g, r):
        j = 2 * (8 * (g & 7) + r) + (g >> 3)
        return pl.ds(pl.multiple_of(j * LANES, LANES), LANES)

    def group_rows(g):
        return pl.ds(pl.multiple_of(g * 8, 8), 8)

    def turn_rows(src, start, dst):
        def collect(g, nothing):
            for k, tile in enumerate(spread([src[start:start + 8, block_span(g, r)] for r in range(8)])):
                rows8[k, group_rows(g), :] = tile
            return nothing

        lax.fori_loop(0, blocks // 8, collect, 0, unroll=2)

        def turn(k, nothing):
            dst[start + k] = rows8[k].T
            return nothing

        lax.fori_loop(0, 8, turn, 0, unroll=2)

    def by_half(ref):
        return jnp.concatenate([ref[pl.ds(0, blocks // 2, stride=2), :], ref[pl.ds(1, blocks // 2, stride=2), :]], axis=0)

    for start in range(0, 24, 8):
        turn_rows(basis, start, basis_t)

    def last_row(q, nothing):
        for u in range(8):
            at = (u % 2) * (blocks // 2) + q * 4 + u // 2
            mixed[pl.ds(at, 1), :] = basis[24:25, pl.ds(pl.multiple_of((q * 8 + u) * LANES, LANES), LANES)]
        return nothing

    lax.fori_loop(0, blocks // 8, last_row, 0)
    basis_t[24] = mixed[...].T
    w_t[...] = by_half(w).T

    def entry_values(row, count):
        rows = iota((count, LANES), 0)
        lanes = iota((count, LANES), 1)
        total = jnp.sum(jnp.where(rows == lanes, jnp.broadcast_to(row, (count, LANES)), 0.0), axis=1, keepdims=True)
        return jnp.broadcast_to(total, (count, LANES))

    def splat(base, i):
        return jnp.broadcast_to(entries[pl.ds(base + i, 1), :], (8, LANES))

    def left_sides(block_of):
        is_low = iota((ROWS, LANES), 1) < batches
        lows, highs = [], []
        for q in range(GROUP // 2):
            first, second = block_of(2 * q), block_of(2 * q + 1)
            lows.append(jnp.where(is_low, first, pltpu.roll(second, batches, 1)))
            highs.append(jnp.where(is_low, pltpu.roll(first, batches, 1), second))
        pad = jnp.zeros((16 - ROWS, GROUP * batches), F32)
        low = jnp.concatenate(lows, axis=1)
        high = jnp.concatenate(highs, axis=1)
        return three_parts(jnp.concatenate([low, pad, high, pad], axis=0))

    def contributions(parts, matrix, out):
        result = jnp.dot(parts, matrix[...], preferred_element_type=F32)
        pack_contributions(result[0:32] + result[32:64] + result[64:96], out)

    def pack_contributions(result, out):
        is_low = iota((ROWS, LANES), 1) < batches
        for q in range(GROUP // 2):
            cols = slice(q * LANES, (q + 1) * LANES)
            low, high = result[0:ROWS, cols], result[16:16 + ROWS, cols]
            out[2 * q] = jnp.where(is_low, low, pltpu.roll(high, batches, 1))
            out[2 * q + 1] = jnp.where(is_low, pltpu.roll(low, batches, 1), high)

    def scatter(out, buf, key):
        buf[own_b] = out[own_b]
        for peer in peers_b:
            send(out.at[peer.get("c") * 8 + peer.get("z")], buf.at[own_b], key, peer)

    def packed_scale(rows):
        r, c = iota((rows, LANES), 0), iota((rows, LANES), 1)
        high = c >= batches
        k = jnp.where(r < 8, jnp.where(high, r + 8, r), jnp.where(high, r + 12, r + 8))
        k = jnp.where(r == 12, 24, k)
        degree = (
            jnp.where(k >= 1, 1, 0) + jnp.where(k >= 4, 1, 0) + jnp.where(k >= 9, 1, 0) + jnp.where(k >= 16, 1, 0)
        )
        return 1.0 / (1.0 + degree.astype(F32))

    moment_scale = 1.0 / 32.0

    def folded(tiles):
        for bit in (4, 2, 1):
            low = (sub & bit) == 0
            count = len(tiles) // 2
            merged = []
            for first, second in zip(tiles[:count], tiles[count:]):
                given = jnp.where(low, second, first)
                if bit == 4:
                    given = pltpu.roll(given, 4, 0)
                else:
                    given = jnp.where(low, pltpu.roll(given, 8 - bit, 0), pltpu.roll(given, bit, 0))
                merged.append(jnp.where(low, first, second) + given)
            tiles = merged
        return tiles[0]

    def mix_history(column):
        def eight(g, nothing):
            offs = [block_span(g, r) for r in range(8)]
            mixed[group_rows(g), :] = folded([column * (rho[:, off] + MIX_BETA * res[:, off]) for off in offs])
            return nothing

        lax.fori_loop(0, blocks // 8, eight, 0, unroll=2)
        return mixed[...].T

    whole_half = lane < batches

    def correct_density(total):
        total = total * (packed_scale(ROWS) * (MIX_BETA * moment_scale))
        first = total[0:8]
        turned = pltpu.roll(first, batches, 1)
        rest = jnp.concatenate([total[8:13], jnp.zeros((3, LANES), F32)], axis=0)
        rest_turned = pltpu.roll(rest, batches, 1)
        low = jnp.where(whole_half, rest, rest_turned)
        high = jnp.where(whole_half, rest_turned, rest)
        coef[0:8] = jnp.where(whole_half, first, turned)
        coef[8:16] = jnp.where(whole_half, turned, first)
        coef[16:24] = jnp.where(sub < 4, low, pltpu.roll(high, 4, 0))
        coef[24:25] = low[4:5]
        factors = [jnp.broadcast_to(coef[k:k + 1, :], (8, LANES)) for k in range(25)]
        found = []
        for v in range(blocks // 8):
            rows = slice(8 * v, 8 * v + 8)
            value = factors[0] * basis_t[0, rows]
            for k in range(1, 25):
                value = value + factors[k] * basis_t[k, rows]
            found.append(mixed_t[rows] - value)
            den_t[rows] = found[-1]
        return found

    def add_up(terms):
        while len(terms) > 1:
            terms = [sum(terms[n:n + 2][1:], terms[n]) for n in range(0, len(terms), 2)]
        return terms[0]

    def new_moments(dense, where):
        spans = [slice(8 * v, 8 * v + 8) for v in range(blocks // 8)]
        fresh, weighted = [], []
        for rows, value in zip(spans, dense):
            fresh.append(target_t[rows] + coupling_t[rows] * jnp.tanh(value) - value)
            fresh_t[rows] = fresh[-1]
            weighted.append(fresh[-1] * w_t[rows])

        def both_halves(x):
            return x + pltpu.roll(x, batches, 1)

        sums = [add_up([x * basis_t[k, rows] for x, rows in zip(weighted, spans)]) for k in range(25)]
        k0, k1, k2 = (both_halves(folded(sums[kt * 8:kt * 8 + 8])) for kt in range(3))
        k3 = both_halves(sublane_total(sums[24]))[0:1]
        itself = add_up([x * y for x, y in zip(weighted, fresh)])
        sums = [
            jnp.where(where == i, itself, add_up([x * res_t[i, rows] for x, rows in zip(weighted, spans)]))
            for i in range(HIST)
        ]
        total = jnp.sum(folded(sums), axis=1, keepdims=True)
        row = sublane_total(jnp.where(lane == sub + batches, total, 0.0))[0:1, :]
        new_a[own_a, 0:8] = jnp.where(whole_half, k0, k1)
        new_a[own_a, 8:12] = jnp.where(whole_half, k2, pltpu.roll(k2, 4, 0))[0:4]
        new_a[own_a, 12:13] = jnp.where(half, k3, row)

    row = group_sum(int0_b, INT0_B)
    entries[0:40, :] = entry_values(row, 40)

    def pair(i, j):
        s = (i - j) % 8
        return splat(0, 8 * s + i) if s <= 4 else splat(0, 8 * ((j - i) % 8) + j)

    weights0 = mixing_weights([[pair(i, j) for j in range(i + 1)] for i in range(HIST)])
    column0 = history_column(weights0)

    def history_block(i, s):
        row = last_a[s, i % 4:i % 4 + 1]
        return jnp.concatenate([hist_a[i // 2][s, i % 2], row if i < 4 else pltpu.roll(row, batches, 1)], axis=0)

    def mixed_block(values, packed, s):
        total = jnp.broadcast_to(values[0][0:1], (ROWS - 1, LANES)) * hist_a[0][s, 0]
        for i in range(1, HIST):
            total = total + jnp.broadcast_to(values[i][0:1], (ROWS - 1, LANES)) * hist_a[i // 2][s, i % 2]
        last = packed * last_a[s]
        last = last[0:1] + last[1:2] + last[2:3] + last[3:4]
        return jnp.concatenate([total, last + pltpu.roll(last, batches, 1)], axis=0)

    arrived(hist_0, ON_A, 4)
    for chunk in range(1, 4):
        arrived(hist_a[chunk], HIST_KEYS[chunk], GROUP - 1)
    arrived(last_a, LAST_A, GROUP - 1)
    packed0 = jnp.where(lane < batches, column0, pltpu.roll(column0, 4, 0))[0:4]
    contributions(left_sides(lambda s: mixed_block(weights0, packed0, s)), same_atom, send0)
    scatter(send0, pb0_b, PB0_B)
    loads[LD_RHO].wait()
    loads[LD_TARGET].wait()
    loads[LD_COUPLING].wait()
    loads[LD_INDEX].wait()
    mixed_t[...] = mix_history(column0)
    target_t[...] = by_half(t).T
    coupling_t[...] = by_half(cpl).T
    turn_rows(res, 0, res_t)

    arrived(slot_a, SLOT_A, GROUP - 1)
    place_of = iota((GROUP * 16, LANES), 0)
    number = me["x"] * (GROUP * batches) + me["y"] * 4
    number = number + (place_of >> 7) * 512 + ((place_of >> 4) & 7) * 16 + ((place_of >> 2) & 3) * LANES + (place_of & 3)
    for q in range(GROUP // 2):
        slots = jnp.where(half, slot_a[2 * q], pltpu.roll(slot_a[2 * q + 1], batches, 1))
        owned_slot[:, q * LANES:(q + 1) * LANES] = jnp.where(number == slots, 1.0, 0.0).astype(jnp.bfloat16)

    def slot_sums(parts):
        return lax.dot_general(owned_slot[...], parts, (((1,), (1,)), ((), ())), preferred_element_type=F32)

    for i in range(HIST):
        parts = left_sides(lambda s: history_block(i, s))
        for part in range(3):
            sides8[part * 256 + i * 32:part * 256 + i * 32 + 32, :] = parts[part * 32:part * 32 + 32]
    sums = slot_sums(sides8[...])
    sums = sums[:, 0:256] + sums[:, 256:512] + sums[:, 512:768]
    for p in range(GROUP):
        send_old[p] = sums[p * 16:p * 16 + 16]
    other = 1 - me["c"]
    send(send_old.at[pl.ds(other * 8, 8)], old_c, OLD_C, {"c": other})
    pb0_total = group_sum(pb0_b, PB0_B)

    where = slot_index[0]
    new_moments(correct_density(pb0_total), where)
    gather(new_a, own_a, NEW_A, peers_a)

    arrived(old_c, OLD_C, 8)
    for z in range(8):
        mine_old[z] = send_old[me["c"] * 8 + z] + old_c[z]
    old_z[me["z"]] = mine_old[me["z"]]
    for peer in peers_z:
        send(mine_old.at[peer["z"]], old_z.at[me["z"]], OLD_Z, peer)

    for n in range(4):
        cols = slice(n * 256, n * 256 + 256)
        out = jnp.dot(sides8[...], same_atom[:, cols], preferred_element_type=F32)
        old_out[:, cols] = out[0:256] + out[256:512] + out[512:768]

    arrived(new_a, NEW_A, GROUP - 1)
    row = new_a[0, 12:13]
    for s in range(1, GROUP):
        row = row + new_a[s, 12:13]
    int1_b[own_b] = pltpu.roll(row, batches, 1)
    gather(int1_b, own_b, INT1_B, peers_b)
    fresh_parts = left_sides(lambda s: new_a[s])
    part_of = lane >> 5

    def every_part(x):
        x = x + pltpu.roll(x, 64, 1)
        return x + pltpu.roll(x, 32, 1)

    def packed_slots(low, high):
        return jnp.where(
            part_of < 2,
            jnp.where(part_of == 0, low, pltpu.roll(low, 4, 0)),
            jnp.where(part_of == 2, high, pltpu.roll(high, 4, 0)),
        )[0:4]

    fresh_sums = slot_sums(jnp.concatenate([fresh_parts, jnp.zeros((32, GROUP * batches), jnp.bfloat16)], axis=0))
    for p in range(GROUP):
        send_fresh[p] = packed_slots(
            every_part(fresh_sums[p * 16:p * 16 + 8]), every_part(fresh_sums[p * 16 + 8:p * 16 + 16])
        )
    scatter(send_fresh, fresh_b, FRESH_B)
    out = jnp.dot(fresh_parts, same_atom[...], preferred_element_type=F32)
    fresh_out[...] = out[0:32] + out[32:64] + out[64:96]
    old_total = group_sum(old_z, OLD_Z, 8)
    row = group_sum(int1_b, INT1_B)
    entries[40:48, :] = entry_values(row, 8)
    fresh_row = [splat(40, i) for i in range(HIST)]
    weights1 = mixing_weights([
        [jnp.where(where == i, fresh_row[j], jnp.where(where == j, fresh_row[i], pair(i, j))) for j in range(i + 1)]
        for i in range(HIST)
    ])

    kept = [jnp.where(where == i, 0.0, weights1[i]) for i in range(HIST)]
    fresh_weight = jnp.where(where == 0, weights1[0], 0.0)
    for i in range(1, HIST):
        fresh_weight = fresh_weight + jnp.where(where == i, weights1[i], 0.0)
    is_low = lane < batches
    for q in range(GROUP // 2):
        cols = slice(q * LANES, (q + 1) * LANES)
        tiles = []
        for r in range(4):
            tile = fresh_weight * fresh_out[8 * r:8 * r + 8, cols]
            for i in range(HIST):
                tile = tile + kept[i] * old_out[i * 32 + 8 * r:i * 32 + 8 * r + 8, cols]
            tiles.append(tile)
        for low, high, rows in ((tiles[0], tiles[2], 8), (tiles[1], tiles[3], ROWS - 8)):
            at = slice(0, 8) if rows == 8 else slice(8, ROWS)
            send1[2 * q, at] = jnp.where(is_low, low, pltpu.roll(high, batches, 1))[0:rows]
            send1[2 * q + 1, at] = jnp.where(is_low, pltpu.roll(low, batches, 1), high)[0:rows]
    scatter(send1, pb1_b, PB1_B)

    lower = kept[3]
    upper = kept[7]
    for n in range(3):
        lower = jnp.where(part_of == n, kept[n], lower)
        upper = jnp.where(part_of == n, kept[n + 4], upper)
    fresh_total = group_sum(fresh_b, FRESH_B)
    owned = []
    for n in range(2):
        rows = slice(8 * n, 8 * n + 8)
        value = old_total[rows, 0:LANES] * lower + old_total[rows, LANES:2 * LANES] * upper
        owned.append(every_part(value))
    piece = (packed_slots(*owned) + fresh_total * fresh_weight[0:4]) * moment_scale
    own_zy = me["z"] * 4 + me["y"]
    mom_zy[own_zy] = piece
    gather(mom_zy, own_zy, MOM_ZY, peers_zy)

    mixed_t[...] = mix_history(history_column(kept)) + jnp.broadcast_to(fresh_weight[0:1], (blocks, LANES)) * (
        den_t[...] + MIX_BETA * fresh_t[...]
    )
    correct_density(group_sum(pb1_b, PB1_B))
    by_block = den_t[...].T
    den[pl.ds(0, blocks // 2, stride=2), :] = by_block[0:blocks // 2]
    den[pl.ds(1, blocks // 2, stride=2), :] = by_block[blocks // 2:blocks]
    arrived(mom_zy, MOM_ZY, len(peers_zy))
    by_slot = jnp.concatenate([mom_zy[p] for p in range(32)], axis=0).T
    for g in range(4):
        cols, at = slice(g * LANES, (g + 1) * LANES), g * 32
        mom[0:8, cols] = by_slot[at:at + 8]
        mom[8:16, cols] = by_slot[at + 16:at + 24]
        mom[16:20, cols] = by_slot[at + 8:at + 12]
        mom[20:24, cols] = by_slot[at + 24:at + 28]
        mom[24:25, cols] = by_slot[at + 12:at + 13]

    for buf, key, count in (
        (int0_a, INT0_A, 15), (int0_b, INT0_B, 15), (atom_a, ATOM_A, 15), (atom_b, ATOM_B, 15),
        (slot_a, SLOT_A, 15), (hist_0, HIST_0, 11), (hist_0, ON_A, 4), (hist_1, HIST_1, 15), (hist_2, HIST_2, 15), (hist_3, HIST_3, 15),
        (last_a, LAST_A, 15),
        (new_a, NEW_A, 15), (int1_b, INT1_B, 15),
        (pb0_b, PB0_B, 15), (pb1_b, PB1_B, 15), (old_c, OLD_C, 8), (old_z, OLD_Z, 7), (fresh_b, FRESH_B, 15), (mom_zy, MOM_ZY, 31),
    ):
        sent(buf, key, count)


def hand_over(den, mom, den_h, mom_h, sem):
    copies = [pltpu.make_async_copy(den, den_h, sem.at[0]), pltpu.make_async_copy(mom, mom_h, sem.at[1])]
    for copy in copies:
        copy.start()
    for copy in copies:
        copy.wait()


def local(weights, target, coupling, basis, rho_hist, res_hist, batch_atom, owner_slot, slot_index):
    points = weights.shape[0]
    blocks = points // LANES
    harmonics = basis.shape[0]
    batches = batch_atom.shape[0]
    slots = owner_slot.shape[0]
    dense = lambda x: x.reshape(blocks, LANES)
    operands = (
        dense(weights), dense(target), dense(coupling), basis, rho_hist, res_hist,
        batch_atom.reshape(1, batches), owner_slot.reshape(slots // LANES, LANES), slot_index,
    )
    hbm = pl.BlockSpec(memory_space=pltpu.HBM)
    vmem = pl.BlockSpec(memory_space=pltpu.VMEM)
    dense_rows = lambda: pltpu.VMEM((blocks, LANES), F32)
    small = lambda dtype: pltpu.VMEM((GROUP, 1, LANES), dtype)
    pair_block = lambda: pltpu.VMEM((GROUP, 2, ROWS - 1, LANES), F32)
    block = lambda count: pltpu.VMEM((count, ROWS, LANES), F32)
    relation = pltpu.VMEM((GROUP * batches, GROUP * batches), jnp.bfloat16)
    density, moments = pl.pallas_call(
        body,
        out_shape=(
            jax.ShapeDtypeStruct((blocks, LANES), F32),
            jax.ShapeDtypeStruct((harmonics, slots // 8), F32),
        ),
        in_specs=[hbm] * len(operands),
        out_specs=(vmem, vmem),
        scratch_shapes=[
            pltpu.VMEM((blocks, LANES), F32),
            pltpu.VMEM((blocks, LANES), F32),
            pltpu.VMEM((blocks, LANES), F32),
            pltpu.VMEM((harmonics, points), F32),
            pltpu.VMEM((HIST, points), F32),
            pltpu.VMEM((HIST, points), F32),
            pltpu.VMEM((HIST, points), F32),
            pltpu.VMEM((1, batches), jnp.int32),
            pltpu.VMEM((slots // LANES, LANES), jnp.int32),
            pltpu.VMEM((8, blocks, LANES), F32),
            dense_rows(), dense_rows(), dense_rows(), dense_rows(), dense_rows(), dense_rows(), dense_rows(),
            pltpu.VMEM((harmonics, blocks, LANES), F32),
            pltpu.VMEM((HIST, blocks, LANES), F32),
            pltpu.VMEM((32, LANES), F32),
            pltpu.SMEM((2,), jnp.int32),
            pltpu.VMEM((48, LANES), F32),
            relation,
            pltpu.VMEM((GROUP * 16, GROUP * batches), jnp.bfloat16),
            pltpu.VMEM((HIST * 3 * 32, GROUP * batches), jnp.bfloat16),
            pltpu.VMEM((HIST * 32, GROUP * batches), F32),
            pltpu.VMEM((32, GROUP * batches), F32),
            small(F32), small(F32), small(F32), small(jnp.int32), small(jnp.int32), small(jnp.int32),
            pair_block(), pair_block(), pair_block(), pair_block(),
            pltpu.VMEM((GROUP, 4, LANES), F32),
            block(GROUP), block(GROUP), block(GROUP),
            pltpu.VMEM((8, 16, 2 * LANES), F32),
            pltpu.VMEM((8, 16, 2 * LANES), F32),
            pltpu.VMEM((GROUP, 4, LANES), F32),
            pltpu.VMEM((32, 4, LANES), F32),
            block(GROUP), block(GROUP),
            pltpu.VMEM((GROUP, 16, 2 * LANES), F32),
            pltpu.VMEM((8, 16, 2 * LANES), F32),
            pltpu.VMEM((GROUP, 4, LANES), F32),
            pltpu.SemaphoreType.DMA((LOCALS,)),
            pltpu.SemaphoreType.DMA((EXCHANGES,)),
            pltpu.SemaphoreType.DMA((EXCHANGES,)),
        ],
        compiler_params=pltpu.CompilerParams(collective_id=0, has_side_effects=True, vmem_limit_bytes=24 << 20),
    )(
        *(pltpu.with_memory_space_constraint(x, pltpu.HBM) for x in operands)
    )
    density, moments = pl.pallas_call(
        hand_over,
        out_shape=(
            jax.ShapeDtypeStruct((blocks, LANES), F32),
            jax.ShapeDtypeStruct((harmonics, slots // 8), F32),
        ),
        in_specs=[vmem, vmem],
        out_specs=(hbm, hbm),
        scratch_shapes=[pltpu.SemaphoreType.DMA((2,))],
        compiler_params=pltpu.CompilerParams(vmem_limit_bytes=1 << 20),
    )(density, moments)
    return density.reshape(points), moments


def solution(mesh):
    torus = Mesh(mesh.devices.reshape(tuple(SIZES.values())), AXES)
    points = P(AXES)
    rows = P(None, AXES)
    return jax.shard_map(
        local,
        mesh=torus,
        in_specs=(points, points, points, rows, rows, rows, points, P(), P()),
        out_specs=(points, P(None, ("x", "c"))),
        check_vma=False,
    )
```

```python
import itertools

import jax
import jax.numpy as jnp
from jax import lax
from jax.experimental import pallas as pl
from jax.experimental.pallas import tpu as pltpu
from jax.sharding import Mesh
from jax.sharding import PartitionSpec as P

AXES = ("z", "y", "x", "c")
SIZES = {"z": 8, "y": 4, "x": 4, "c": 2}
HIST = 8
LANES = 128
MESH = pl.DeviceIdType.MESH
F32 = jnp.float32
MIX_BETA = 0.5
RIDGE_SHARE = 0.1
GROUP = 16
ROWS = 13
INT0_A, INT0_B, ATOM_A, ATOM_B, SLOT_A, HIST_0, HIST_1, HIST_2, HIST_3, LAST_A, NEW_A, INT1_B, PB0_B, PB1_B, OLD_C, OLD_Z, FRESH_B, MOM_ZY, ON_A = range(19)
EXCHANGES = 19
HIST_KEYS = (HIST_0, HIST_1, HIST_2, HIST_3)
LD_RES, LD_W, LD_ATOM, LD_OWNER, LD_BASIS, LD_RHO, LD_TARGET, LD_COUPLING, LD_INDEX = range(9)
LOCALS = 9


def iota(shape, dim):
    return lax.broadcasted_iota(jnp.int32, shape, dim)


def sublane_total(x):
    x = x + pltpu.roll(x, 4, 0)
    x = x + pltpu.roll(x, 2, 0)
    return x + pltpu.roll(x, 1, 0)


def mixing_weights(entry):
    matrix = [[entry[i][j] for j in range(i + 1)] for i in range(HIST)]
    trace = matrix[0][0]
    for i in range(1, HIST):
        trace = trace + matrix[i][i]
    ridge = trace * (RIDGE_SHARE / HIST)
    for i in range(HIST):
        matrix[i][i] = matrix[i][i] + ridge
    forward = [jnp.ones((8, LANES), F32) for _ in range(HIST)]
    pivot = [None] * HIST
    lower = [[None] * HIST for _ in range(HIST)]
    for j in range(HIST):
        pivot[j] = 1.0 / matrix[j][j]
        for i in range(j + 1, HIST):
            ratio = matrix[i][j] * pivot[j]
            for k in range(j + 1, i + 1):
                matrix[i][k] = matrix[i][k] - ratio * matrix[k][j]
            forward[i] = forward[i] - ratio * forward[j]
            lower[i][j] = ratio
    solved = [None] * HIST
    for i in reversed(range(HIST)):
        value = forward[i] * pivot[i]
        for k in range(i + 1, HIST):
            value = value - lower[k][i] * solved[k]
        solved[i] = value
    total = solved[0]
    for i in range(1, HIST):
        total = total + solved[i]
    scale = 1.0 / total
    return [value * scale for value in solved]


def history_column(values):
    sub = iota((8, LANES), 0)
    column = jnp.zeros((8, LANES), F32)
    for i in range(HIST):
        column = jnp.where(sub == i, values[i], column)
    return column


def three_parts(x):
    high = x.astype(jnp.bfloat16)
    rest = x - high.astype(F32)
    middle = rest.astype(jnp.bfloat16)
    low = (rest - middle.astype(F32)).astype(jnp.bfloat16)
    return jnp.concatenate([high, middle, low], axis=0)


def body(
    w_h, t_h, cpl_h, basis_h, rho_h, res_h, atom_h, owner_h, index_h,
    den, mom,
    w, t, cpl, basis, rho, res, wres, atom, owner, rows8, mixed, w_t, target_t, coupling_t, mixed_t, den_t, fresh_t, basis_t, res_t, coef, slot_index,
    entries, same_atom, owned_slot, sides8, old_out, fresh_out,
    int0_a, int0_b, int1_b, atom_a, atom_b, slot_a,
    hist_0, hist_1, hist_2, hist_3, last_a, new_a, pb0_b, pb1_b, old_c, old_z, fresh_b, mom_zy, send0, send1, send_old, mine_old, send_fresh,
    local_sem, send_sem, recv_sem,
):
    me = {name: lax.axis_index(name) for name in AXES}
    own_a = me["y"] * 4 + me["x"]
    hist_a = (hist_0, hist_1, hist_2, hist_3)
    own_b = me["c"] * 8 + me["z"]
    blocks = w.shape[0]

    loads = {}

    def load(*copies):
        for key, src, dst in copies:
            loads[key] = pltpu.make_async_copy(src, dst, local_sem.at[key])
            loads[key].start()

    load((LD_RES, res_h, res), (LD_W, w_h, w), (LD_BASIS, basis_h, basis), (LD_ATOM, atom_h, atom))

    def steps_along(*names):
        steps = [s for s in itertools.product(*(range(SIZES[name]) for name in names)) if any(s)]
        hops = lambda s: sum(min(d, SIZES[name] - d) for d, name in zip(s, names))
        return sorted(steps, key=hops, reverse=True)

    def peers(*names):
        return [
            {name: lax.rem(me[name] + d, SIZES[name]) for d, name in zip(s, names)} for s in steps_along(*names)
        ]

    peers_a, peers_b, peers_z, peers_zy = peers("y", "x"), peers("z", "c"), peers("z"), peers("z", "y")
    peers_near = [peer for peer, step in zip(peers_a, steps_along("y", "x")) if step[1] != 2]

    barrier = pltpu.get_barrier_semaphore()
    for peer in peers_a + peers_b:
        pl.semaphore_signal(barrier, inc=1, device_id=peer, device_id_type=MESH)
    load(
        (LD_OWNER, owner_h, owner), (LD_RHO, rho_h, rho), (LD_TARGET, t_h, t), (LD_COUPLING, cpl_h, cpl),
        (LD_INDEX, index_h, slot_index),
    )

    def send(src, dst, key, peer):
        pltpu.make_async_remote_copy(
            src_ref=src, dst_ref=dst, send_sem=send_sem.at[key], recv_sem=recv_sem.at[key],
            device_id=peer, device_id_type=MESH,
        ).start()

    def gather(buf, own, key, peers):
        for peer in peers:
            send(buf.at[own], buf.at[own], key, peer)

    def arrived(buf, key, count):
        view = buf.at[pl.ds(0, count)]
        pltpu.make_async_copy(view, view, recv_sem.at[key]).wait()

    def sent(buf, key, count):
        view = buf.at[pl.ds(0, count)]
        pltpu.make_async_copy(view, view, send_sem.at[key]).wait()

    sub = iota((8, LANES), 0)
    lane = iota((8, LANES), 1)

    loads[LD_RES].wait()
    loads[LD_W].wait()

    def products(q, accs):
        accs = list(accs)
        for u in range(8):
            off = pl.multiple_of((q * 8 + u) * LANES, LANES)
            r = res[:, pl.ds(off, LANES)]
            rw = r * jnp.broadcast_to(w[pl.ds(q * 8 + u, 1), :], (8, LANES))
            wres[:, pl.ds(off, LANES)] = rw
            accs[0] = accs[0] + rw * r
            for s in range(1, 5):
                accs[s] = accs[s] + rw * pltpu.roll(r, s, 0)
        return tuple(accs)

    zero = jnp.zeros((8, LANES), F32)
    accs = lax.fori_loop(0, blocks // 8, products, (zero,) * 5)
    placed = zero
    for s in range(5):
        total = jnp.sum(accs[s], axis=1, keepdims=True)
        placed = jnp.where(lane == 8 * s + sub, total, placed)
    int0_a[own_a] = sublane_total(placed)[0:1, :]

    batches = 64
    loads[LD_BASIS].wait()

    def place(b, parts, k01, k2):
        k01 = jnp.where(lane == b, parts[0], k01)
        k01 = jnp.where(lane == b + batches, parts[1], k01)
        return k01, jnp.where(lane == b + jnp.where(sub >= 4, batches, 0), parts[2], k2)

    def batch_spans(b):
        return [pl.ds(pl.multiple_of((2 * b + h) * LANES, LANES), LANES) for h in range(2)]

    def chunk_moments(chunk):
        def one(b, carry):
            carry = list(carry)
            offs = batch_spans(b)
            tiles = [[basis[kt * 8:kt * 8 + 8, off] for off in offs] for kt in range(3)]
            for n in range(2):
                i = 2 * chunk + n
                field = [jnp.broadcast_to(wres[i:i + 1, off], (8, LANES)) for off in offs]
                parts = [
                    jnp.sum(tiles[kt][0] * field[0] + tiles[kt][1] * field[1], axis=1, keepdims=True)
                    for kt in range(3)
                ]
                carry[2 * n], carry[2 * n + 1] = place(b, parts, carry[2 * n], carry[2 * n + 1])
            return tuple(carry)

        return lax.fori_loop(0, batches, one, (zero,) * 4, unroll=8)

    def last_harmonic(b, placed):
        offs = batch_spans(b)
        last = [wres[:, off] * jnp.broadcast_to(basis[24:25, off], (8, LANES)) for off in offs]
        return jnp.where(lane == b, jnp.sum(last[0] + last[1], axis=1, keepdims=True), placed)

    def put_moments(buf, at, k01, k2):
        buf[(*at, slice(0, 8))] = k01
        buf[(*at, slice(8, 12))] = (k2 + pltpu.roll(k2, 4, 0))[0:4]

    def fill_chunk(chunk):
        found = chunk_moments(chunk)
        for n in range(2):
            put_moments(hist_a[chunk], (own_a, n), found[2 * n], found[2 * n + 1])

    loads[LD_ATOM].wait()
    atom_wide = jnp.concatenate([atom[...], atom[...]], axis=1)
    atom_a[own_a] = atom_wide
    atom_b[own_b] = atom_wide
    fill_chunk(0)

    pl.semaphore_wait(barrier, len(peers_a) + len(peers_b))
    gather(int0_a, own_a, INT0_A, peers_a)
    gather(atom_a, own_a, ATOM_A, peers_a)
    gather(atom_b, own_b, ATOM_B, peers_b)
    gather(hist_a[0], own_a, HIST_0, peers_near)
    for chunk in range(1, 4):
        if chunk == 3:
            last = lax.fori_loop(0, batches, last_harmonic, zero, unroll=8)
            last = jnp.where(lane < batches, last, pltpu.roll(pltpu.roll(last, 4, 0), batches, 1))
            last_a[own_a] = last[0:4]
            gather(last_a, own_a, LAST_A, peers_a)
        fill_chunk(chunk)
        gather(hist_a[chunk], own_a, HIST_KEYS[chunk], peers_a)

    loads[LD_OWNER].wait()
    wide_sub = iota((batches, LANES), 0)
    wide_lane = iota((batches, LANES), 1)
    own_lane = wide_lane == wide_sub

    def as_column(row):
        return jnp.sum(jnp.where(own_lane, jnp.broadcast_to(row, (batches, LANES)), 0.0), axis=1, keepdims=True)

    atom_col = as_column(atom_wide.astype(F32))

    def look_up(j, found):
        owners = jnp.broadcast_to(owner[pl.ds(j, 1), :].astype(F32), (batches, LANES))
        number = (wide_lane + j * LANES).astype(F32)
        return found + jnp.where(number == atom_col, owners, 0.0)

    found = lax.fori_loop(0, owner.shape[0], look_up, jnp.zeros((batches, LANES), F32))
    slot_col = jnp.sum(found, axis=1, keepdims=True)
    slot_a[own_a] = jnp.sum(jnp.where(own_lane, slot_col, 0.0), axis=0, keepdims=True).astype(jnp.int32)
    gather(slot_a, own_a, SLOT_A, peers_a)

    def group_sum(buf, key, count=GROUP):
        arrived(buf, key, count - 1)
        total = buf[0]
        for i in range(1, count):
            total = total + buf[i]
        return total

    int0_b[own_b] = group_sum(int0_a, INT0_A)
    gather(int0_b, own_b, INT0_B, peers_b)

    arrived(hist_0, HIST_0, len(peers_near))
    for y in range(4):
        for n, step in ((0, 1), (1, 3)):
            block_at = hist_0.at[y * 4 + lax.rem(me["x"] + 4 - step, 4), n]
            send(block_at, block_at, ON_A, {"x": lax.rem(me["x"] + step, 4)})

    arrived(atom_a, ATOM_A, GROUP - 1)
    arrived(atom_b, ATOM_B, GROUP - 1)
    half = iota((1, LANES), 1) < batches
    atoms_b = [jnp.where(half, atom_b[2 * q], atom_b[2 * q + 1]).astype(F32) for q in range(GROUP // 2)]

    def relate_atoms(s, nothing):
        atoms_a = as_column(atom_a[s].astype(F32))
        at = pl.ds(pl.multiple_of(s * batches, batches), batches)
        for q in range(GROUP // 2):
            cols = pl.ds(q * LANES, LANES)
            same_atom[at, cols] = jnp.where(atoms_a == atoms_b[q], 1.0, 0.0).astype(jnp.bfloat16)
        return nothing

    lax.fori_loop(0, GROUP, relate_atoms, 0)

    def spread(tiles):
        for bit in (4, 2, 1):
            low = (sub & bit) == 0
            swapped = list(tiles)
            for j in range(8):
                if not j & bit:
                    first, second = tiles[j], tiles[j | bit]
                    swapped[j] = jnp.where(low, first, pltpu.roll(second, bit, 0))
                    swapped[j | bit] = jnp.where(low, pltpu.roll(first, 8 - bit, 0), second)
            tiles = swapped
        return tiles

    def block_span(g, r):
        j = 2 * (8 * (g & 7) + r) + (g >> 3)
        return pl.ds(pl.multiple_of(j * LANES, LANES), LANES)

    def group_rows(g):
        return pl.ds(pl.multiple_of(g * 8, 8), 8)

    def turn_rows(src, start, dst):
        def collect(g, nothing):
            for k, tile in enumerate(spread([src[start:start + 8, block_span(g, r)] for r in range(8)])):
                rows8[k, group_rows(g), :] = tile
            return nothing

        lax.fori_loop(0, blocks // 8, collect, 0, unroll=2)

        def turn(k, nothing):
            dst[start + k] = rows8[k].T
            return nothing

        lax.fori_loop(0, 8, turn, 0, unroll=2)

    def by_half(ref):
        return jnp.concatenate([ref[pl.ds(0, blocks // 2, stride=2), :], ref[pl.ds(1, blocks // 2, stride=2), :]], axis=0)

    for start in range(0, 24, 8):
        turn_rows(basis, start, basis_t)

    def last_row(q, nothing):
        for u in range(8):
            at = (u % 2) * (blocks // 2) + q * 4 + u // 2
            mixed[pl.ds(at, 1), :] = basis[24:25, pl.ds(pl.multiple_of((q * 8 + u) * LANES, LANES), LANES)]
        return nothing

    lax.fori_loop(0, blocks // 8, last_row, 0)
    basis_t[24] = mixed[...].T
    w_t[...] = by_half(w).T

    def entry_values(row, count):
        rows = iota((count, LANES), 0)
        lanes = iota((count, LANES), 1)
        total = jnp.sum(jnp.where(rows == lanes, jnp.broadcast_to(row, (count, LANES)), 0.0), axis=1, keepdims=True)
        return jnp.broadcast_to(total, (count, LANES))

    def splat(base, i):
        return jnp.broadcast_to(entries[pl.ds(base + i, 1), :], (8, LANES))

    def left_sides(block_of):
        is_low = iota((ROWS, LANES), 1) < batches
        lows, highs = [], []
        for q in range(GROUP // 2):
            first, second = block_of(2 * q), block_of(2 * q + 1)
            crossed = pltpu.roll(jnp.where(is_low, second, first), batches, 1)
            lows.append(jnp.where(is_low, first, crossed))
            highs.append(jnp.where(is_low, crossed, second))
        pad = jnp.zeros((16 - ROWS, GROUP * batches), F32)
        low = jnp.concatenate(lows, axis=1)
        high = jnp.concatenate(highs, axis=1)
        return three_parts(jnp.concatenate([low, pad, high, pad], axis=0))

    def contributions(parts, matrix, out):
        result = jnp.dot(parts, matrix[...], preferred_element_type=F32)
        pack_contributions(result[0:32] + result[32:64] + result[64:96], out)

    def pack_contributions(result, out):
        is_low = iota((ROWS, LANES), 1) < batches
        for q in range(GROUP // 2):
            cols = slice(q * LANES, (q + 1) * LANES)
            low, high = result[0:ROWS, cols], result[16:16 + ROWS, cols]
            crossed = pltpu.roll(jnp.where(is_low, high, low), batches, 1)
            out[2 * q] = jnp.where(is_low, low, crossed)
            out[2 * q + 1] = jnp.where(is_low, crossed, high)

    def scatter(out, buf, key):
        buf[own_b] = out[own_b]
        for peer in peers_b:
            send(out.at[peer.get("c") * 8 + peer.get("z")], buf.at[own_b], key, peer)

    def packed_scale(rows):
        r, c = iota((rows, LANES), 0), iota((rows, LANES), 1)
        high = c >= batches
        k = jnp.where(r < 8, jnp.where(high, r + 8, r), jnp.where(high, r + 12, r + 8))
        k = jnp.where(r == 12, 24, k)
        degree = (
            jnp.where(k >= 1, 1, 0) + jnp.where(k >= 4, 1, 0) + jnp.where(k >= 9, 1, 0) + jnp.where(k >= 16, 1, 0)
        )
        return 1.0 / (1.0 + degree.astype(F32))

    moment_scale = 1.0 / 32.0

    def folded(tiles):
        for bit in (4, 2, 1):
            low = (sub & bit) == 0
            count = len(tiles) // 2
            merged = []
            for first, second in zip(tiles[:count], tiles[count:]):
                given = jnp.where(low, second, first)
                if bit == 4:
                    given = pltpu.roll(given, 4, 0)
                else:
                    given = jnp.where(low, pltpu.roll(given, 8 - bit, 0), pltpu.roll(given, bit, 0))
                merged.append(jnp.where(low, first, second) + given)
            tiles = merged
        return tiles[0]

    def mix_history(column):
        def eight(g, nothing):
            offs = [block_span(g, r) for r in range(8)]
            mixed[group_rows(g), :] = folded([column * (rho[:, off] + MIX_BETA * res[:, off]) for off in offs])
            return nothing

        lax.fori_loop(0, blocks // 8, eight, 0, unroll=2)
        return mixed[...].T

    whole_half = lane < batches

    def correct_density(total):
        total = total * (packed_scale(ROWS) * (MIX_BETA * moment_scale))
        first = total[0:8]
        turned = pltpu.roll(first, batches, 1)
        rest = jnp.concatenate([total[8:13], jnp.zeros((3, LANES), F32)], axis=0)
        rest_turned = pltpu.roll(rest, batches, 1)
        low = jnp.where(whole_half, rest, rest_turned)
        high = jnp.where(whole_half, rest_turned, rest)
        coef[0:8] = jnp.where(whole_half, first, turned)
        coef[8:16] = jnp.where(whole_half, turned, first)
        coef[16:24] = jnp.where(sub < 4, low, pltpu.roll(high, 4, 0))
        coef[24:25] = low[4:5]
        factors = [jnp.broadcast_to(coef[k:k + 1, :], (8, LANES)) for k in range(25)]
        found = []
        for v in range(blocks // 8):
            rows = slice(8 * v, 8 * v + 8)
            value = factors[0] * basis_t[0, rows]
            for k in range(1, 25):
                value = value + factors[k] * basis_t[k, rows]
            found.append(mixed_t[rows] - value)
            den_t[rows] = found[-1]
        return found

    def add_up(terms):
        while len(terms) > 1:
            terms = [sum(terms[n:n + 2][1:], terms[n]) for n in range(0, len(terms), 2)]
        return terms[0]

    def new_moments(dense, where):
        spans = [slice(8 * v, 8 * v + 8) for v in range(blocks // 8)]
        fresh, weighted = [], []
        for rows, value in zip(spans, dense):
            fresh.append(target_t[rows] + coupling_t[rows] * jnp.tanh(value) - value)
            fresh_t[rows] = fresh[-1]
            weighted.append(fresh[-1] * w_t[rows])

        def both_halves(x):
            return x + pltpu.roll(x, batches, 1)

        sums = [add_up([x * basis_t[k, rows] for x, rows in zip(weighted, spans)]) for k in range(25)]
        k0, k1, k2 = (both_halves(folded(sums[kt * 8:kt * 8 + 8])) for kt in range(3))
        k3 = both_halves(sublane_total(sums[24]))[0:1]
        itself = add_up([x * y for x, y in zip(weighted, fresh)])
        sums = [
            jnp.where(where == i, itself, add_up([x * res_t[i, rows] for x, rows in zip(weighted, spans)]))
            for i in range(HIST)
        ]
        total = jnp.sum(folded(sums), axis=1, keepdims=True)
        row = sublane_total(jnp.where(lane == sub + batches, total, 0.0))[0:1, :]
        new_a[own_a, 0:8] = jnp.where(whole_half, k0, k1)
        new_a[own_a, 8:12] = jnp.where(whole_half, k2, pltpu.roll(k2, 4, 0))[0:4]
        new_a[own_a, 12:13] = jnp.where(half, k3, row)

    row = group_sum(int0_b, INT0_B)
    entries[0:40, :] = entry_values(row, 40)

    def pair(i, j):
        s = (i - j) % 8
        return splat(0, 8 * s + i) if s <= 4 else splat(0, 8 * ((j - i) % 8) + j)

    weights0 = mixing_weights([[pair(i, j) for j in range(i + 1)] for i in range(HIST)])
    column0 = history_column(weights0)

    def history_block(i, s):
        row = last_a[s, i % 4:i % 4 + 1]
        return jnp.concatenate([hist_a[i // 2][s, i % 2], row if i < 4 else pltpu.roll(row, batches, 1)], axis=0)

    def mixed_block(values, packed, s):
        total = jnp.broadcast_to(values[0][0:1], (ROWS - 1, LANES)) * hist_a[0][s, 0]
        for i in range(1, HIST):
            total = total + jnp.broadcast_to(values[i][0:1], (ROWS - 1, LANES)) * hist_a[i // 2][s, i % 2]
        last = packed * last_a[s]
        last = last[0:1] + last[1:2] + last[2:3] + last[3:4]
        return jnp.concatenate([total, last + pltpu.roll(last, batches, 1)], axis=0)

    arrived(hist_0, ON_A, 4)
    for chunk in range(1, 4):
        arrived(hist_a[chunk], HIST_KEYS[chunk], GROUP - 1)
    arrived(last_a, LAST_A, GROUP - 1)
    packed0 = jnp.where(lane < batches, column0, pltpu.roll(column0, 4, 0))[0:4]
    contributions(left_sides(lambda s: mixed_block(weights0, packed0, s)), same_atom, send0)
    scatter(send0, pb0_b, PB0_B)
    loads[LD_RHO].wait()
    loads[LD_TARGET].wait()
    loads[LD_COUPLING].wait()
    loads[LD_INDEX].wait()
    mixed_t[...] = mix_history(column0)
    target_t[...] = by_half(t).T
    coupling_t[...] = by_half(cpl).T
    turn_rows(res, 0, res_t)

    arrived(slot_a, SLOT_A, GROUP - 1)
    place_of = iota((GROUP * 16, LANES), 0)
    number = me["x"] * (GROUP * batches) + me["y"] * 4
    number = number + (place_of >> 7) * 512 + ((place_of >> 4) & 7) * 16 + ((place_of >> 2) & 3) * LANES + (place_of & 3)
    for q in range(GROUP // 2):
        slots = jnp.where(half, slot_a[2 * q], pltpu.roll(slot_a[2 * q + 1], batches, 1))
        owned_slot[:, q * LANES:(q + 1) * LANES] = jnp.where(number == slots, 1.0, 0.0).astype(jnp.bfloat16)

    def slot_sums(parts):
        return lax.dot_general(owned_slot[...], parts, (((1,), (1,)), ((), ())), preferred_element_type=F32)

    for i in range(HIST):
        parts = left_sides(lambda s: history_block(i, s))
        for part in range(3):
            sides8[part * 256 + i * 32:part * 256 + i * 32 + 32, :] = parts[part * 32:part * 32 + 32]
    sums = slot_sums(sides8[...])
    sums = sums[:, 0:256] + sums[:, 256:512] + sums[:, 512:768]
    for p in range(GROUP):
        send_old[p] = sums[p * 16:p * 16 + 16]
    other = 1 - me["c"]
    send(send_old.at[pl.ds(other * 8, 8)], old_c, OLD_C, {"c": other})
    pb0_total = group_sum(pb0_b, PB0_B)

    where = slot_index[0]
    new_moments(correct_density(pb0_total), where)
    gather(new_a, own_a, NEW_A, peers_a)

    arrived(old_c, OLD_C, 8)
    for z in range(8):
        mine_old[z] = send_old[me["c"] * 8 + z] + old_c[z]
    old_z[me["z"]] = mine_old[me["z"]]
    for peer in peers_z:
        send(mine_old.at[peer["z"]], old_z.at[me["z"]], OLD_Z, peer)

    for n in range(4):
        cols = slice(n * 256, n * 256 + 256)
        out = jnp.dot(sides8[...], same_atom[:, cols], preferred_element_type=F32)
        old_out[:, cols] = out[0:256] + out[256:512] + out[512:768]

    arrived(new_a, NEW_A, GROUP - 1)
    row = new_a[0, 12:13]
    for s in range(1, GROUP):
        row = row + new_a[s, 12:13]
    int1_b[own_b] = pltpu.roll(row, batches, 1)
    gather(int1_b, own_b, INT1_B, peers_b)
    fresh_parts = left_sides(lambda s: new_a[s])
    part_of = lane >> 5

    def every_part(x):
        x = x + pltpu.roll(x, 64, 1)
        return x + pltpu.roll(x, 32, 1)

    def packed_slots(low, high):
        return jnp.where(
            part_of < 2,
            jnp.where(part_of == 0, low, pltpu.roll(low, 4, 0)),
            jnp.where(part_of == 2, high, pltpu.roll(high, 4, 0)),
        )[0:4]

    fresh_sums = slot_sums(jnp.concatenate([fresh_parts, jnp.zeros((32, GROUP * batches), jnp.bfloat16)], axis=0))
    for p in range(GROUP):
        send_fresh[p] = packed_slots(
            every_part(fresh_sums[p * 16:p * 16 + 8]), every_part(fresh_sums[p * 16 + 8:p * 16 + 16])
        )
    scatter(send_fresh, fresh_b, FRESH_B)
    out = jnp.dot(fresh_parts, same_atom[...], preferred_element_type=F32)
    fresh_out[...] = out[0:32] + out[32:64] + out[64:96]
    old_total = group_sum(old_z, OLD_Z, 8)
    row = group_sum(int1_b, INT1_B)
    entries[40:48, :] = entry_values(row, 8)
    fresh_row = [splat(40, i) for i in range(HIST)]
    weights1 = mixing_weights([
        [jnp.where(where == i, fresh_row[j], jnp.where(where == j, fresh_row[i], pair(i, j))) for j in range(i + 1)]
        for i in range(HIST)
    ])

    kept = [jnp.where(where == i, 0.0, weights1[i]) for i in range(HIST)]
    fresh_weight = jnp.where(where == 0, weights1[0], 0.0)
    for i in range(1, HIST):
        fresh_weight = fresh_weight + jnp.where(where == i, weights1[i], 0.0)
    is_low = lane < batches
    for q in range(GROUP // 2):
        cols = slice(q * LANES, (q + 1) * LANES)
        tiles = []
        for r in range(4):
            tile = fresh_weight * fresh_out[8 * r:8 * r + 8, cols]
            for i in range(HIST):
                tile = tile + kept[i] * old_out[i * 32 + 8 * r:i * 32 + 8 * r + 8, cols]
            tiles.append(tile)
        for low, high, rows in ((tiles[0], tiles[2], 8), (tiles[1], tiles[3], ROWS - 8)):
            at = slice(0, 8) if rows == 8 else slice(8, ROWS)
            crossed = pltpu.roll(jnp.where(is_low, high, low), batches, 1)
            send1[2 * q, at] = jnp.where(is_low, low, crossed)[0:rows]
            send1[2 * q + 1, at] = jnp.where(is_low, crossed, high)[0:rows]
    scatter(send1, pb1_b, PB1_B)

    lower = kept[3]
    upper = kept[7]
    for n in range(3):
        lower = jnp.where(part_of == n, kept[n], lower)
        upper = jnp.where(part_of == n, kept[n + 4], upper)
    fresh_total = group_sum(fresh_b, FRESH_B)
    owned = []
    for n in range(2):
        rows = slice(8 * n, 8 * n + 8)
        value = old_total[rows, 0:LANES] * lower + old_total[rows, LANES:2 * LANES] * upper
        owned.append(every_part(value))
    piece = (packed_slots(*owned) + fresh_total * fresh_weight[0:4]) * moment_scale
    own_zy = me["z"] * 4 + me["y"]
    mom_zy[own_zy] = piece
    gather(mom_zy, own_zy, MOM_ZY, peers_zy)

    mixed_t[...] = mix_history(history_column(kept)) + jnp.broadcast_to(fresh_weight[0:1], (blocks, LANES)) * (
        den_t[...] + MIX_BETA * fresh_t[...]
    )
    correct_density(group_sum(pb1_b, PB1_B))
    by_block = den_t[...].T
    den[pl.ds(0, blocks // 2, stride=2), :] = by_block[0:blocks // 2]
    den[pl.ds(1, blocks // 2, stride=2), :] = by_block[blocks // 2:blocks]
    arrived(mom_zy, MOM_ZY, len(peers_zy))
    by_slot = jnp.concatenate([mom_zy[p] for p in range(32)], axis=0).T
    for g in range(4):
        cols, at = slice(g * LANES, (g + 1) * LANES), g * 32
        mom[0:8, cols] = by_slot[at:at + 8]
        mom[8:16, cols] = by_slot[at + 16:at + 24]
        mom[16:20, cols] = by_slot[at + 8:at + 12]
        mom[20:24, cols] = by_slot[at + 24:at + 28]
        mom[24:25, cols] = by_slot[at + 12:at + 13]

    for buf, key, count in (
        (int0_a, INT0_A, 15), (int0_b, INT0_B, 15), (atom_a, ATOM_A, 15), (atom_b, ATOM_B, 15),
        (slot_a, SLOT_A, 15), (hist_0, HIST_0, 11), (hist_0, ON_A, 4), (hist_1, HIST_1, 15), (hist_2, HIST_2, 15), (hist_3, HIST_3, 15),
        (last_a, LAST_A, 15),
        (new_a, NEW_A, 15), (int1_b, INT1_B, 15),
        (pb0_b, PB0_B, 15), (pb1_b, PB1_B, 15), (old_c, OLD_C, 8), (old_z, OLD_Z, 7), (fresh_b, FRESH_B, 15), (mom_zy, MOM_ZY, 31),
    ):
        sent(buf, key, count)


def hand_over(den, mom, den_h, mom_h, sem):
    copies = [pltpu.make_async_copy(den, den_h, sem.at[0]), pltpu.make_async_copy(mom, mom_h, sem.at[1])]
    for copy in copies:
        copy.start()
    for copy in copies:
        copy.wait()


def local(weights, target, coupling, basis, rho_hist, res_hist, batch_atom, owner_slot, slot_index):
    points = weights.shape[0]
    blocks = points // LANES
    harmonics = basis.shape[0]
    batches = batch_atom.shape[0]
    slots = owner_slot.shape[0]
    dense = lambda x: x.reshape(blocks, LANES)
    operands = (
        dense(weights), dense(target), dense(coupling), basis, rho_hist, res_hist,
        batch_atom.reshape(1, batches), owner_slot.reshape(slots // LANES, LANES), slot_index,
    )
    hbm = pl.BlockSpec(memory_space=pltpu.HBM)
    vmem = pl.BlockSpec(memory_space=pltpu.VMEM)
    dense_rows = lambda: pltpu.VMEM((blocks, LANES), F32)
    small = lambda dtype: pltpu.VMEM((GROUP, 1, LANES), dtype)
    pair_block = lambda: pltpu.VMEM((GROUP, 2, ROWS - 1, LANES), F32)
    block = lambda count: pltpu.VMEM((count, ROWS, LANES), F32)
    relation = pltpu.VMEM((GROUP * batches, GROUP * batches), jnp.bfloat16)
    density, moments = pl.pallas_call(
        body,
        out_shape=(
            jax.ShapeDtypeStruct((blocks, LANES), F32),
            jax.ShapeDtypeStruct((harmonics, slots // 8), F32),
        ),
        in_specs=[hbm] * len(operands),
        out_specs=(vmem, vmem),
        scratch_shapes=[
            pltpu.VMEM((blocks, LANES), F32),
            pltpu.VMEM((blocks, LANES), F32),
            pltpu.VMEM((blocks, LANES), F32),
            pltpu.VMEM((harmonics, points), F32),
            pltpu.VMEM((HIST, points), F32),
            pltpu.VMEM((HIST, points), F32),
            pltpu.VMEM((HIST, points), F32),
            pltpu.VMEM((1, batches), jnp.int32),
            pltpu.VMEM((slots // LANES, LANES), jnp.int32),
            pltpu.VMEM((8, blocks, LANES), F32),
            dense_rows(), dense_rows(), dense_rows(), dense_rows(), dense_rows(), dense_rows(), dense_rows(),
            pltpu.VMEM((harmonics, blocks, LANES), F32),
            pltpu.VMEM((HIST, blocks, LANES), F32),
            pltpu.VMEM((32, LANES), F32),
            pltpu.SMEM((2,), jnp.int32),
            pltpu.VMEM((48, LANES), F32),
            relation,
            pltpu.VMEM((GROUP * 16, GROUP * batches), jnp.bfloat16),
            pltpu.VMEM((HIST * 3 * 32, GROUP * batches), jnp.bfloat16),
            pltpu.VMEM((HIST * 32, GROUP * batches), F32),
            pltpu.VMEM((32, GROUP * batches), F32),
            small(F32), small(F32), small(F32), small(jnp.int32), small(jnp.int32), small(jnp.int32),
            pair_block(), pair_block(), pair_block(), pair_block(),
            pltpu.VMEM((GROUP, 4, LANES), F32),
            block(GROUP), block(GROUP), block(GROUP),
            pltpu.VMEM((8, 16, 2 * LANES), F32),
            pltpu.VMEM((8, 16, 2 * LANES), F32),
            pltpu.VMEM((GROUP, 4, LANES), F32),
            pltpu.VMEM((32, 4, LANES), F32),
            block(GROUP), block(GROUP),
            pltpu.VMEM((GROUP, 16, 2 * LANES), F32),
            pltpu.VMEM((8, 16, 2 * LANES), F32),
            pltpu.VMEM((GROUP, 4, LANES), F32),
            pltpu.SemaphoreType.DMA((LOCALS,)),
            pltpu.SemaphoreType.DMA((EXCHANGES,)),
            pltpu.SemaphoreType.DMA((EXCHANGES,)),
        ],
        compiler_params=pltpu.CompilerParams(collective_id=0, has_side_effects=True, vmem_limit_bytes=24 << 20),
    )(
        *(pltpu.with_memory_space_constraint(x, pltpu.HBM) for x in operands)
    )
    density, moments = pl.pallas_call(
        hand_over,
        out_shape=(
            jax.ShapeDtypeStruct((blocks, LANES), F32),
            jax.ShapeDtypeStruct((harmonics, slots // 8), F32),
        ),
        in_specs=[vmem, vmem],
        out_specs=(hbm, hbm),
        scratch_shapes=[pltpu.SemaphoreType.DMA((2,))],
        compiler_params=pltpu.CompilerParams(vmem_limit_bytes=1 << 20),
    )(density, moments)
    return density.reshape(points), moments


def solution(mesh):
    torus = Mesh(mesh.devices.reshape(tuple(SIZES.values())), AXES)
    points = P(AXES)
    rows = P(None, AXES)
    return jax.shard_map(
        local,
        mesh=torus,
        in_specs=(points, points, points, rows, rows, rows, points, P(), P()),
        out_specs=(points, P(None, ("x", "c"))),
        check_vma=False,
    )
```
